32 devices in a mesh: groups: 2 (over y), kvb: 4 (over z), tp: 4 (over x, core).
Axes of the slice: x: 2, y: 2, z: 4, core: 2. Of those that a mesh axis runs over, the one named last changes fastest.
Arguments:
- residual: bfloat16 [32, 8192], P(('groups', 'kvb')), parts along dimension 0, may hold values from -3 to 3
- queries: bfloat16 [32, 8192], P(('groups', 'kvb'), 'tp'), parts along dimension 0, may hold values from -60 to 60
- new_kv: bfloat16 [32, 2048], P(('groups', 'kvb')), parts along dimension 0, may hold values from -6 to 6
- kv_cache: bfloat16 [2048, 16, 2048], P(('groups', 'kvb', 'tp')), parts along dimension 0, may hold values from -6 to 6
- lengths: int32 [32], P('groups'), parts along dimension 0, may hold values from 1 to 2048, as said below
- slot_seq: int32 [2048], P(('groups', 'kvb', 'tp')), parts along dimension 0, may hold values from 0 to 15, as said below
- slot_block: int32 [2048], P(('groups', 'kvb', 'tp')), parts along dimension 0, may hold values from 0 to 127, as said below
- block_counts: int32 [32], P(('groups', 'kvb', 'tp')), parts along dimension 0, may hold values from 16 to 64, as said below
- out_weight: bfloat16 [8192, 8192], P('tp'), may hold values from -0.5 to 0.5
- norm_gain: bfloat16 [8192], P('tp'), may hold values from 0.099609375 to 1.8984375
Outputs:
- stream: bfloat16 [32, 8192], P(('groups', 'kvb'), 'tp'), parts along dimension 0
- normed: bfloat16 [32, 8192], P(('groups', 'kvb'), 'tp'), parts along dimension 0
The draws below stay inside these ranges and needn't reach their ends.
There are 2 independent parts, one for each index of `groups`. The reference program is written for one: setup_inputs(seed, part) draws one part's arguments, and reference() takes and returns one part's arrays. A program takes and returns all parts, laid end to end along the dimension named above; an argument that names none is the same for every part. Nothing has to cross between parts.
Inputs may be any that keep to these rules, and one draw needn't show every extreme that they name: `block_counts`: slots below a device's count hold cache blocks, those at or beyond it none; at least one device's count is 64. `slot_seq`: each pair of a sequence s and a block b below ceil(lengths[s] / 16) sits in exactly one live slot of the group. `slot_block`: some sequence has exactly 128 blocks; none has more. `lengths`: some sequence has exactly 16 * (128) tokens.
All inputs are finite; a program needn't handle non-finite values.
Results may differ from the reference program's by a relative error of at most 0.006.
Values may be sent and summed in bfloat16 or wider, within the bound.
No kernel may reach another device: no remote copies, remote signals or barrier semaphores. Data moves between devices by JAX's collectives and lax.ppermute only.
A program may use at most 64 MiB of HBM per device.

```python
import jax
import jax.numpy as jnp
from jax import lax

D = 8192
QH = 64
KVH = 8
HD = 128
BLK = 16
POOL = 64
GROUP = 16
SEQS = 16
SLOTS = 1024


def layout(key):
    base = jax.random.fold_in(key, 7)
    streams = jax.random.split(base, 8)
    floor_count = max(POOL // 4, 1)
    divider = jax.random.randint(streams[0], (GROUP,), 1, 5)
    jitter = jax.random.randint(streams[1], (GROUP,), 0, 4)
    counts = jnp.maximum(POOL // divider - jitter, floor_count)
    fullest = jax.random.randint(streams[2], (), 0, GROUP)
    counts = jnp.where(jnp.arange(GROUP) == fullest, POOL, counts).astype(jnp.int32)
    used = (jnp.arange(POOL)[None, :] < counts[:, None]).reshape(-1)
    priority = jax.random.permutation(streams[3], SLOTS).astype(jnp.int32)
    priority = jnp.where(used, priority, priority + SLOTS)
    order = jnp.argsort(priority)
    rank = jnp.argsort(order).astype(jnp.int32)
    total_used = jnp.sum(counts).astype(jnp.int32)
    most_blocks = SLOTS // 8
    longest = jax.random.randint(streams[7], (), 0, SEQS)
    seq_ids = jnp.arange(SEQS, dtype=jnp.int32)
    is_long = seq_ids == longest
    remaining = total_used - most_blocks
    seq_weight = jnp.where(is_long, 0, jax.random.randint(streams[4], (SEQS,), 1, 64)).astype(jnp.int32)
    cumulative = jnp.cumsum(seq_weight).astype(jnp.int32)
    share_ends = (remaining - (SEQS - 1)) * cumulative // cumulative[-1]
    share_starts = jnp.concatenate([jnp.zeros((1,), jnp.int32), share_ends[:-1]])
    proposed = jnp.where(is_long, 0, share_ends - share_starts + 1)
    capped = jnp.minimum(proposed, most_blocks)
    deficit = remaining - jnp.sum(capped)
    headroom = jnp.where(is_long, 0, most_blocks - capped)
    before = jnp.cumsum(headroom) - headroom
    extra = jnp.clip(deficit - before, 0, headroom)
    blocks = jnp.where(is_long, most_blocks, capped + extra).astype(jnp.int32)
    ends = jnp.cumsum(blocks).astype(jnp.int32)
    starts = (ends - blocks).astype(jnp.int32)
    owner = jnp.sum((rank[:, None] >= ends[None, :]).astype(jnp.int32), axis=1)
    owner = jnp.minimum(owner, SEQS - 1)
    start_of = jnp.take(starts, owner)
    filler = jax.random.randint(streams[5], (SLOTS,), 0, SEQS)
    seq_table = jnp.where(used, owner, filler).astype(jnp.int32)
    block_table = jnp.where(used, rank - start_of, 0).astype(jnp.int32)
    dropped = jnp.where(is_long, 0, jax.random.randint(streams[6], (SEQS,), 0, BLK))
    seq_lengths = (BLK * blocks - dropped).astype(jnp.int32)
    return (seq_lengths, seq_table, block_table, counts)


def draw_lengths(key, part):
    return layout(key)[0]


def draw_slot_seq(key, part):
    return layout(key)[1]


def draw_slot_block(key, part):
    return layout(key)[2]


def draw_block_counts(key, part):
    return layout(key)[3]


def draw_kv_cache(key, part):
    cache = jax.random.normal(jax.random.fold_in(key, 29), (SLOTS, BLK, 2 * KVH * HD), jnp.float32)
    cache = jnp.clip(cache, -6.0, 6.0)
    return cache.astype(jnp.bfloat16)


def draw_queries(key, part):
    values = jax.random.normal(jax.random.fold_in(key, 41), (SEQS, QH * HD), jnp.float32)
    values = jnp.clip(values, -6.0, 6.0)
    return values.astype(jnp.bfloat16)


def levels(key, extent, shards, least, high):
    def one(dim, blocks):
        steps = jax.random.uniform(jax.random.fold_in(jax.random.fold_in(key, 6), dim), (blocks,), jnp.float32, least / len(shards), high / len(shards))
        return jnp.repeat(jnp.exp(steps), extent[dim] // blocks).reshape((-1,) + (1,) * (len(extent) - dim - 1))

    loudness = one(*shards[0])
    for cut in shards[1:]:
        loudness = loudness * one(*cut)
    return loudness


def noise(own_key, extent, scale, reach, shards=(), kind=jnp.bfloat16):
    drawn = jax.random.normal(own_key, extent, jnp.float32) * scale
    if len(shards) > 0:
        drawn = levels(own_key, extent, shards, -0.22, 0.18) * drawn
    return jnp.clip(drawn, min=-reach, max=reach).astype(kind)


def setup_inputs(seed: int = 0, part: int = 0) -> dict:
    streams_of = jax.random.split(jax.random.key(seed), 11)
    own_keys = jax.random.split(jax.random.fold_in(streams_of[10], part), 11)
    residual = noise(own_keys[0], (SEQS, D), 0.5, 3.0, ((0, 4),))
    queries = draw_queries(jax.random.fold_in(jax.random.fold_in(streams_of[10], part), 71), part)
    new_kv = noise(own_keys[2], (SEQS, 2 * KVH * HD), 1.0, 6.0, ((0, 4),))
    kv_cache = draw_kv_cache(jax.random.fold_in(jax.random.fold_in(streams_of[10], part), 71), part)
    lengths = draw_lengths(jax.random.fold_in(jax.random.fold_in(streams_of[10], part), 71), part)
    slot_seq = draw_slot_seq(jax.random.fold_in(jax.random.fold_in(streams_of[10], part), 71), part)
    slot_block = draw_slot_block(jax.random.fold_in(jax.random.fold_in(streams_of[10], part), 71), part)
    block_counts = draw_block_counts(jax.random.fold_in(jax.random.fold_in(streams_of[10], part), 71), part)
    out_weight = noise(streams_of[8], (QH * HD, D), HD ** -0.5, 0.5, ((0, 4),))
    norm_gain = jnp.clip(1.0 + 0.18 * jax.random.normal(streams_of[9], (D,), jnp.float32), 0.099609375, 1.8984375).astype(jnp.bfloat16)
    return dict(residual=residual, queries=queries, new_kv=new_kv, kv_cache=kv_cache, lengths=lengths, slot_seq=slot_seq, slot_block=slot_block, block_counts=block_counts, out_weight=out_weight, norm_gain=norm_gain)


NEGATIVE = -1e+30
EPSILON = 1e-06

def pool_partial(grouped, cache_pool, seq_pool, block_pool, live_count, lengths):
    pool_size = cache_pool.shape[0]
    key_rows = cache_pool[:, :, :KVH * HD].reshape(pool_size * BLK, KVH, HD).astype(jnp.float32)
    value_rows = cache_pool[:, :, KVH * HD:].reshape(pool_size * BLK, KVH, HD).astype(jnp.float32)
    token_seq = jnp.repeat(seq_pool, BLK)
    position = (block_pool[:, None] * BLK + jnp.arange(BLK, dtype=jnp.int32)[None, :]).reshape(-1)
    slot_live = jnp.repeat(jnp.arange(pool_size, dtype=jnp.int32) < live_count, BLK)
    member = token_seq[None, :] == jnp.arange(SEQS, dtype=jnp.int32)[:, None]
    length_of = lax.optimization_barrier(jnp.sum(jnp.where(member, lengths[:, None], 0), axis=0))
    live = member & (position < length_of)[None, :] & slot_live[None, :]
    mask = live[:, None, None, :]
    scores = jnp.einsum('sgqd,ngd->sgqn', grouped.astype(jnp.float32), key_rows) * HD ** (-0.5)
    peak_now = lax.optimization_barrier(jnp.max(jnp.where(mask, scores, NEGATIVE), axis=-1))
    weights = jnp.where(mask, jnp.exp(scores - peak_now[..., None]), 0.0)
    weight_sum = lax.optimization_barrier(jnp.sum(weights, axis=-1))
    rounded = weights.astype(jnp.bfloat16).astype(jnp.float32)
    partial_rows = jnp.einsum('sgqn,ngd->sgqd', rounded, value_rows)
    return (peak_now, weight_sum, partial_rows)

def reference(residual, queries, new_kv, kv_cache, lengths, slot_seq, slot_block, block_counts, out_weight, norm_gain):
    grouped = queries.reshape(SEQS, KVH, QH // KVH, HD)
    cache_groups = kv_cache.reshape(GROUP, POOL, BLK, 2 * KVH * HD)
    seq_groups = slot_seq.reshape(GROUP, POOL)
    block_groups = slot_block.reshape(GROUP, POOL)

    def one_pool(pieces):
        return pool_partial(grouped, pieces[0], pieces[1], pieces[2], pieces[3], lengths)
    peaks, sums, partials = lax.map(one_pool, (cache_groups, seq_groups, block_groups, block_counts))
    new_keys = new_kv[:, :KVH * HD].reshape(SEQS, KVH, HD).astype(jnp.float32)
    new_values = new_kv[:, KVH * HD:].reshape(SEQS, KVH, HD).astype(jnp.float32)
    fresh = jnp.einsum('sgqd,sgd->sgq', grouped.astype(jnp.float32), new_keys) * HD ** (-0.5)
    overall = jnp.maximum(lax.optimization_barrier(jnp.max(peaks, axis=0)), fresh)
    scaling = jnp.exp(peaks - overall[None])
    fresh_weight = jnp.exp(fresh - overall)
    denominator = lax.optimization_barrier(jnp.sum(scaling * sums, axis=0)) + fresh_weight
    numerator = lax.optimization_barrier(jnp.sum(scaling[..., None] * partials, axis=0)) + fresh_weight[..., None] * new_values[:, :, None, :]
    attended = (numerator / denominator[..., None]).reshape(SEQS, QH * HD).astype(jnp.bfloat16)
    projected = jnp.dot(attended, out_weight, preferred_element_type=jnp.float32)
    stream = (residual.astype(jnp.float32) + projected).astype(jnp.bfloat16)
    stream_wide = lax.optimization_barrier(stream).astype(jnp.float32)
    mean_square = lax.optimization_barrier(jnp.mean(stream_wide * stream_wide, axis=1, keepdims=True))
    normed = (stream_wide * lax.rsqrt(mean_square + EPSILON) * norm_gain.astype(jnp.float32)).astype(jnp.bfloat16)
    return (stream, normed)
```

```python
import jax
import jax.numpy as jnp
from jax import lax
from jax.experimental import pallas as pl
from jax.experimental.pallas import tpu as pltpu
from jax.sharding import PartitionSpec as P

QH = 64
KVH = 8
HD = 128
BLK = 16

MASKED = -1e30
FLOOR = -1e20
EPSILON = 1e-06
UNIT = HD ** (-0.5) * 1.4426950408889634
STATS = 128


def attend_body(
    lengths, count, slot_seq, slot_block, wide, cache, out, stacked, *, kvb_count, tp_count
):
    slots = cache.shape[0]
    tokens = slots * BLK
    seq_rep = wide.shape[1]
    seq_total = kvb_count * seq_rep
    local_heads = wide.shape[2] // HD
    group_size = QH // KVH
    seq = slot_seq[...]
    length_of = jnp.zeros_like(seq)
    for s in range(seq_total):
        length_of = jnp.where(seq == s, lengths[s], length_of)
    slot_ids = lax.broadcasted_iota(jnp.int32, seq.shape, 1)
    remaining = jnp.clip(length_of - slot_block[...] * BLK, 0, BLK)
    remaining = jnp.where(slot_ids < count[0], remaining, 0)
    row = lax.broadcasted_iota(jnp.int32, (8, slots), 0)
    codes = jnp.where(row == 0, seq, jnp.where(row == 1, remaining, 0))
    spread = (
        lax.broadcasted_iota(jnp.int32, (slots, tokens), 1) // BLK
        == lax.broadcasted_iota(jnp.int32, (slots, tokens), 0)
    )
    per_token = jnp.dot(
        codes.astype(jnp.float32).astype(jnp.bfloat16),
        jnp.where(spread, 1.0, 0.0).astype(jnp.bfloat16),
        preferred_element_type=jnp.float32,
    )
    seq_ids = lax.broadcasted_iota(jnp.int32, (seq_total, tokens), 0).astype(jnp.float32)
    offsets = (lax.broadcasted_iota(jnp.int32, (seq_total, tokens), 1) % BLK).astype(jnp.float32)
    live = (per_token[0:1] == seq_ids) & (offsets < per_token[1:2])
    bias = jnp.where(live, 0.0, MASKED)

    for k in range(kvb_count):
        for t in range(tp_count):
            stacked[t, k * seq_rep : (k + 1) * seq_rep, :] = wide[k * tp_count + t].astype(
                jnp.float32
            )

    lane = lax.broadcasted_iota(jnp.int32, (seq_total, STATS), 1)
    stats = [jnp.zeros((seq_total, STATS), jnp.float32) for _ in range(tp_count)]
    for g in range(KVH):
        heads = [divmod(g * group_size + j, local_heads) for j in range(group_size)]
        rows = jnp.concatenate(
            [stacked[t, :, h * HD : (h + 1) * HD] for t, h in heads], axis=0
        ).astype(jnp.bfloat16)
        keys = cache[:, :, g * HD : (g + 1) * HD].reshape(tokens, HD)
        values = cache[:, :, (KVH + g) * HD : (KVH + g + 1) * HD].reshape(tokens, HD)
        scores = lax.dot_general(
            rows, keys, (((1,), (1,)), ((), ())), preferred_element_type=jnp.float32
        )
        scores = scores.reshape(group_size, seq_total, tokens) * UNIT + bias[None]
        peaks = jnp.maximum(jnp.max(scores, axis=2, keepdims=True), FLOOR)
        peaks = peaks.astype(jnp.bfloat16).astype(jnp.float32)
        weights = jnp.exp2(scores - peaks)
        sums = jnp.sum(weights, axis=2, keepdims=True)
        partial = jnp.dot(
            weights.astype(jnp.bfloat16).reshape(group_size * seq_total, tokens),
            values,
            preferred_element_type=jnp.float32,
        )
        high = sums.astype(jnp.bfloat16).astype(jnp.float32)
        low = sums - high
        for j, (t, h) in enumerate(heads):
            mine = partial[j * seq_total : (j + 1) * seq_total]
            for k in range(kvb_count):
                out[k * tp_count + t, :, h * HD : (h + 1) * HD] = mine[
                    k * seq_rep : (k + 1) * seq_rep
                ].astype(jnp.bfloat16)
            for part, value in enumerate((peaks, high, low)):
                stats[t] = jnp.where(lane == part * local_heads + h, value[j], stats[t])
    for t in range(tp_count):
        for k in range(kvb_count):
            out[k * tp_count + t, :, local_heads * HD :] = stats[t][
                k * seq_rep : (k + 1) * seq_rep
            ].astype(jnp.bfloat16)


def project_body(tp_index, got, queries, new_kv, weight, out, *, local_heads):
    sources, seq_rep, _ = got.shape
    group_size = QH // KVH
    width = local_heads * HD
    kv_local = max(1, local_heads // group_size)
    kv_first = tp_index[0] * local_heads // group_size
    lane = lax.broadcasted_iota(jnp.int32, (seq_rep, local_heads), 1)
    fresh = jnp.zeros((seq_rep, local_heads), jnp.float32)
    fresh_values = []
    for v in range(kv_local):
        at = pl.multiple_of((kv_first + v) * HD, HD)
        key = new_kv[:, pl.ds(at, HD)].astype(jnp.float32)
        at = pl.multiple_of((KVH + kv_first + v) * HD, HD)
        fresh_values.append(new_kv[:, pl.ds(at, HD)].astype(jnp.float32))
        for h in range(v * local_heads // kv_local, (v + 1) * local_heads // kv_local):
            query = queries[:, h * HD : (h + 1) * HD].astype(jnp.float32)
            score = jnp.sum(query * key, axis=1, keepdims=True)
            fresh = jnp.where(lane == h, score, fresh)
    fresh = fresh * UNIT
    peaks, sums = [], []
    overall = fresh
    for d in range(sources):
        stats = got[d, :, width:].astype(jnp.float32)
        peaks.append(stats[:, :local_heads])
        sums.append(
            stats[:, local_heads : 2 * local_heads] + stats[:, 2 * local_heads : 3 * local_heads]
        )
        overall = jnp.maximum(overall, peaks[-1])
    scaling = [jnp.exp2(p - overall) for p in peaks]
    fresh_weight = jnp.exp2(fresh - overall)
    denominator = fresh_weight
    for d in range(sources):
        denominator = denominator + scaling[d] * sums[d]
    inverse = 1.0 / denominator
    scaling = [s * inverse for s in scaling]
    fresh_weight = fresh_weight * inverse
    attended = []
    for h in range(local_heads):
        total = fresh_weight[:, h : h + 1] * fresh_values[h * kv_local // local_heads]
        for d in range(sources):
            total = total + scaling[d][:, h : h + 1] * got[d, :, h * HD : (h + 1) * HD].astype(
                jnp.float32
            )
        attended.append(total.astype(jnp.bfloat16))
    attended = jnp.concatenate(attended, axis=1)
    step = min(1024, weight.shape[1])
    for n in range(weight.shape[1] // step):
        out[:, n * step : (n + 1) * step] = jnp.dot(
            attended, weight[:, n * step : (n + 1) * step], preferred_element_type=jnp.float32
        ).astype(out.dtype)


def finish_body(tp_index, pieces, residual, gain, stream_out, normed_out):
    full = residual[...].astype(jnp.float32)
    width = full.shape[1]
    total = pieces[0].astype(jnp.float32)
    for t in range(1, pieces.shape[0]):
        total = total + pieces[t].astype(jnp.float32)
    full = (full + total).astype(jnp.bfloat16).astype(jnp.float32)
    mean_square = jnp.sum(full * full, axis=1, keepdims=True) / width
    inverse = lax.rsqrt(mean_square + EPSILON)
    own = stream_out.shape[1]
    at = pl.multiple_of(tp_index[0] * own, own)
    mine = residual[:, pl.ds(at, own)].astype(jnp.float32)
    total = pieces[0, :, pl.ds(at, own)].astype(jnp.float32)
    for t in range(1, pieces.shape[0]):
        total = total + pieces[t, :, pl.ds(at, own)].astype(jnp.float32)
    stream = (mine + total).astype(jnp.bfloat16)
    stream_out[...] = stream
    normed_out[...] = (stream.astype(jnp.float32) * inverse * gain[...].astype(jnp.float32)).astype(
        jnp.bfloat16
    )


def vmem():
    return pl.BlockSpec(memory_space=pltpu.VMEM)


def smem():
    return pl.BlockSpec(memory_space=pltpu.SMEM)


def on_device(
    residual,
    queries,
    new_kv,
    kv_cache,
    lengths,
    slot_seq,
    slot_block,
    block_counts,
    out_weight,
    norm_gain,
):
    tp_count = lax.axis_size("tp")
    kvb_count = lax.axis_size("kvb")
    device_total = kvb_count * tp_count
    tp_index = lax.axis_index("tp").reshape(1)
    seq_rep, own_width = queries.shape
    local_heads = own_width // HD
    seq_total = kvb_count * seq_rep
    wide = lax.all_to_all(
        jnp.broadcast_to(queries[None], (device_total, seq_rep, own_width)),
        ("kvb", "tp"),
        split_axis=0,
        concat_axis=0,
        tiled=True,
    )
    sent = pl.pallas_call(
        lambda *refs: attend_body(*refs, kvb_count=kvb_count, tp_count=tp_count),
        out_shape=jax.ShapeDtypeStruct((device_total, seq_rep, own_width + STATS), jnp.bfloat16),
        in_specs=[smem(), smem(), vmem(), vmem(), vmem(), vmem()],
        out_specs=vmem(),
        scratch_shapes=[pltpu.VMEM((tp_count, seq_total, own_width), jnp.float32)],
        compiler_params=pltpu.CompilerParams(vmem_limit_bytes=16 << 20),
        name="attend",
    )(lengths, block_counts, slot_seq[None], slot_block[None], wide, kv_cache)
    got = lax.all_to_all(sent, ("kvb", "tp"), split_axis=0, concat_axis=0, tiled=True)
    projected = pl.pallas_call(
        lambda *refs: project_body(*refs, local_heads=local_heads),
        out_shape=jax.ShapeDtypeStruct((seq_rep, out_weight.shape[1]), jnp.bfloat16),
        in_specs=[smem(), vmem(), vmem(), vmem(), vmem()],
        out_specs=vmem(),
        compiler_params=pltpu.CompilerParams(vmem_limit_bytes=48 << 20),
        name="project",
    )(tp_index, got, queries, new_kv, out_weight)
    pieces = lax.all_gather(projected, "tp", axis=0, tiled=False)
    own = jax.ShapeDtypeStruct((seq_rep, norm_gain.shape[0]), jnp.bfloat16)
    return pl.pallas_call(
        finish_body,
        out_shape=(own, own),
        in_specs=[smem(), vmem(), vmem(), vmem()],
        out_specs=(vmem(), vmem()),
        compiler_params=pltpu.CompilerParams(vmem_limit_bytes=8 << 20),
        name="finish",
    )(tp_index, pieces, residual, norm_gain[None])


def solution(mesh):
    placed = (
        P(("groups", "kvb"), None),
        P(("groups", "kvb"), "tp"),
        P(("groups", "kvb"), None),
        P(("groups", "kvb", "tp"), None, None),
        P("groups"),
        P(("groups", "kvb", "tp")),
        P(("groups", "kvb", "tp")),
        P(("groups", "kvb", "tp")),
        P("tp", None),
        P("tp"),
    )
    return jax.shard_map(
        on_device,
        mesh=mesh,
        in_specs=placed,
        out_specs=(P(("groups", "kvb"), "tp"), P(("groups", "kvb"), "tp")),
        check_vma=False,
    )
```

```python
import jax
import jax.numpy as jnp
from jax import lax
from jax.experimental import pallas as pl
from jax.experimental.pallas import tpu as pltpu
from jax.sharding import PartitionSpec as P

QH = 64
KVH = 8
HD = 128
BLK = 16

MASKED = -1e30
FLOOR = -1e20
EPSILON = 1e-06
UNIT = HD ** (-0.5) * 1.4426950408889634
STATS = 128
COVER = 20_000_000_000


def prepare_body(
    lengths, count, slot_seq, slot_block, queries, new_kv, bias, fresh_out, value_out, own_out
):
    seq_total, tokens = bias.shape
    slots = tokens // BLK
    seq_rep, own_width = queries.shape
    local_heads = own_width // HD
    group_size = QH // KVH
    kvb_count = seq_total // seq_rep
    seq = slot_seq[...]
    length_of = jnp.zeros_like(seq)
    for s in range(seq_total):
        length_of = jnp.where(seq == s, lengths[s], length_of)
    slot_ids = lax.broadcasted_iota(jnp.int32, seq.shape, 1)
    remaining = jnp.clip(length_of - slot_block[...] * BLK, 0, BLK)
    remaining = jnp.where(slot_ids < count[0], remaining, 0)
    row = lax.broadcasted_iota(jnp.int32, (8, slots), 0)
    codes = jnp.where(row == 0, seq, jnp.where(row == 1, remaining, 0))
    spread = (
        lax.broadcasted_iota(jnp.int32, (slots, tokens), 1) // BLK
        == lax.broadcasted_iota(jnp.int32, (slots, tokens), 0)
    )
    per_token = jnp.dot(
        codes.astype(jnp.float32).astype(jnp.bfloat16),
        jnp.where(spread, 1.0, 0.0).astype(jnp.bfloat16),
        preferred_element_type=jnp.float32,
    )
    row = lax.broadcasted_iota(jnp.int32, (seq_total, tokens), 0)
    replica = lax.axis_index("kvb") - row // seq_rep
    replica = jnp.where(replica < 0, replica + kvb_count, replica)
    seq_ids = (replica * seq_rep + row % seq_rep).astype(jnp.float32)
    offsets = (lax.broadcasted_iota(jnp.int32, (seq_total, tokens), 1) % BLK).astype(jnp.float32)
    live = (per_token[0:1] == seq_ids) & (offsets < per_token[1:2])
    bias[...] = jnp.where(live, 0.0, MASKED)

    own_out[...] = queries[...]
    kv_local = max(1, local_heads // group_size)
    kv_first = lax.axis_index("tp") * local_heads // group_size
    lane = lax.broadcasted_iota(jnp.int32, (seq_rep, STATS), 1)
    fresh = jnp.zeros((seq_rep, STATS), jnp.float32)
    for v in range(kv_local):
        at = pl.multiple_of((kv_first + v) * HD, HD)
        key = new_kv[:, pl.ds(at, HD)].astype(jnp.float32)
        at = pl.multiple_of((KVH + kv_first + v) * HD, HD)
        value_out[:, v * HD : (v + 1) * HD] = new_kv[:, pl.ds(at, HD)].astype(jnp.float32)
        for h in range(v * local_heads // kv_local, (v + 1) * local_heads // kv_local):
            query = queries[:, h * HD : (h + 1) * HD].astype(jnp.float32)
            score = jnp.sum(query * key, axis=1, keepdims=True)
            fresh = jnp.where(lane == h, score, fresh)
    fresh_out[...] = fresh * UNIT


def attend_body(bias_ref, wide, cache, out, stacked):
    tp_count, kvb_count, seq_rep, own_width = wide.shape
    tokens = cache.shape[0] * BLK
    seq_total = kvb_count * seq_rep
    local_heads = own_width // HD
    group_size = QH // KVH
    bias = bias_ref[...]
    me = lax.axis_index("kvb")
    places = []
    for r in range(kvb_count):
        k = jnp.where(me < r, me - r + kvb_count, me - r)
        places.append(k * tp_count)
        for t in range(tp_count):
            stacked[t, r * seq_rep : (r + 1) * seq_rep, :] = wide[t, r].astype(jnp.float32)

    lane = lax.broadcasted_iota(jnp.int32, (seq_total, STATS), 1)
    stats = [jnp.zeros((seq_total, STATS), jnp.float32) for _ in range(tp_count)]
    for g in range(KVH):
        heads = [divmod(g * group_size + j, local_heads) for j in range(group_size)]
        rows = jnp.concatenate(
            [stacked[t, :, h * HD : (h + 1) * HD] for t, h in heads], axis=0
        ).astype(jnp.bfloat16)
        keys = cache[:, :, g * HD : (g + 1) * HD].reshape(tokens, HD)
        values = cache[:, :, (KVH + g) * HD : (KVH + g + 1) * HD].reshape(tokens, HD)
        scores = lax.dot_general(
            rows, keys, (((1,), (1,)), ((), ())), preferred_element_type=jnp.float32
        )
        scores = scores.reshape(group_size, seq_total, tokens) * UNIT + bias[None]
        peaks = jnp.maximum(jnp.max(scores, axis=2, keepdims=True), FLOOR)
        peaks = peaks.astype(jnp.bfloat16).astype(jnp.float32)
        weights = jnp.exp2(scores - peaks)
        sums = jnp.sum(weights, axis=2, keepdims=True)
        partial = jnp.dot(
            weights.astype(jnp.bfloat16).reshape(group_size * seq_total, tokens),
            values,
            preferred_element_type=jnp.float32,
        )
        high = sums.astype(jnp.bfloat16).astype(jnp.float32)
        low = sums - high
        for j, (t, h) in enumerate(heads):
            mine = partial[j * seq_total : (j + 1) * seq_total]
            for r in range(kvb_count):
                out[places[r] + t, :, h * HD : (h + 1) * HD] = mine[
                    r * seq_rep : (r + 1) * seq_rep
                ].astype(jnp.bfloat16)
            for part, value in enumerate((peaks, high, low)):
                stats[t] = jnp.where(lane == part * local_heads + h, value[j], stats[t])
    for t in range(tp_count):
        for r in range(kvb_count):
            out[places[r] + t, :, local_heads * HD :] = stats[t][
                r * seq_rep : (r + 1) * seq_rep
            ].astype(jnp.bfloat16)


def project_body(got, fresh_ref, value_ref, weight, out):
    sources, seq_rep, width = got.shape
    width = width - STATS
    local_heads = width // HD
    kv_local = value_ref.shape[1] // HD
    fresh = fresh_ref[:, :local_heads]
    peaks, sums = [], []
    overall = fresh
    for d in range(sources):
        stats = got[d, :, width:].astype(jnp.float32)
        peaks.append(stats[:, :local_heads])
        sums.append(
            stats[:, local_heads : 2 * local_heads] + stats[:, 2 * local_heads : 3 * local_heads]
        )
        overall = jnp.maximum(overall, peaks[-1])
    scaling = [jnp.exp2(p - overall) for p in peaks]
    fresh_weight = jnp.exp2(fresh - overall)
    denominator = fresh_weight
    for d in range(sources):
        denominator = denominator + scaling[d] * sums[d]
    inverse = 1.0 / denominator
    scaling = [s * inverse for s in scaling]
    fresh_weight = fresh_weight * inverse
    attended = []
    for h in range(local_heads):
        v = h * kv_local // local_heads
        total = fresh_weight[:, h : h + 1] * value_ref[:, v * HD : (v + 1) * HD]
        for d in range(sources):
            total = total + scaling[d][:, h : h + 1] * got[d, :, h * HD : (h + 1) * HD].astype(
                jnp.float32
            )
        attended.append(total.astype(jnp.bfloat16))
    attended = jnp.concatenate(attended, axis=1)
    step = min(1024, weight.shape[1])
    for n in range(weight.shape[1] // step):
        out[:, n * step : (n + 1) * step] = jnp.dot(
            attended, weight[:, n * step : (n + 1) * step], preferred_element_type=jnp.float32
        ).astype(out.dtype)


def finish_body(pieces, residual, gain, stream_out, normed_out):
    full = residual[...].astype(jnp.float32)
    width = full.shape[1]
    total = pieces[0].astype(jnp.float32)
    for t in range(1, pieces.shape[0]):
        total = total + pieces[t].astype(jnp.float32)
    full = (full + total).astype(jnp.bfloat16).astype(jnp.float32)
    mean_square = jnp.sum(full * full, axis=1, keepdims=True) / width
    inverse = lax.rsqrt(mean_square + EPSILON)
    own = stream_out.shape[1]
    at = pl.multiple_of(lax.axis_index("tp") * own, own)
    mine = residual[:, pl.ds(at, own)].astype(jnp.float32)
    total = pieces[0, :, pl.ds(at, own)].astype(jnp.float32)
    for t in range(1, pieces.shape[0]):
        total = total + pieces[t, :, pl.ds(at, own)].astype(jnp.float32)
    stream = (mine + total).astype(jnp.bfloat16)
    stream_out[...] = stream
    normed_out[...] = (stream.astype(jnp.float32) * inverse * gain[...].astype(jnp.float32)).astype(
        jnp.bfloat16
    )


def vmem():
    return pl.BlockSpec(memory_space=pltpu.VMEM)


def resident(array):
    return pltpu.with_memory_space_constraint(array, pltpu.VMEM)


def smem():
    return pl.BlockSpec(memory_space=pltpu.SMEM)


def on_device(
    residual,
    queries,
    new_kv,
    kv_cache,
    lengths,
    slot_seq,
    slot_block,
    block_counts,
    out_weight,
    norm_gain,
):
    tp_count = lax.axis_size("tp")
    kvb_count = lax.axis_size("kvb")
    device_total = kvb_count * tp_count
    seq_rep, own_width = queries.shape
    seq_total = kvb_count * seq_rep
    tokens = kv_cache.shape[0] * BLK
    kv_local = max(1, own_width // HD * KVH // QH)
    arrived = [
        lax.ppermute(queries, "kvb", [(k, (k + r) % kvb_count) for k in range(kvb_count)])
        for r in range(1, kvb_count)
    ]
    bias, fresh, fresh_values, own_queries = pl.pallas_call(
        prepare_body,
        out_shape=(
            jax.ShapeDtypeStruct((seq_total, tokens), jnp.float32),
            jax.ShapeDtypeStruct((seq_rep, STATS), jnp.float32),
            jax.ShapeDtypeStruct((seq_rep, kv_local * HD), jnp.float32),
            jax.ShapeDtypeStruct((seq_rep, own_width), jnp.bfloat16),
        ),
        in_specs=[smem(), smem(), vmem(), vmem(), vmem(), vmem()],
        out_specs=(vmem(), vmem(), vmem(), vmem()),
        compiler_params=pltpu.CompilerParams(vmem_limit_bytes=4 << 20),
        cost_estimate=pl.CostEstimate(flops=COVER, transcendentals=0, bytes_accessed=1 << 20),
        name="prepare",
    )(lengths, block_counts, slot_seq[None], slot_block[None], queries, new_kv)
    wide = lax.all_gather(jnp.stack([own_queries] + arrived), "tp", axis=0, tiled=False)
    sent = pl.pallas_call(
        attend_body,
        out_shape=jax.ShapeDtypeStruct((device_total, seq_rep, own_width + STATS), jnp.bfloat16),
        in_specs=[vmem(), vmem(), vmem()],
        out_specs=vmem(),
        scratch_shapes=[pltpu.VMEM((tp_count, seq_total, own_width), jnp.float32)],
        compiler_params=pltpu.CompilerParams(vmem_limit_bytes=10 << 20),
        cost_estimate=pl.CostEstimate(flops=COVER, transcendentals=0, bytes_accessed=1 << 20),
        name="attend",
    )(bias, wide, resident(kv_cache))
    got = lax.all_to_all(sent, ("kvb", "tp"), split_axis=0, concat_axis=0, tiled=True)
    projected = pl.pallas_call(
        project_body,
        out_shape=jax.ShapeDtypeStruct((seq_rep, out_weight.shape[1]), jnp.bfloat16),
        in_specs=[vmem(), vmem(), vmem(), vmem()],
        out_specs=vmem(),
        compiler_params=pltpu.CompilerParams(vmem_limit_bytes=4 << 20),
        name="project",
    )(got, fresh, fresh_values, resident(out_weight))
    pieces = lax.all_gather(projected, "tp", axis=0, tiled=False)
    own = jax.ShapeDtypeStruct((seq_rep, norm_gain.shape[0]), jnp.bfloat16)
    return pl.pallas_call(
        finish_body,
        out_shape=(own, own),
        in_specs=[vmem(), vmem(), vmem()],
        out_specs=(vmem(), vmem()),
        compiler_params=pltpu.CompilerParams(vmem_limit_bytes=4 << 20),
        name="finish",
    )(pieces, residual, norm_gain[None])


def solution(mesh):
    placed = (
        P(("groups", "kvb"), None),
        P(("groups", "kvb"), "tp"),
        P(("groups", "kvb"), None),
        P(("groups", "kvb", "tp"), None, None),
        P("groups"),
        P(("groups", "kvb", "tp")),
        P(("groups", "kvb", "tp")),
        P(("groups", "kvb", "tp")),
        P("tp", None),
        P("tp"),
    )
    return jax.shard_map(
        on_device,
        mesh=mesh,
        in_specs=placed,
        out_specs=(P(("groups", "kvb"), "tp"), P(("groups", "kvb"), "tp")),
        check_vma=False,
    )
```

```python
import jax
import jax.numpy as jnp
from jax import lax
from jax.experimental import pallas as pl
from jax.experimental.pallas import tpu as pltpu
from jax.sharding import PartitionSpec as P

QH = 64
KVH = 8
HD = 128
BLK = 16

MASKED = -1e30
FLOOR = -1e20
EPSILON = 1e-06
UNIT = HD ** (-0.5) * 1.4426950408889634
STATS = 128
COVER = 20_000_000_000


def prepare_body(*refs):
    count, inputs, (bias, fresh_out, value_out, own_out) = refs[0], refs[1:6], refs[6:10]
    held, arrived = refs[10:15], refs[15]
    copies = [
        pltpu.make_async_copy(source, target, arrived.at[n])
        for n, (source, target) in enumerate(zip(inputs, held))
    ]
    for copy in copies:
        copy.start()
    for copy in copies:
        copy.wait()
    lengths, slot_seq, slot_block, queries, new_kv = held
    seq_total, tokens = bias.shape
    slots = tokens // BLK
    seq_rep, own_width = queries.shape
    local_heads = own_width // HD
    group_size = QH // KVH
    kvb_count = seq_total // seq_rep
    seq = slot_seq[...]
    length_of = jnp.zeros_like(seq)
    for s in range(seq_total):
        length_of = jnp.where(seq == s, lengths[s], length_of)
    slot_ids = lax.broadcasted_iota(jnp.int32, seq.shape, 1)
    remaining = jnp.clip(length_of - slot_block[...] * BLK, 0, BLK)
    remaining = jnp.where(slot_ids < count[0], remaining, 0)
    row = lax.broadcasted_iota(jnp.int32, (8, slots), 0)
    codes = jnp.where(row == 0, seq, jnp.where(row == 1, remaining, 0))
    spread = (
        lax.broadcasted_iota(jnp.int32, (slots, tokens), 1) // BLK
        == lax.broadcasted_iota(jnp.int32, (slots, tokens), 0)
    )
    per_token = jnp.dot(
        codes.astype(jnp.float32).astype(jnp.bfloat16),
        jnp.where(spread, 1.0, 0.0).astype(jnp.bfloat16),
        preferred_element_type=jnp.float32,
    )
    row = lax.broadcasted_iota(jnp.int32, (seq_total, tokens), 0)
    replica = lax.axis_index("kvb") - row // seq_rep
    replica = jnp.where(replica < 0, replica + kvb_count, replica)
    seq_ids = (replica * seq_rep + row % seq_rep).astype(jnp.float32)
    offsets = (lax.broadcasted_iota(jnp.int32, (seq_total, tokens), 1) % BLK).astype(jnp.float32)
    live = (per_token[0:1] == seq_ids) & (offsets < per_token[1:2])
    bias[...] = jnp.where(live, 0.0, MASKED)

    own_out[...] = queries[...]
    kv_local = max(1, local_heads // group_size)
    kv_first = lax.axis_index("tp") * local_heads // group_size
    lane = lax.broadcasted_iota(jnp.int32, (seq_rep, STATS), 1)
    fresh = jnp.zeros((seq_rep, STATS), jnp.float32)
    for v in range(kv_local):
        at = pl.multiple_of((kv_first + v) * HD, HD)
        key = new_kv[:, pl.ds(at, HD)].astype(jnp.float32)
        at = pl.multiple_of((KVH + kv_first + v) * HD, HD)
        value_out[:, v * HD : (v + 1) * HD] = new_kv[:, pl.ds(at, HD)].astype(jnp.float32)
        for h in range(v * local_heads // kv_local, (v + 1) * local_heads // kv_local):
            query = queries[:, h * HD : (h + 1) * HD].astype(jnp.float32)
            score = jnp.sum(query * key, axis=1, keepdims=True)
            fresh = jnp.where(lane == h, score, fresh)
    fresh_out[...] = fresh * UNIT


def attend_body(bias_ref, wide, cache, *refs):
    outs, stacked = refs[:-1], refs[-1]
    tp_count, kvb_count, seq_rep, own_width = wide.shape
    tokens = cache.shape[0] * BLK
    seq_total = kvb_count * seq_rep
    local_heads = own_width // HD
    group_size = QH // KVH
    kv_local = max(1, local_heads // group_size)
    per_kv = local_heads // kv_local
    bias = bias_ref[...]
    for r in range(kvb_count):
        for t in range(tp_count):
            stacked[t, r * seq_rep : (r + 1) * seq_rep, :] = wide[t, r].astype(jnp.float32)

    me = lax.axis_index("tp")
    lane = lax.broadcasted_iota(jnp.int32, (seq_total, STATS), 1)
    for d, out in enumerate(outs):
        t = jnp.where(me + d < tp_count, me + d, me + d - tp_count)
        stats = jnp.zeros((seq_total, STATS), jnp.float32)
        for v in range(kv_local):
            heads = range(v * per_kv, (v + 1) * per_kv)
            rows = jnp.concatenate(
                [stacked[t, :, h * HD : (h + 1) * HD] for h in heads], axis=0
            ).astype(jnp.bfloat16)
            g = t * local_heads // group_size + v
            at = pl.multiple_of(g * HD, HD)
            keys = cache[:, :, pl.ds(at, HD)].reshape(tokens, HD)
            at = pl.multiple_of((KVH + g) * HD, HD)
            values = cache[:, :, pl.ds(at, HD)].reshape(tokens, HD)
            scores = lax.dot_general(
                rows, keys, (((1,), (1,)), ((), ())), preferred_element_type=jnp.float32
            )
            scores = scores.reshape(per_kv, seq_total, tokens) * UNIT + bias[None]
            peaks = jnp.maximum(jnp.max(scores, axis=2, keepdims=True), FLOOR)
            peaks = peaks.astype(jnp.bfloat16).astype(jnp.float32)
            weights = jnp.exp2(scores - peaks)
            sums = jnp.sum(weights, axis=2, keepdims=True)
            partial = jnp.dot(
                weights.astype(jnp.bfloat16).reshape(per_kv * seq_total, tokens),
                values,
                preferred_element_type=jnp.float32,
            )
            high = sums.astype(jnp.bfloat16).astype(jnp.float32)
            low = sums - high
            for j, h in enumerate(heads):
                out[:, h * HD : (h + 1) * HD] = partial[
                    j * seq_total : (j + 1) * seq_total
                ].astype(jnp.bfloat16)
                for part, value in enumerate((peaks, high, low)):
                    stats = jnp.where(lane == part * local_heads + h, value[j], stats)
        out[:, local_heads * HD :] = stats.astype(jnp.bfloat16)


def unpack(ref, local_heads):
    stats = ref[:, local_heads * HD :].astype(jnp.float32)
    sums = stats[:, local_heads : 2 * local_heads] + stats[:, 2 * local_heads : 3 * local_heads]
    return stats[:, :local_heads], sums


def merge_body(*refs, sources):
    parts, outs = refs[:sources], refs[sources:]
    seq_total, width = parts[0].shape
    seq_rep = outs[0].shape[0]
    local_heads = (width - STATS) // HD
    pairs = [unpack(part, local_heads) for part in parts]
    peak = pairs[0][0]
    for other, _ in pairs[1:]:
        peak = jnp.maximum(peak, other)
    scaling = [jnp.exp2(p - peak) for p, _ in pairs]
    total = sum(s * c for s, (_, c) in zip(scaling, pairs))
    high = total.astype(jnp.bfloat16).astype(jnp.float32)
    pad = jnp.zeros((seq_total, STATS - 3 * local_heads), jnp.float32)
    stats = jnp.concatenate([peak, high, total - high, pad], axis=1)
    blocks = [
        sum(
            s[:, h : h + 1] * part[:, h * HD : (h + 1) * HD].astype(jnp.float32)
            for s, part in zip(scaling, parts)
        )
        for h in range(local_heads)
    ]
    for h, block in enumerate(blocks + [stats]):
        for r, out in enumerate(outs):
            out[:, h * HD : (h + 1) * HD] = block[r * seq_rep : (r + 1) * seq_rep].astype(
                jnp.bfloat16
            )


def project_body(*refs, sources):
    parts = refs[:sources]
    fresh_ref, value_ref, weight, out = refs[sources:]
    local_heads = (parts[0].shape[1] - STATS) // HD
    kv_local = value_ref.shape[1] // HD
    pairs = [unpack(part, local_heads) for part in parts]
    fresh = fresh_ref[:, :local_heads]
    overall = fresh
    for peak, _ in pairs:
        overall = jnp.maximum(overall, peak)
    scaling = [jnp.exp2(peak - overall) for peak, _ in pairs]
    fresh_weight = jnp.exp2(fresh - overall)
    inverse = 1.0 / (fresh_weight + sum(s * c for s, (_, c) in zip(scaling, pairs)))
    scaling = [s * inverse for s in scaling]
    fresh_weight = fresh_weight * inverse
    attended = []
    for h in range(local_heads):
        v = h * kv_local // local_heads
        total = fresh_weight[:, h : h + 1] * value_ref[:, v * HD : (v + 1) * HD]
        for s, part in zip(scaling, parts):
            total = total + s[:, h : h + 1] * part[:, h * HD : (h + 1) * HD].astype(jnp.float32)
        attended.append(total.astype(jnp.bfloat16))
    attended = jnp.concatenate(attended, axis=1)
    step = min(1024, weight.shape[1])
    for at in range(0, weight.shape[1], step):
        out[:, at : at + step] = jnp.dot(
            attended, weight[:, at : at + step], preferred_element_type=jnp.float32
        ).astype(out.dtype)


def finish_body(pieces, residual, gain, stream_out, normed_out):
    full = residual[...].astype(jnp.float32)
    width = full.shape[1]
    total = pieces[0].astype(jnp.float32)
    for t in range(1, pieces.shape[0]):
        total = total + pieces[t].astype(jnp.float32)
    full = (full + total).astype(jnp.bfloat16).astype(jnp.float32)
    mean_square = jnp.sum(full * full, axis=1, keepdims=True) / width
    inverse = lax.rsqrt(mean_square + EPSILON)
    own = stream_out.shape[1]
    at = pl.multiple_of(lax.axis_index("tp") * own, own)
    mine = residual[:, pl.ds(at, own)].astype(jnp.float32)
    total = pieces[0, :, pl.ds(at, own)].astype(jnp.float32)
    for t in range(1, pieces.shape[0]):
        total = total + pieces[t, :, pl.ds(at, own)].astype(jnp.float32)
    stream = (mine + total).astype(jnp.bfloat16)
    stream_out[...] = stream
    normed_out[...] = (stream.astype(jnp.float32) * inverse * gain[...].astype(jnp.float32)).astype(
        jnp.bfloat16
    )


def vmem():
    return pl.BlockSpec(memory_space=pltpu.VMEM)


def resident(array):
    return pltpu.with_memory_space_constraint(array, pltpu.VMEM)


def hbm():
    return pl.BlockSpec(memory_space=pltpu.HBM)


def on_device(
    residual,
    queries,
    new_kv,
    kv_cache,
    lengths,
    slot_seq,
    slot_block,
    block_counts,
    out_weight,
    norm_gain,
):
    tp_count = lax.axis_size("tp")
    kvb_count = lax.axis_size("kvb")
    seq_rep, own_width = queries.shape
    seq_total = kvb_count * seq_rep
    tokens = kv_cache.shape[0] * BLK
    kv_local = max(1, own_width // HD * KVH // QH)
    arrived = [
        lax.ppermute(queries, "kvb", [(k, (k + r) % kvb_count) for k in range(kvb_count)])
        for r in range(1, kvb_count)
    ]
    bias, fresh, fresh_values, own_queries = pl.pallas_call(
        prepare_body,
        out_shape=(
            jax.ShapeDtypeStruct((seq_total, tokens), jnp.float32),
            jax.ShapeDtypeStruct((seq_rep, STATS), jnp.float32),
            jax.ShapeDtypeStruct((seq_rep, kv_local * HD), jnp.float32),
            jax.ShapeDtypeStruct((seq_rep, own_width), jnp.bfloat16),
        ),
        in_specs=[pl.BlockSpec(memory_space=pltpu.SMEM)] + [hbm()] * 5,
        out_specs=(vmem(), vmem(), vmem(), vmem()),
        scratch_shapes=[
            pltpu.SMEM(lengths.shape, jnp.int32),
            pltpu.VMEM((1,) + slot_seq.shape, jnp.int32),
            pltpu.VMEM((1,) + slot_block.shape, jnp.int32),
            pltpu.VMEM(queries.shape, queries.dtype),
            pltpu.VMEM(new_kv.shape, new_kv.dtype),
            pltpu.SemaphoreType.DMA((5,)),
        ],
        compiler_params=pltpu.CompilerParams(vmem_limit_bytes=4 << 20),
        cost_estimate=pl.CostEstimate(flops=COVER, transcendentals=0, bytes_accessed=1 << 20),
        name="prepare",
    )(block_counts, *[
        pltpu.with_memory_space_constraint(array, pltpu.HBM)
        for array in (lengths, slot_seq[None], slot_block[None], queries, new_kv)
    ])
    wide = lax.all_gather(jnp.stack([own_queries] + arrived), "tp", axis=0, tiled=False)
    block = jax.ShapeDtypeStruct((seq_total, own_width + STATS), jnp.bfloat16)
    sent = pl.pallas_call(
        attend_body,
        out_shape=(block,) * tp_count,
        in_specs=[vmem(), vmem(), vmem()],
        out_specs=(vmem(),) * tp_count,
        scratch_shapes=[pltpu.VMEM((tp_count, seq_total, own_width), jnp.float32)],
        compiler_params=pltpu.CompilerParams(vmem_limit_bytes=10 << 20),
        cost_estimate=pl.CostEstimate(flops=COVER, transcendentals=0, bytes_accessed=1 << 20),
        name="attend",
    )(bias, wide, resident(kv_cache))
    parts = [sent[0]] + [
        lax.ppermute(sent[d], "tp", [(t, (t + d) % tp_count) for t in range(tp_count)])
        for d in range(1, tp_count)
    ]
    block = jax.ShapeDtypeStruct((seq_rep, own_width + STATS), jnp.bfloat16)
    dealt = pl.pallas_call(
        lambda *refs: merge_body(*refs, sources=tp_count),
        out_shape=(block,) * kvb_count,
        in_specs=[vmem()] * tp_count,
        out_specs=(vmem(),) * kvb_count,
        compiler_params=pltpu.CompilerParams(vmem_limit_bytes=4 << 20),
        name="merge",
    )(*parts)
    parts = [dealt[0]] + [
        lax.ppermute(dealt[r], "kvb", [(k, (k - r) % kvb_count) for k in range(kvb_count)])
        for r in range(1, kvb_count)
    ]
    projected = pl.pallas_call(
        lambda *refs: project_body(*refs, sources=kvb_count),
        out_shape=jax.ShapeDtypeStruct((seq_rep, out_weight.shape[1]), jnp.bfloat16),
        in_specs=[vmem()] * (kvb_count + 3),
        out_specs=vmem(),
        compiler_params=pltpu.CompilerParams(vmem_limit_bytes=4 << 20),
        name="project",
    )(*parts, fresh, fresh_values, resident(out_weight))
    pieces = lax.all_gather(projected, "tp", axis=0, tiled=False)
    own = jax.ShapeDtypeStruct((seq_rep, norm_gain.shape[0]), jnp.bfloat16)
    return pl.pallas_call(
        finish_body,
        out_shape=(own, own),
        in_specs=[vmem(), vmem(), vmem()],
        out_specs=(vmem(), vmem()),
        compiler_params=pltpu.CompilerParams(vmem_limit_bytes=4 << 20),
        name="finish",
    )(pieces, residual, norm_gain[None])


def solution(mesh):
    placed = (
        P(("groups", "kvb"), None),
        P(("groups", "kvb"), "tp"),
        P(("groups", "kvb"), None),
        P(("groups", "kvb", "tp"), None, None),
        P("groups"),
        P(("groups", "kvb", "tp")),
        P(("groups", "kvb", "tp")),
        P(("groups", "kvb", "tp")),
        P("tp", None),
        P("tp"),
    )
    return jax.shard_map(
        on_device,
        mesh=mesh,
        in_specs=placed,
        out_specs=(P(("groups", "kvb"), "tp"), P(("groups", "kvb"), "tp")),
        check_vma=False,
    )
```

```python
import jax
import jax.numpy as jnp
from jax import lax
from jax.experimental import pallas as pl
from jax.experimental.pallas import tpu as pltpu
from jax.sharding import PartitionSpec as P

QH = 64
KVH = 8
HD = 128
BLK = 16

MASKED = -1e30
FLOOR = -1e20
EPSILON = 1e-06
UNIT = HD ** (-0.5) * 1.4426950408889634
STATS = 128
COVER = 20_000_000_000
SHARES = (10, 4, 10, 8)
STEP = 512


def prepare_body(*refs):
    count, inputs, (bias, fresh_out, value_out, own_out) = refs[0], refs[1:6], refs[6:10]
    held, arrived = refs[10:15], refs[15]
    copies = [
        pltpu.make_async_copy(source, target, arrived.at[n])
        for n, (source, target) in enumerate(zip(inputs, held))
    ]
    for copy in copies:
        copy.start()
    for copy in copies:
        copy.wait()
    lengths, slot_seq, slot_block, queries, new_kv = held
    seq_total, tokens = bias.shape
    slots = tokens // BLK
    seq_rep, own_width = queries.shape
    local_heads = own_width // HD
    group_size = QH // KVH
    kvb_count = seq_total // seq_rep
    seq = slot_seq[...]
    length_of = jnp.zeros_like(seq)
    for s in range(seq_total):
        length_of = jnp.where(seq == s, lengths[s], length_of)
    slot_ids = lax.broadcasted_iota(jnp.int32, seq.shape, 1)
    remaining = jnp.clip(length_of - slot_block[...] * BLK, 0, BLK)
    remaining = jnp.where(slot_ids < count[0], remaining, 0)
    row = lax.broadcasted_iota(jnp.int32, (8, slots), 0)
    codes = jnp.where(row == 0, seq, jnp.where(row == 1, remaining, 0))
    spread = (
        lax.broadcasted_iota(jnp.int32, (slots, tokens), 1) // BLK
        == lax.broadcasted_iota(jnp.int32, (slots, tokens), 0)
    )
    per_token = jnp.dot(
        codes.astype(jnp.float32).astype(jnp.bfloat16),
        jnp.where(spread, 1.0, 0.0).astype(jnp.bfloat16),
        preferred_element_type=jnp.float32,
    )
    row = lax.broadcasted_iota(jnp.int32, (seq_total, tokens), 0)
    replica = lax.axis_index("kvb") - row // seq_rep
    replica = jnp.where(replica < 0, replica + kvb_count, replica)
    seq_ids = (replica * seq_rep + row % seq_rep).astype(jnp.float32)
    offsets = (lax.broadcasted_iota(jnp.int32, (seq_total, tokens), 1) % BLK).astype(jnp.float32)
    live = (per_token[0:1] == seq_ids) & (offsets < per_token[1:2])
    bias[...] = jnp.where(live, 0.0, MASKED)

    own_out[...] = queries[...]
    kv_local = max(1, local_heads // group_size)
    kv_first = lax.axis_index("tp") * local_heads // group_size
    lane = lax.broadcasted_iota(jnp.int32, (seq_rep, STATS), 1)
    fresh = jnp.zeros((seq_rep, STATS), jnp.float32)
    for v in range(kv_local):
        at = pl.multiple_of((kv_first + v) * HD, HD)
        key = new_kv[:, pl.ds(at, HD)].astype(jnp.float32)
        at = pl.multiple_of((KVH + kv_first + v) * HD, HD)
        value_out[:, v * HD : (v + 1) * HD] = new_kv[:, pl.ds(at, HD)].astype(jnp.float32)
        for h in range(v * local_heads // kv_local, (v + 1) * local_heads // kv_local):
            query = queries[:, h * HD : (h + 1) * HD].astype(jnp.float32)
            score = jnp.sum(query * key, axis=1, keepdims=True)
            fresh = jnp.where(lane == h, score, fresh)
    fresh_out[...] = fresh * UNIT


def attend_body(bias_ref, wide, cache, weight, *refs):
    outs, (chunk, stacked, arrived) = refs[:-3], refs[-3:]
    early = pltpu.make_async_copy(weight.at[:, pl.ds(0, chunk.shape[1])], chunk, arrived)
    early.start()
    tp_count, kvb_count, seq_rep, own_width = wide.shape
    tokens = cache.shape[0] * BLK
    seq_total = kvb_count * seq_rep
    local_heads = own_width // HD
    group_size = QH // KVH
    kv_local = max(1, local_heads // group_size)
    per_kv = local_heads // kv_local
    bias = bias_ref[...]
    for r in range(kvb_count):
        for t in range(tp_count):
            stacked[t, r * seq_rep : (r + 1) * seq_rep, :] = wide[t, r].astype(jnp.float32)

    me = lax.axis_index("tp")
    lane = lax.broadcasted_iota(jnp.int32, (seq_total, STATS), 1)
    for d, out in enumerate(outs):
        t = jnp.where(me + d < tp_count, me + d, me + d - tp_count)
        stats = jnp.zeros((seq_total, STATS), jnp.float32)
        for v in range(kv_local):
            heads = range(v * per_kv, (v + 1) * per_kv)
            rows = jnp.concatenate(
                [stacked[t, :, h * HD : (h + 1) * HD] for h in heads], axis=0
            ).astype(jnp.bfloat16)
            g = t * local_heads // group_size + v
            at = pl.multiple_of(g * HD, HD)
            keys = cache[:, :, pl.ds(at, HD)].reshape(tokens, HD)
            at = pl.multiple_of((KVH + g) * HD, HD)
            values = cache[:, :, pl.ds(at, HD)].reshape(tokens, HD)
            scores = lax.dot_general(
                rows, keys, (((1,), (1,)), ((), ())), preferred_element_type=jnp.float32
            )
            scores = scores.reshape(per_kv, seq_total, tokens) * UNIT + bias[None]
            peaks = jnp.maximum(jnp.max(scores, axis=2, keepdims=True), FLOOR)
            peaks = peaks.astype(jnp.bfloat16).astype(jnp.float32)
            weights = jnp.exp2(scores - peaks)
            sums = jnp.sum(weights, axis=2, keepdims=True)
            partial = jnp.dot(
                weights.astype(jnp.bfloat16).reshape(per_kv * seq_total, tokens),
                values,
                preferred_element_type=jnp.float32,
            )
            high = sums.astype(jnp.bfloat16).astype(jnp.float32)
            low = sums - high
            for j, h in enumerate(heads):
                out[:, h * HD : (h + 1) * HD] = partial[
                    j * seq_total : (j + 1) * seq_total
                ].astype(jnp.bfloat16)
                for part, value in enumerate((peaks, high, low)):
                    stats = jnp.where(lane == part * local_heads + h, value[j], stats)
        out[:, local_heads * HD :] = stats.astype(jnp.bfloat16)
    early.wait()


def fetch_body(weight, *refs, first):
    chunk, arrived = refs[-2:]
    copy = pltpu.make_async_copy(weight.at[:, pl.ds(first, chunk.shape[1])], chunk, arrived)
    copy.start()
    copy.wait()


def unpack(ref, local_heads):
    stats = ref[:, local_heads * HD :].astype(jnp.float32)
    sums = stats[:, local_heads : 2 * local_heads] + stats[:, 2 * local_heads : 3 * local_heads]
    return stats[:, :local_heads], sums


def merge_body(*refs, sources):
    parts, outs = refs[:sources], refs[sources:]
    seq_total, width = parts[0].shape
    seq_rep = outs[0].shape[0]
    local_heads = (width - STATS) // HD
    pairs = [unpack(part, local_heads) for part in parts]
    peak = pairs[0][0]
    for other, _ in pairs[1:]:
        peak = jnp.maximum(peak, other)
    scaling = [jnp.exp2(p - peak) for p, _ in pairs]
    total = sum(s * c for s, (_, c) in zip(scaling, pairs))
    high = total.astype(jnp.bfloat16).astype(jnp.float32)
    pad = jnp.zeros((seq_total, STATS - 3 * local_heads), jnp.float32)
    stats = jnp.concatenate([peak, high, total - high, pad], axis=1)
    blocks = [
        sum(
            s[:, h : h + 1] * part[:, h * HD : (h + 1) * HD].astype(jnp.float32)
            for s, part in zip(scaling, parts)
        )
        for h in range(local_heads)
    ]
    for h, block in enumerate(blocks + [stats]):
        for r, out in enumerate(outs):
            out[:, h * HD : (h + 1) * HD] = block[r * seq_rep : (r + 1) * seq_rep].astype(
                jnp.bfloat16
            )


def project_body(*refs, sources):
    parts = refs[:sources]
    fresh_ref, value_ref, weight = refs[sources : sources + 3]
    chunks = list(refs[sources + 3 : -3])
    out, late, arrived = refs[-3:]
    first = weight.shape[1] - late.shape[1]
    last_copy = pltpu.make_async_copy(weight.at[:, pl.ds(first, late.shape[1])], late, arrived)
    last_copy.start()
    local_heads = (parts[0].shape[1] - STATS) // HD
    kv_local = value_ref.shape[1] // HD
    pairs = [unpack(part, local_heads) for part in parts]
    fresh = fresh_ref[:, :local_heads]
    overall = fresh
    for peak, _ in pairs:
        overall = jnp.maximum(overall, peak)
    scaling = [jnp.exp2(peak - overall) for peak, _ in pairs]
    fresh_weight = jnp.exp2(fresh - overall)
    inverse = 1.0 / (fresh_weight + sum(s * c for s, (_, c) in zip(scaling, pairs)))
    scaling = [s * inverse for s in scaling]
    fresh_weight = fresh_weight * inverse
    attended = []
    for h in range(local_heads):
        v = h * kv_local // local_heads
        total = fresh_weight[:, h : h + 1] * value_ref[:, v * HD : (v + 1) * HD]
        for s, part in zip(scaling, parts):
            total = total + s[:, h : h + 1] * part[:, h * HD : (h + 1) * HD].astype(jnp.float32)
        attended.append(total.astype(jnp.bfloat16))
    attended = jnp.concatenate(attended, axis=1)
    first = 0
    for chunk in chunks + [late]:
        if chunk is late:
            last_copy.wait()
        step = min(STEP, chunk.shape[1])
        for at in range(0, chunk.shape[1], step):
            out[:, first + at : first + at + step] = jnp.dot(
                attended, chunk[:, at : at + step], preferred_element_type=jnp.float32
            ).astype(out.dtype)
        first += chunk.shape[1]


def finish_body(pieces, residual, gain, stream_out, normed_out):
    full = residual[...].astype(jnp.float32)
    width = full.shape[1]
    total = pieces[0].astype(jnp.float32)
    for t in range(1, pieces.shape[0]):
        total = total + pieces[t].astype(jnp.float32)
    full = (full + total).astype(jnp.bfloat16).astype(jnp.float32)
    mean_square = jnp.sum(full * full, axis=1, keepdims=True) / width
    inverse = lax.rsqrt(mean_square + EPSILON)
    own = stream_out.shape[1]
    at = pl.multiple_of(lax.axis_index("tp") * own, own)
    mine = residual[:, pl.ds(at, own)].astype(jnp.float32)
    total = pieces[0, :, pl.ds(at, own)].astype(jnp.float32)
    for t in range(1, pieces.shape[0]):
        total = total + pieces[t, :, pl.ds(at, own)].astype(jnp.float32)
    stream = (mine + total).astype(jnp.bfloat16)
    stream_out[...] = stream
    normed_out[...] = (stream.astype(jnp.float32) * inverse * gain[...].astype(jnp.float32)).astype(
        jnp.bfloat16
    )


def vmem():
    return pl.BlockSpec(memory_space=pltpu.VMEM)


def resident(array):
    return pltpu.with_memory_space_constraint(array, pltpu.VMEM)


def hbm():
    return pl.BlockSpec(memory_space=pltpu.HBM)


def on_device(
    residual,
    queries,
    new_kv,
    kv_cache,
    lengths,
    slot_seq,
    slot_block,
    block_counts,
    out_weight,
    norm_gain,
):
    tp_count = lax.axis_size("tp")
    kvb_count = lax.axis_size("kvb")
    seq_rep, own_width = queries.shape
    seq_total = kvb_count * seq_rep
    tokens = kv_cache.shape[0] * BLK
    kv_local = max(1, own_width // HD * KVH // QH)
    arrived = [
        lax.ppermute(queries, "kvb", [(k, (k + r) % kvb_count) for k in range(kvb_count)])
        for r in range(1, kvb_count)
    ]
    bias, fresh, fresh_values, own_queries = pl.pallas_call(
        prepare_body,
        out_shape=(
            jax.ShapeDtypeStruct((seq_total, tokens), jnp.float32),
            jax.ShapeDtypeStruct((seq_rep, STATS), jnp.float32),
            jax.ShapeDtypeStruct((seq_rep, kv_local * HD), jnp.float32),
            jax.ShapeDtypeStruct((seq_rep, own_width), jnp.bfloat16),
        ),
        in_specs=[pl.BlockSpec(memory_space=pltpu.SMEM)] + [hbm()] * 5,
        out_specs=(vmem(), vmem(), vmem(), vmem()),
        scratch_shapes=[
            pltpu.SMEM(lengths.shape, jnp.int32),
            pltpu.VMEM((1,) + slot_seq.shape, jnp.int32),
            pltpu.VMEM((1,) + slot_block.shape, jnp.int32),
            pltpu.VMEM(queries.shape, queries.dtype),
            pltpu.VMEM(new_kv.shape, new_kv.dtype),
            pltpu.SemaphoreType.DMA((5,)),
        ],
        compiler_params=pltpu.CompilerParams(vmem_limit_bytes=4 << 20),
        cost_estimate=pl.CostEstimate(flops=COVER, transcendentals=0, bytes_accessed=1 << 20),
        name="prepare",
    )(block_counts, *[
        pltpu.with_memory_space_constraint(array, pltpu.HBM)
        for array in (lengths, slot_seq[None], slot_block[None], queries, new_kv)
    ])
    wide = lax.all_gather(jnp.stack([own_queries] + arrived), "tp", axis=0, tiled=False)
    depth, columns = out_weight.shape
    out_weight = pltpu.with_memory_space_constraint(out_weight, pltpu.HBM)
    share = [columns * n // sum(SHARES) for n in SHARES]

    def fetch(first, size, *after):
        return pl.pallas_call(
            lambda *refs: fetch_body(*refs, first=first),
            out_shape=pltpu.VMEM((depth, size), out_weight.dtype),
            in_specs=[hbm()] + [pl.BlockSpec(memory_space=pl.ANY)] * len(after),
            out_specs=vmem(),
            scratch_shapes=[pltpu.SemaphoreType.DMA],
            compiler_params=pltpu.CompilerParams(vmem_limit_bytes=1 << 20),
            cost_estimate=pl.CostEstimate(flops=COVER, transcendentals=0, bytes_accessed=1 << 20),
            name="fetch",
        )(out_weight, *after)

    block = jax.ShapeDtypeStruct((seq_total, own_width + STATS), jnp.bfloat16)
    *sent, under_attend = pl.pallas_call(
        attend_body,
        out_shape=(block,) * tp_count + (pltpu.VMEM((depth, share[0]), out_weight.dtype),),
        in_specs=[vmem(), vmem(), vmem(), hbm()],
        out_specs=(vmem(),) * (tp_count + 1),
        scratch_shapes=[
            pltpu.VMEM((tp_count, seq_total, own_width), jnp.float32),
            pltpu.SemaphoreType.DMA,
        ],
        compiler_params=pltpu.CompilerParams(vmem_limit_bytes=10 << 20),
        cost_estimate=pl.CostEstimate(flops=COVER, transcendentals=0, bytes_accessed=1 << 20),
        name="attend",
    )(bias, wide, resident(kv_cache), out_weight)
    parts = [sent[0]] + [
        lax.ppermute(sent[d], "tp", [(t, (t + d) % tp_count) for t in range(tp_count)])
        for d in range(1, tp_count)
    ]
    block = jax.ShapeDtypeStruct((seq_rep, own_width + STATS), jnp.bfloat16)
    beside_tp = fetch(share[0], share[1], sent[0])
    dealt = pl.pallas_call(
        lambda *refs: merge_body(*refs, sources=tp_count),
        out_shape=(block,) * kvb_count,
        in_specs=[vmem()] * tp_count,
        out_specs=(vmem(),) * kvb_count,
        compiler_params=pltpu.CompilerParams(vmem_limit_bytes=4 << 20),
        name="merge",
    )(*parts)
    parts = [dealt[0]] + [
        lax.ppermute(dealt[r], "kvb", [(k, (k - r) % kvb_count) for k in range(kvb_count)])
        for r in range(1, kvb_count)
    ]
    beside_kvb = fetch(share[0] + share[1], share[2], dealt[0])
    projected = pl.pallas_call(
        lambda *refs: project_body(*refs, sources=kvb_count),
        out_shape=jax.ShapeDtypeStruct((seq_rep, out_weight.shape[1]), jnp.bfloat16),
        in_specs=[vmem()] * (kvb_count + 2) + [hbm()] + [vmem()] * 3,
        out_specs=vmem(),
        scratch_shapes=[pltpu.VMEM((depth, share[3]), out_weight.dtype), pltpu.SemaphoreType.DMA],
        compiler_params=pltpu.CompilerParams(vmem_limit_bytes=12 << 20),
        name="project",
    )(*parts, fresh, fresh_values, out_weight, under_attend, beside_tp, beside_kvb)
    pieces = lax.all_gather(projected, "tp", axis=0, tiled=False)
    own = jax.ShapeDtypeStruct((seq_rep, norm_gain.shape[0]), jnp.bfloat16)
    return pl.pallas_call(
        finish_body,
        out_shape=(own, own),
        in_specs=[vmem(), vmem(), vmem()],
        out_specs=(vmem(), vmem()),
        compiler_params=pltpu.CompilerParams(vmem_limit_bytes=4 << 20),
        name="finish",
    )(pieces, residual, norm_gain[None])


def solution(mesh):
    placed = (
        P(("groups", "kvb"), None),
        P(("groups", "kvb"), "tp"),
        P(("groups", "kvb"), None),
        P(("groups", "kvb", "tp"), None, None),
        P("groups"),
        P(("groups", "kvb", "tp")),
        P(("groups", "kvb", "tp")),
        P(("groups", "kvb", "tp")),
        P("tp", None),
        P("tp"),
    )
    return jax.shard_map(
        on_device,
        mesh=mesh,
        in_specs=placed,
        out_specs=(P(("groups", "kvb"), "tp"), P(("groups", "kvb"), "tp")),
        check_vma=False,
    )
```

```python
import jax
import jax.numpy as jnp
from jax import lax
from jax.experimental import pallas as pl
from jax.experimental.pallas import tpu as pltpu
from jax.sharding import PartitionSpec as P

QH = 64
KVH = 8
HD = 128
BLK = 16

MASKED = -1e30
FLOOR = -1e20
EPSILON = 1e-06
UNIT = HD ** (-0.5) * 1.4426950408889634
STATS = 128
COVER = 20_000_000_000
SHARES = (3, 5, 4, 9, 11)
STEP = 512


def prepare_body(*refs):
    count, inputs, (bias, fresh_out, value_out, own_out) = refs[0], refs[1:6], refs[6:10]
    held, arrived = refs[10:15], refs[15]
    copies = [
        pltpu.make_async_copy(source, target, arrived.at[n])
        for n, (source, target) in enumerate(zip(inputs, held))
    ]
    for copy in copies:
        copy.start()
    for copy in copies:
        copy.wait()
    lengths, slot_seq, slot_block, queries, new_kv = held
    seq_total, tokens = bias.shape
    slots = tokens // BLK
    seq_rep, own_width = queries.shape
    local_heads = own_width // HD
    group_size = QH // KVH
    kvb_count = seq_total // seq_rep
    seq = slot_seq[...]
    length_of = jnp.zeros_like(seq)
    for s in range(seq_total):
        length_of = jnp.where(seq == s, lengths[s], length_of)
    slot_ids = lax.broadcasted_iota(jnp.int32, seq.shape, 1)
    remaining = jnp.clip(length_of - slot_block[...] * BLK, 0, BLK)
    remaining = jnp.where(slot_ids < count[0], remaining, 0)
    row = lax.broadcasted_iota(jnp.int32, (8, slots), 0)
    codes = jnp.where(row == 0, seq, jnp.where(row == 1, remaining, 0))
    spread = (
        lax.broadcasted_iota(jnp.int32, (slots, tokens), 1) // BLK
        == lax.broadcasted_iota(jnp.int32, (slots, tokens), 0)
    )
    per_token = jnp.dot(
        codes.astype(jnp.float32).astype(jnp.bfloat16),
        jnp.where(spread, 1.0, 0.0).astype(jnp.bfloat16),
        preferred_element_type=jnp.float32,
    )
    row = lax.broadcasted_iota(jnp.int32, (seq_total, tokens), 0)
    replica = lax.axis_index("kvb") - row // seq_rep
    replica = jnp.where(replica < 0, replica + kvb_count, replica)
    seq_ids = (replica * seq_rep + row % seq_rep).astype(jnp.float32)
    offsets = (lax.broadcasted_iota(jnp.int32, (seq_total, tokens), 1) % BLK).astype(jnp.float32)
    live = (per_token[0:1] == seq_ids) & (offsets < per_token[1:2])
    bias[...] = jnp.where(live, 0.0, MASKED)

    own_out[...] = queries[...]
    kv_local = max(1, local_heads // group_size)
    kv_first = lax.axis_index("tp") * local_heads // group_size
    lane = lax.broadcasted_iota(jnp.int32, (seq_rep, STATS), 1)
    fresh = jnp.zeros((seq_rep, STATS), jnp.float32)
    for v in range(kv_local):
        at = pl.multiple_of((kv_first + v) * HD, HD)
        key = new_kv[:, pl.ds(at, HD)].astype(jnp.float32)
        at = pl.multiple_of((KVH + kv_first + v) * HD, HD)
        value_out[:, v * HD : (v + 1) * HD] = new_kv[:, pl.ds(at, HD)].astype(jnp.float32)
        for h in range(v * local_heads // kv_local, (v + 1) * local_heads // kv_local):
            query = queries[:, h * HD : (h + 1) * HD].astype(jnp.float32)
            score = jnp.sum(query * key, axis=1, keepdims=True)
            fresh = jnp.where(lane == h, score, fresh)
    fresh_out[...] = fresh * UNIT


def attend_body(bias_ref, queries, cache, out, stacked, *, shift):
    kvb_count, seq_rep, own_width = queries.shape
    tp_count = lax.axis_size("tp")
    tokens = cache.shape[0] * BLK
    seq_total = kvb_count * seq_rep
    local_heads = own_width // HD
    group_size = QH // KVH
    kv_local = max(1, local_heads // group_size)
    per_kv = local_heads // kv_local
    bias = bias_ref[...]
    for r in range(kvb_count):
        stacked[r * seq_rep : (r + 1) * seq_rep, :] = queries[r].astype(jnp.float32)
    t = lax.axis_index("tp") + shift
    t = jnp.where(t < tp_count, t, t - tp_count)
    lane = lax.broadcasted_iota(jnp.int32, (seq_total, STATS), 1)
    stats = jnp.zeros((seq_total, STATS), jnp.float32)
    for v in range(kv_local):
        heads = range(v * per_kv, (v + 1) * per_kv)
        rows = jnp.concatenate(
            [stacked[:, h * HD : (h + 1) * HD] for h in heads], axis=0
        ).astype(jnp.bfloat16)
        g = t * local_heads // group_size + v
        at = pl.multiple_of(g * HD, HD)
        keys = cache[:, :, pl.ds(at, HD)].reshape(tokens, HD)
        at = pl.multiple_of((KVH + g) * HD, HD)
        values = cache[:, :, pl.ds(at, HD)].reshape(tokens, HD)
        scores = lax.dot_general(
            rows, keys, (((1,), (1,)), ((), ())), preferred_element_type=jnp.float32
        )
        scores = scores.reshape(per_kv, seq_total, tokens) * UNIT + bias[None]
        peaks = jnp.maximum(jnp.max(scores, axis=2, keepdims=True), FLOOR)
        peaks = peaks.astype(jnp.bfloat16).astype(jnp.float32)
        weights = jnp.exp2(scores - peaks)
        sums = jnp.sum(weights, axis=2, keepdims=True)
        partial = jnp.dot(
            weights.astype(jnp.bfloat16).reshape(per_kv * seq_total, tokens),
            values,
            preferred_element_type=jnp.float32,
        )
        high = sums.astype(jnp.bfloat16).astype(jnp.float32)
        low = sums - high
        for j, h in enumerate(heads):
            out[:, h * HD : (h + 1) * HD] = partial[j * seq_total : (j + 1) * seq_total].astype(
                jnp.bfloat16
            )
            for part, value in enumerate((peaks, high, low)):
                stats = jnp.where(lane == part * local_heads + h, value[j], stats)
    out[:, local_heads * HD :] = stats.astype(jnp.bfloat16)


def fetch_body(weight, *refs, first):
    chunk, arrived = refs[-2:]
    copy = pltpu.make_async_copy(weight.at[:, pl.ds(first, chunk.shape[1])], chunk, arrived)
    copy.start()
    copy.wait()


def unpack(ref, local_heads):
    stats = ref[:, local_heads * HD :].astype(jnp.float32)
    sums = stats[:, local_heads : 2 * local_heads] + stats[:, 2 * local_heads : 3 * local_heads]
    return stats[:, :local_heads], sums


def merge_body(*refs, sources):
    parts, outs = refs[:sources], refs[sources:]
    seq_total, width = parts[0].shape
    seq_rep = outs[0].shape[0]
    local_heads = (width - STATS) // HD
    pairs = [unpack(part, local_heads) for part in parts]
    peak = pairs[0][0]
    for other, _ in pairs[1:]:
        peak = jnp.maximum(peak, other)
    scaling = [jnp.exp2(p - peak) for p, _ in pairs]
    total = sum(s * c for s, (_, c) in zip(scaling, pairs))
    high = total.astype(jnp.bfloat16).astype(jnp.float32)
    pad = jnp.zeros((seq_total, STATS - 3 * local_heads), jnp.float32)
    stats = jnp.concatenate([peak, high, total - high, pad], axis=1)
    blocks = [
        sum(
            s[:, h : h + 1] * part[:, h * HD : (h + 1) * HD].astype(jnp.float32)
            for s, part in zip(scaling, parts)
        )
        for h in range(local_heads)
    ]
    for h, block in enumerate(blocks + [stats]):
        for r, out in enumerate(outs):
            out[:, h * HD : (h + 1) * HD] = block[r * seq_rep : (r + 1) * seq_rep].astype(
                jnp.bfloat16
            )


def project_body(*refs, sources):
    parts = refs[:sources]
    fresh_ref, value_ref, weight = refs[sources : sources + 3]
    chunks = list(refs[sources + 3 : -3])
    out, late, arrived = refs[-3:]
    first = weight.shape[1] - late.shape[1]
    last_copy = pltpu.make_async_copy(weight.at[:, pl.ds(first, late.shape[1])], late, arrived)
    last_copy.start()
    local_heads = (parts[0].shape[1] - STATS) // HD
    kv_local = value_ref.shape[1] // HD
    pairs = [unpack(part, local_heads) for part in parts]
    fresh = fresh_ref[:, :local_heads]
    overall = fresh
    for peak, _ in pairs:
        overall = jnp.maximum(overall, peak)
    scaling = [jnp.exp2(peak - overall) for peak, _ in pairs]
    fresh_weight = jnp.exp2(fresh - overall)
    inverse = 1.0 / (fresh_weight + sum(s * c for s, (_, c) in zip(scaling, pairs)))
    scaling = [s * inverse for s in scaling]
    fresh_weight = fresh_weight * inverse
    attended = []
    for h in range(local_heads):
        v = h * kv_local // local_heads
        total = fresh_weight[:, h : h + 1] * value_ref[:, v * HD : (v + 1) * HD]
        for s, part in zip(scaling, parts):
            total = total + s[:, h : h + 1] * part[:, h * HD : (h + 1) * HD].astype(jnp.float32)
        attended.append(total.astype(jnp.bfloat16))
    attended = jnp.concatenate(attended, axis=1)
    first = 0
    for chunk in chunks + [late]:
        if chunk is late:
            last_copy.wait()
        for at in range(0, chunk.shape[1], STEP):
            step = min(STEP, chunk.shape[1] - at)
            out[:, first + at : first + at + step] = jnp.dot(
                attended, chunk[:, at : at + step], preferred_element_type=jnp.float32
            ).astype(out.dtype)
        first += chunk.shape[1]


def finish_body(pieces, residual, gain, stream_out, normed_out):
    full = residual[...].astype(jnp.float32)
    width = full.shape[1]
    total = pieces[0].astype(jnp.float32)
    for t in range(1, pieces.shape[0]):
        total = total + pieces[t].astype(jnp.float32)
    full = (full + total).astype(jnp.bfloat16).astype(jnp.float32)
    mean_square = jnp.sum(full * full, axis=1, keepdims=True) / width
    inverse = lax.rsqrt(mean_square + EPSILON)
    own = stream_out.shape[1]
    at = pl.multiple_of(lax.axis_index("tp") * own, own)
    mine = residual[:, pl.ds(at, own)].astype(jnp.float32)
    total = pieces[0, :, pl.ds(at, own)].astype(jnp.float32)
    for t in range(1, pieces.shape[0]):
        total = total + pieces[t, :, pl.ds(at, own)].astype(jnp.float32)
    stream = (mine + total).astype(jnp.bfloat16)
    stream_out[...] = stream
    normed_out[...] = (stream.astype(jnp.float32) * inverse * gain[...].astype(jnp.float32)).astype(
        jnp.bfloat16
    )


def vmem():
    return pl.BlockSpec(memory_space=pltpu.VMEM)


def resident(array):
    return pltpu.with_memory_space_constraint(array, pltpu.VMEM)


def hbm():
    return pl.BlockSpec(memory_space=pltpu.HBM)


def on_device(
    residual,
    queries,
    new_kv,
    kv_cache,
    lengths,
    slot_seq,
    slot_block,
    block_counts,
    out_weight,
    norm_gain,
):
    tp_count = lax.axis_size("tp")
    kvb_count = lax.axis_size("kvb")
    seq_rep, own_width = queries.shape
    seq_total = kvb_count * seq_rep
    tokens = kv_cache.shape[0] * BLK
    kv_local = max(1, own_width // HD * KVH // QH)
    arrived = [
        lax.ppermute(queries, "kvb", [(k, (k + r) % kvb_count) for k in range(kvb_count)])
        for r in range(1, kvb_count)
    ]
    bias, fresh, fresh_values, own_queries = pl.pallas_call(
        prepare_body,
        out_shape=(
            jax.ShapeDtypeStruct((seq_total, tokens), jnp.float32),
            jax.ShapeDtypeStruct((seq_rep, STATS), jnp.float32),
            jax.ShapeDtypeStruct((seq_rep, kv_local * HD), jnp.float32),
            jax.ShapeDtypeStruct((seq_rep, own_width), jnp.bfloat16),
        ),
        in_specs=[pl.BlockSpec(memory_space=pltpu.SMEM)] + [hbm()] * 5,
        out_specs=(vmem(), vmem(), vmem(), vmem()),
        scratch_shapes=[
            pltpu.SMEM(lengths.shape, jnp.int32),
            pltpu.VMEM((1,) + slot_seq.shape, jnp.int32),
            pltpu.VMEM((1,) + slot_block.shape, jnp.int32),
            pltpu.VMEM(queries.shape, queries.dtype),
            pltpu.VMEM(new_kv.shape, new_kv.dtype),
            pltpu.SemaphoreType.DMA((5,)),
        ],
        compiler_params=pltpu.CompilerParams(vmem_limit_bytes=4 << 20),
        cost_estimate=pl.CostEstimate(flops=COVER, transcendentals=0, bytes_accessed=1 << 20),
        name="prepare",
    )(block_counts, *[
        pltpu.with_memory_space_constraint(array, pltpu.HBM)
        for array in (lengths, slot_seq[None], slot_block[None], queries, new_kv)
    ])
    wide = jnp.stack([own_queries] + arrived)
    cache = resident(kv_cache)
    depth, columns = out_weight.shape
    out_weight = pltpu.with_memory_space_constraint(out_weight, pltpu.HBM)
    share = [columns * n // sum(SHARES) for n in SHARES]

    def fetch(first, size, *after):
        return pl.pallas_call(
            lambda *refs: fetch_body(*refs, first=first),
            out_shape=pltpu.VMEM((depth, size), out_weight.dtype),
            in_specs=[hbm()] + [pl.BlockSpec(memory_space=pl.ANY)] * len(after),
            out_specs=vmem(),
            scratch_shapes=[pltpu.SemaphoreType.DMA],
            compiler_params=pltpu.CompilerParams(vmem_limit_bytes=1 << 20),
            cost_estimate=pl.CostEstimate(flops=COVER, transcendentals=0, bytes_accessed=1 << 20),
            name="fetch",
        )(out_weight, *after)

    def attend(rows, shift):
        return pl.pallas_call(
            lambda *refs: attend_body(*refs, shift=shift),
            out_shape=jax.ShapeDtypeStruct((seq_total, own_width + STATS), jnp.bfloat16),
            in_specs=[vmem(), vmem(), vmem()],
            out_specs=vmem(),
            scratch_shapes=[pltpu.VMEM((seq_total, own_width), jnp.float32)],
            compiler_params=pltpu.CompilerParams(vmem_limit_bytes=6 << 20),
            cost_estimate=pl.CostEstimate(flops=COVER, transcendentals=0, bytes_accessed=1 << 20),
            name="attend",
        )(bias, rows, cache)

    def shifted(rows, shift):
        return lax.ppermute(rows, "tp", [(t, (t + shift) % tp_count) for t in range(tp_count)])

    starts = [sum(share[:n]) for n in range(len(share))]
    chunks = [fetch(starts[0], share[0]), fetch(starts[1], share[1], wide)]
    asked = [shifted(wide, -d) for d in range(1, tp_count)]
    parts = [attend(wide, 0)]
    for d in range(1, tp_count):
        parts.append(shifted(attend(asked[d - 1], d), d))
    chunks.append(fetch(starts[2], share[2], parts[0]))
    block = jax.ShapeDtypeStruct((seq_rep, own_width + STATS), jnp.bfloat16)
    dealt = pl.pallas_call(
        lambda *refs: merge_body(*refs, sources=tp_count),
        out_shape=(block,) * kvb_count,
        in_specs=[vmem()] * tp_count,
        out_specs=(vmem(),) * kvb_count,
        compiler_params=pltpu.CompilerParams(vmem_limit_bytes=4 << 20),
        name="merge",
    )(*parts)
    parts = [dealt[0]] + [
        lax.ppermute(dealt[r], "kvb", [(k, (k - r) % kvb_count) for k in range(kvb_count)])
        for r in range(1, kvb_count)
    ]
    chunks.append(fetch(starts[3], share[3], dealt[0]))
    projected = pl.pallas_call(
        lambda *refs: project_body(*refs, sources=kvb_count),
        out_shape=jax.ShapeDtypeStruct((seq_rep, out_weight.shape[1]), jnp.bfloat16),
        in_specs=[vmem()] * (kvb_count + 2) + [hbm()] + [vmem()] * len(chunks),
        out_specs=vmem(),
        scratch_shapes=[pltpu.VMEM((depth, share[4]), out_weight.dtype), pltpu.SemaphoreType.DMA],
        compiler_params=pltpu.CompilerParams(vmem_limit_bytes=12 << 20),
        name="project",
    )(*parts, fresh, fresh_values, out_weight, *chunks)
    pieces = lax.all_gather(projected, "tp", axis=0, tiled=False)
    own = jax.ShapeDtypeStruct((seq_rep, norm_gain.shape[0]), jnp.bfloat16)
    return pl.pallas_call(
        finish_body,
        out_shape=(own, own),
        in_specs=[vmem(), vmem(), vmem()],
        out_specs=(vmem(), vmem()),
        compiler_params=pltpu.CompilerParams(vmem_limit_bytes=4 << 20),
        name="finish",
    )(pieces, residual, norm_gain[None])


def solution(mesh):
    placed = (
        P(("groups", "kvb"), None),
        P(("groups", "kvb"), "tp"),
        P(("groups", "kvb"), None),
        P(("groups", "kvb", "tp"), None, None),
        P("groups"),
        P(("groups", "kvb", "tp")),
        P(("groups", "kvb", "tp")),
        P(("groups", "kvb", "tp")),
        P("tp", None),
        P("tp"),
    )
    return jax.shard_map(
        on_device,
        mesh=mesh,
        in_specs=placed,
        out_specs=(P(("groups", "kvb"), "tp"), P(("groups", "kvb"), "tp")),
        check_vma=False,
    )
```

```python
import jax
import jax.numpy as jnp
from jax import lax
from jax.experimental import pallas as pl
from jax.experimental.pallas import tpu as pltpu
from jax.sharding import PartitionSpec as P

QH = 64
KVH = 8
HD = 128
BLK = 16

MASKED = -1e30
FLOOR = -1e20
EPSILON = 1e-06
UNIT = HD ** (-0.5) * 1.4426950408889634
STATS = 128
COVER = 20_000_000_000
SHARES = (4, 4, 4, 9, 11)
STEP = 512


def once(body):
    trips = jnp.where(lax.axis_index("tp") >= 0, 1, 0)

    def trip(_, carried):
        body()
        return carried

    lax.fori_loop(0, trips, trip, 0)


def beside(weight, chunk, arrived, first, body):
    copy = pltpu.make_async_copy(weight.at[:, pl.ds(first, chunk.shape[1])], chunk, arrived)
    copy.start()
    once(body)
    copy.wait()


def prepare_body(count, *refs, first):
    inputs, weight, outs, chunk = refs[:5], refs[5], refs[6:10], refs[10]
    held, arrived, landed = refs[11:16], refs[16], refs[17]
    copies = [
        pltpu.make_async_copy(source, target, arrived.at[n])
        for n, (source, target) in enumerate(zip(inputs, held))
    ]
    for copy in copies:
        copy.start()

    def run():
        for copy in copies:
            copy.wait()
        prepare(count, *held, *outs)

    beside(weight, chunk, landed, first, run)


def prepare(
    count, lengths, slot_seq, slot_block, queries, new_kv, bias, fresh_out, value_out, own_out
):
    seq_total, tokens = bias.shape
    slots = tokens // BLK
    seq_rep, own_width = queries.shape
    local_heads = own_width // HD
    group_size = QH // KVH
    kvb_count = seq_total // seq_rep
    seq = slot_seq[...]
    length_of = jnp.zeros_like(seq)
    for s in range(seq_total):
        length_of = jnp.where(seq == s, lengths[s], length_of)
    slot_ids = lax.broadcasted_iota(jnp.int32, seq.shape, 1)
    remaining = jnp.clip(length_of - slot_block[...] * BLK, 0, BLK)
    remaining = jnp.where(slot_ids < count[0], remaining, 0)
    row = lax.broadcasted_iota(jnp.int32, (8, slots), 0)
    codes = jnp.where(row == 0, seq, jnp.where(row == 1, remaining, 0))
    spread = (
        lax.broadcasted_iota(jnp.int32, (slots, tokens), 1) // BLK
        == lax.broadcasted_iota(jnp.int32, (slots, tokens), 0)
    )
    per_token = jnp.dot(
        codes.astype(jnp.float32).astype(jnp.bfloat16),
        jnp.where(spread, 1.0, 0.0).astype(jnp.bfloat16),
        preferred_element_type=jnp.float32,
    )
    row = lax.broadcasted_iota(jnp.int32, (seq_total, tokens), 0)
    replica = lax.axis_index("kvb") - row // seq_rep
    replica = jnp.where(replica < 0, replica + kvb_count, replica)
    seq_ids = (replica * seq_rep + row % seq_rep).astype(jnp.float32)
    offsets = (lax.broadcasted_iota(jnp.int32, (seq_total, tokens), 1) % BLK).astype(jnp.float32)
    live = (per_token[0:1] == seq_ids) & (offsets < per_token[1:2])
    bias[...] = jnp.where(live, 0.0, MASKED)

    own_out[...] = queries[...]
    kv_local = max(1, local_heads // group_size)
    kv_first = lax.axis_index("tp") * local_heads // group_size
    lane = lax.broadcasted_iota(jnp.int32, (seq_rep, STATS), 1)
    fresh = jnp.zeros((seq_rep, STATS), jnp.float32)
    for v in range(kv_local):
        at = pl.multiple_of((kv_first + v) * HD, HD)
        key = new_kv[:, pl.ds(at, HD)].astype(jnp.float32)
        at = pl.multiple_of((KVH + kv_first + v) * HD, HD)
        value_out[:, v * HD : (v + 1) * HD] = new_kv[:, pl.ds(at, HD)].astype(jnp.float32)
        for h in range(v * local_heads // kv_local, (v + 1) * local_heads // kv_local):
            query = queries[:, h * HD : (h + 1) * HD].astype(jnp.float32)
            score = jnp.sum(query * key, axis=1, keepdims=True)
            fresh = jnp.where(lane == h, score, fresh)
    fresh_out[...] = fresh * UNIT


def attend_first_body(bias_ref, queries, cache, weight, out, chunk, stacked, arrived, *, first):
    run = lambda: attend_body(bias_ref, queries, cache, out, stacked, shift=0)
    beside(weight, chunk, arrived, first, run)


def attend_body(bias_ref, queries, cache, out, stacked, *, shift):
    kvb_count, seq_rep, own_width = queries.shape
    tp_count = lax.axis_size("tp")
    tokens = cache.shape[0] * BLK
    seq_total = kvb_count * seq_rep
    local_heads = own_width // HD
    group_size = QH // KVH
    kv_local = max(1, local_heads // group_size)
    per_kv = local_heads // kv_local
    bias = bias_ref[...]
    for r in range(kvb_count):
        stacked[r * seq_rep : (r + 1) * seq_rep, :] = queries[r].astype(jnp.float32)
    t = lax.axis_index("tp") + shift
    t = jnp.where(t < tp_count, t, t - tp_count)
    lane = lax.broadcasted_iota(jnp.int32, (seq_total, STATS), 1)
    stats = jnp.zeros((seq_total, STATS), jnp.float32)
    for v in range(kv_local):
        heads = range(v * per_kv, (v + 1) * per_kv)
        rows = jnp.concatenate(
            [stacked[:, h * HD : (h + 1) * HD] for h in heads], axis=0
        ).astype(jnp.bfloat16)
        g = t * local_heads // group_size + v
        at = pl.multiple_of(g * HD, HD)
        keys = cache[:, :, pl.ds(at, HD)].reshape(tokens, HD)
        at = pl.multiple_of((KVH + g) * HD, HD)
        values = cache[:, :, pl.ds(at, HD)].reshape(tokens, HD)
        scores = lax.dot_general(
            rows, keys, (((1,), (1,)), ((), ())), preferred_element_type=jnp.float32
        )
        scores = scores.reshape(per_kv, seq_total, tokens) * UNIT + bias[None]
        peaks = jnp.maximum(jnp.max(scores, axis=2, keepdims=True), FLOOR)
        peaks = peaks.astype(jnp.bfloat16).astype(jnp.float32)
        weights = jnp.exp2(scores - peaks)
        sums = jnp.sum(weights, axis=2, keepdims=True)
        partial = jnp.dot(
            weights.astype(jnp.bfloat16).reshape(per_kv * seq_total, tokens),
            values,
            preferred_element_type=jnp.float32,
        )
        high = sums.astype(jnp.bfloat16).astype(jnp.float32)
        low = sums - high
        for j, h in enumerate(heads):
            out[:, h * HD : (h + 1) * HD] = partial[j * seq_total : (j + 1) * seq_total].astype(
                jnp.bfloat16
            )
            for part, value in enumerate((peaks, high, low)):
                stats = jnp.where(lane == part * local_heads + h, value[j], stats)
    out[:, local_heads * HD :] = stats.astype(jnp.bfloat16)


def fetch_body(weight, *refs, first):
    chunk, arrived = refs[-2:]
    copy = pltpu.make_async_copy(weight.at[:, pl.ds(first, chunk.shape[1])], chunk, arrived)
    copy.start()
    copy.wait()


def unpack(ref, local_heads):
    stats = ref[:, local_heads * HD :].astype(jnp.float32)
    sums = stats[:, local_heads : 2 * local_heads] + stats[:, 2 * local_heads : 3 * local_heads]
    return stats[:, :local_heads], sums


def merge_body(*refs, sources):
    parts, outs = refs[:sources], refs[sources:]
    seq_total, width = parts[0].shape
    seq_rep = outs[0].shape[0]
    local_heads = (width - STATS) // HD
    pairs = [unpack(part, local_heads) for part in parts]
    peak = pairs[0][0]
    for other, _ in pairs[1:]:
        peak = jnp.maximum(peak, other)
    scaling = [jnp.exp2(p - peak) for p, _ in pairs]
    total = sum(s * c for s, (_, c) in zip(scaling, pairs))
    high = total.astype(jnp.bfloat16).astype(jnp.float32)
    pad = jnp.zeros((seq_total, STATS - 3 * local_heads), jnp.float32)
    stats = jnp.concatenate([peak, high, total - high, pad], axis=1)
    blocks = [
        sum(
            s[:, h : h + 1] * part[:, h * HD : (h + 1) * HD].astype(jnp.float32)
            for s, part in zip(scaling, parts)
        )
        for h in range(local_heads)
    ]
    for h, block in enumerate(blocks + [stats]):
        for r, out in enumerate(outs):
            out[:, h * HD : (h + 1) * HD] = block[r * seq_rep : (r + 1) * seq_rep].astype(
                jnp.bfloat16
            )


def project_body(*refs, sources):
    parts = refs[:sources]
    fresh_ref, value_ref, weight = refs[sources : sources + 3]
    chunks = list(refs[sources + 3 : -4])
    out, late, arrived, rows = refs[-4:]
    first = weight.shape[1] - late.shape[1]
    last_copy = pltpu.make_async_copy(weight.at[:, pl.ds(first, late.shape[1])], late, arrived)
    last_copy.start()
    def combine():
        local_heads = (parts[0].shape[1] - STATS) // HD
        kv_local = value_ref.shape[1] // HD
        pairs = [unpack(part, local_heads) for part in parts]
        fresh = fresh_ref[:, :local_heads]
        overall = fresh
        for peak, _ in pairs:
            overall = jnp.maximum(overall, peak)
        scaling = [jnp.exp2(peak - overall) for peak, _ in pairs]
        fresh_weight = jnp.exp2(fresh - overall)
        inverse = 1.0 / (fresh_weight + sum(s * c for s, (_, c) in zip(scaling, pairs)))
        scaling = [s * inverse for s in scaling]
        fresh_weight = fresh_weight * inverse
        attended = []
        for h in range(local_heads):
            v = h * kv_local // local_heads
            total = fresh_weight[:, h : h + 1] * value_ref[:, v * HD : (v + 1) * HD]
            for s, part in zip(scaling, parts):
                total = total + s[:, h : h + 1] * part[:, h * HD : (h + 1) * HD].astype(jnp.float32)
            attended.append(total.astype(jnp.bfloat16))
        rows[...] = jnp.concatenate(attended, axis=1)

    once(combine)
    attended = rows[...]
    first = 0
    for chunk in chunks + [late]:
        if chunk is late:
            last_copy.wait()
        for at in range(0, chunk.shape[1], STEP):
            step = min(STEP, chunk.shape[1] - at)
            out[:, first + at : first + at + step] = jnp.dot(
                attended, chunk[:, at : at + step], preferred_element_type=jnp.float32
            ).astype(out.dtype)
        first += chunk.shape[1]


def finish_body(pieces, residual, gain, stream_out, normed_out):
    full = residual[...].astype(jnp.float32)
    width = full.shape[1]
    total = pieces[0].astype(jnp.float32)
    for t in range(1, pieces.shape[0]):
        total = total + pieces[t].astype(jnp.float32)
    full = (full + total).astype(jnp.bfloat16).astype(jnp.float32)
    mean_square = jnp.sum(full * full, axis=1, keepdims=True) / width
    inverse = lax.rsqrt(mean_square + EPSILON)
    own = stream_out.shape[1]
    at = pl.multiple_of(lax.axis_index("tp") * own, own)
    mine = residual[:, pl.ds(at, own)].astype(jnp.float32)
    total = pieces[0, :, pl.ds(at, own)].astype(jnp.float32)
    for t in range(1, pieces.shape[0]):
        total = total + pieces[t, :, pl.ds(at, own)].astype(jnp.float32)
    stream = (mine + total).astype(jnp.bfloat16)
    stream_out[...] = stream
    normed_out[...] = (stream.astype(jnp.float32) * inverse * gain[...].astype(jnp.float32)).astype(
        jnp.bfloat16
    )


def vmem():
    return pl.BlockSpec(memory_space=pltpu.VMEM)


def resident(array):
    return pltpu.with_memory_space_constraint(array, pltpu.VMEM)


def hbm():
    return pl.BlockSpec(memory_space=pltpu.HBM)


def on_device(
    residual,
    queries,
    new_kv,
    kv_cache,
    lengths,
    slot_seq,
    slot_block,
    block_counts,
    out_weight,
    norm_gain,
):
    tp_count = lax.axis_size("tp")
    kvb_count = lax.axis_size("kvb")
    seq_rep, own_width = queries.shape
    seq_total = kvb_count * seq_rep
    tokens = kv_cache.shape[0] * BLK
    kv_local = max(1, own_width // HD * KVH // QH)
    depth, columns = out_weight.shape
    out_weight = pltpu.with_memory_space_constraint(out_weight, pltpu.HBM)
    share = [columns * n // sum(SHARES) for n in SHARES]
    starts = [sum(share[:n]) for n in range(len(share))]
    arrived = [
        lax.ppermute(queries, "kvb", [(k, (k + r) % kvb_count) for k in range(kvb_count)])
        for r in range(1, kvb_count)
    ]
    bias, fresh, fresh_values, own_queries, under_prepare = pl.pallas_call(
        lambda *refs: prepare_body(*refs, first=starts[0]),
        out_shape=(
            jax.ShapeDtypeStruct((seq_total, tokens), jnp.float32),
            jax.ShapeDtypeStruct((seq_rep, STATS), jnp.float32),
            jax.ShapeDtypeStruct((seq_rep, kv_local * HD), jnp.float32),
            jax.ShapeDtypeStruct((seq_rep, own_width), jnp.bfloat16),
            pltpu.VMEM((depth, share[0]), out_weight.dtype),
        ),
        in_specs=[pl.BlockSpec(memory_space=pltpu.SMEM)] + [hbm()] * 6,
        out_specs=(vmem(),) * 5,
        scratch_shapes=[
            pltpu.SMEM(lengths.shape, jnp.int32),
            pltpu.VMEM((1,) + slot_seq.shape, jnp.int32),
            pltpu.VMEM((1,) + slot_block.shape, jnp.int32),
            pltpu.VMEM(queries.shape, queries.dtype),
            pltpu.VMEM(new_kv.shape, new_kv.dtype),
            pltpu.SemaphoreType.DMA((5,)),
            pltpu.SemaphoreType.DMA,
        ],
        compiler_params=pltpu.CompilerParams(vmem_limit_bytes=4 << 20),
        cost_estimate=pl.CostEstimate(flops=COVER, transcendentals=0, bytes_accessed=1 << 20),
        name="prepare",
    )(block_counts, *[
        pltpu.with_memory_space_constraint(array, pltpu.HBM)
        for array in (lengths, slot_seq[None], slot_block[None], queries, new_kv)
    ], out_weight)
    wide = jnp.stack([own_queries] + arrived)
    cache = resident(kv_cache)

    def fetch(first, size, *after):
        return pl.pallas_call(
            lambda *refs: fetch_body(*refs, first=first),
            out_shape=pltpu.VMEM((depth, size), out_weight.dtype),
            in_specs=[hbm()] + [pl.BlockSpec(memory_space=pl.ANY)] * len(after),
            out_specs=vmem(),
            scratch_shapes=[pltpu.SemaphoreType.DMA],
            compiler_params=pltpu.CompilerParams(vmem_limit_bytes=1 << 20),
            cost_estimate=pl.CostEstimate(flops=COVER, transcendentals=0, bytes_accessed=1 << 20),
            name="fetch",
        )(out_weight, *after)

    def attend(rows, shift):
        return pl.pallas_call(
            lambda *refs: attend_body(*refs, shift=shift),
            out_shape=jax.ShapeDtypeStruct((seq_total, own_width + STATS), jnp.bfloat16),
            in_specs=[vmem(), vmem(), vmem()],
            out_specs=vmem(),
            scratch_shapes=[pltpu.VMEM((seq_total, own_width), jnp.float32)],
            compiler_params=pltpu.CompilerParams(vmem_limit_bytes=6 << 20),
            cost_estimate=pl.CostEstimate(flops=COVER, transcendentals=0, bytes_accessed=1 << 20),
            name="attend",
        )(bias, rows, cache)

    def shifted(rows, shift):
        return lax.ppermute(rows, "tp", [(t, (t + shift) % tp_count) for t in range(tp_count)])

    first_part, under_attend = pl.pallas_call(
        lambda *refs: attend_first_body(*refs, first=starts[1]),
        out_shape=(
            jax.ShapeDtypeStruct((seq_total, own_width + STATS), jnp.bfloat16),
            pltpu.VMEM((depth, share[1]), out_weight.dtype),
        ),
        in_specs=[vmem(), vmem(), vmem(), hbm()],
        out_specs=(vmem(), vmem()),
        scratch_shapes=[
            pltpu.VMEM((seq_total, own_width), jnp.float32),
            pltpu.SemaphoreType.DMA,
        ],
        compiler_params=pltpu.CompilerParams(vmem_limit_bytes=6 << 20),
        cost_estimate=pl.CostEstimate(flops=COVER, transcendentals=0, bytes_accessed=1 << 20),
        name="attend_first",
    )(bias, wide, cache, out_weight)
    asked = [shifted(wide, -d) for d in range(1, tp_count)]
    parts = [first_part]
    chunks = [under_prepare, under_attend]
    for d in range(1, tp_count):
        parts.append(shifted(attend(asked[d - 1], d), d))
    chunks.append(fetch(starts[2], share[2], parts[0]))
    block = jax.ShapeDtypeStruct((seq_rep, own_width + STATS), jnp.bfloat16)
    dealt = pl.pallas_call(
        lambda *refs: merge_body(*refs, sources=tp_count),
        out_shape=(block,) * kvb_count,
        in_specs=[vmem()] * tp_count,
        out_specs=(vmem(),) * kvb_count,
        compiler_params=pltpu.CompilerParams(vmem_limit_bytes=4 << 20),
        name="merge",
    )(*parts)
    parts = [dealt[0]] + [
        lax.ppermute(dealt[r], "kvb", [(k, (k - r) % kvb_count) for k in range(kvb_count)])
        for r in range(1, kvb_count)
    ]
    chunks.append(fetch(starts[3], share[3], dealt[0]))
    projected = pl.pallas_call(
        lambda *refs: project_body(*refs, sources=kvb_count),
        out_shape=jax.ShapeDtypeStruct((seq_rep, out_weight.shape[1]), jnp.bfloat16),
        in_specs=[vmem()] * (kvb_count + 2) + [hbm()] + [vmem()] * len(chunks),
        out_specs=vmem(),
        scratch_shapes=[
            pltpu.VMEM((depth, share[4]), out_weight.dtype),
            pltpu.SemaphoreType.DMA,
            pltpu.VMEM((seq_rep, own_width), jnp.bfloat16),
        ],
        compiler_params=pltpu.CompilerParams(vmem_limit_bytes=12 << 20),
        name="project",
    )(*parts, fresh, fresh_values, out_weight, *chunks)
    pieces = lax.all_gather(projected, "tp", axis=0, tiled=False)
    own = jax.ShapeDtypeStruct((seq_rep, norm_gain.shape[0]), jnp.bfloat16)
    return pl.pallas_call(
        finish_body,
        out_shape=(own, own),
        in_specs=[vmem(), vmem(), vmem()],
        out_specs=(vmem(), vmem()),
        compiler_params=pltpu.CompilerParams(vmem_limit_bytes=4 << 20),
        name="finish",
    )(pieces, residual, norm_gain[None])


def solution(mesh):
    placed = (
        P(("groups", "kvb"), None),
        P(("groups", "kvb"), "tp"),
        P(("groups", "kvb"), None),
        P(("groups", "kvb", "tp"), None, None),
        P("groups"),
        P(("groups", "kvb", "tp")),
        P(("groups", "kvb", "tp")),
        P(("groups", "kvb", "tp")),
        P("tp", None),
        P("tp"),
    )
    return jax.shard_map(
        on_device,
        mesh=mesh,
        in_specs=placed,
        out_specs=(P(("groups", "kvb"), "tp"), P(("groups", "kvb"), "tp")),
        check_vma=False,
    )
```

```python
import jax
import jax.numpy as jnp
from jax import lax
from jax.experimental import pallas as pl
from jax.experimental.pallas import tpu as pltpu
from jax.sharding import PartitionSpec as P

QH = 64
KVH = 8
HD = 128
BLK = 16

MASKED = -1e30
FLOOR = -1e20
EPSILON = 1e-06
UNIT = HD ** (-0.5) * 1.4426950408889634
STATS = 128
COVER = 20_000_000_000
SHARES = (4, 4, 4, 9, 11)
LATE = (4, 4, 3)
STEP = 512


def once(body):
    trips = jnp.where(lax.axis_index("tp") >= 0, 1, 0)

    def trip(_, carried):
        body()
        return carried

    lax.fori_loop(0, trips, trip, 0)


def beside(weight, chunk, arrived, first, body):
    copy = pltpu.make_async_copy(weight.at[:, pl.ds(first, chunk.shape[1])], chunk, arrived)
    copy.start()
    once(body)
    copy.wait()


def prepare_body(count, *refs, first):
    inputs, weight, outs, chunk = refs[:5], refs[5], refs[6:10], refs[10]
    held, arrived, landed = refs[11:16], refs[16], refs[17]
    copies = [
        pltpu.make_async_copy(source, target, arrived.at[n])
        for n, (source, target) in enumerate(zip(inputs, held))
    ]
    for copy in copies:
        copy.start()

    def run():
        for copy in copies:
            copy.wait()
        prepare(count, *held, *outs)

    beside(weight, chunk, landed, first, run)


def prepare(
    count, lengths, slot_seq, slot_block, queries, new_kv, bias, fresh_out, value_out, own_out
):
    seq_total, tokens = bias.shape
    slots = tokens // BLK
    seq_rep, own_width = queries.shape
    local_heads = own_width // HD
    group_size = QH // KVH
    kvb_count = seq_total // seq_rep
    seq = slot_seq[...]
    length_of = jnp.zeros_like(seq)
    for s in range(seq_total):
        length_of = jnp.where(seq == s, lengths[s], length_of)
    slot_ids = lax.broadcasted_iota(jnp.int32, seq.shape, 1)
    remaining = jnp.clip(length_of - slot_block[...] * BLK, 0, BLK)
    remaining = jnp.where(slot_ids < count[0], remaining, 0)
    row = lax.broadcasted_iota(jnp.int32, (8, slots), 0)
    codes = jnp.where(row == 0, seq, jnp.where(row == 1, remaining, 0))
    spread = (
        lax.broadcasted_iota(jnp.int32, (slots, tokens), 1) // BLK
        == lax.broadcasted_iota(jnp.int32, (slots, tokens), 0)
    )
    per_token = jnp.dot(
        codes.astype(jnp.float32).astype(jnp.bfloat16),
        jnp.where(spread, 1.0, 0.0).astype(jnp.bfloat16),
        preferred_element_type=jnp.float32,
    )
    row = lax.broadcasted_iota(jnp.int32, (seq_total, tokens), 0)
    replica = lax.axis_index("kvb") - row // seq_rep
    replica = jnp.where(replica < 0, replica + kvb_count, replica)
    seq_ids = (replica * seq_rep + row % seq_rep).astype(jnp.float32)
    offsets = (lax.broadcasted_iota(jnp.int32, (seq_total, tokens), 1) % BLK).astype(jnp.float32)
    live = (per_token[0:1] == seq_ids) & (offsets < per_token[1:2])
    bias[...] = jnp.where(live, 0.0, MASKED)

    own_out[...] = queries[...]
    kv_local = max(1, local_heads // group_size)
    kv_first = lax.axis_index("tp") * local_heads // group_size
    lane = lax.broadcasted_iota(jnp.int32, (seq_rep, STATS), 1)
    fresh = jnp.zeros((seq_rep, STATS), jnp.float32)
    for v in range(kv_local):
        at = pl.multiple_of((kv_first + v) * HD, HD)
        key = new_kv[:, pl.ds(at, HD)].astype(jnp.float32)
        at = pl.multiple_of((KVH + kv_first + v) * HD, HD)
        value_out[:, v * HD : (v + 1) * HD] = new_kv[:, pl.ds(at, HD)].astype(jnp.float32)
        for h in range(v * local_heads // kv_local, (v + 1) * local_heads // kv_local):
            query = queries[:, h * HD : (h + 1) * HD].astype(jnp.float32)
            score = jnp.sum(query * key, axis=1, keepdims=True)
            fresh = jnp.where(lane == h, score, fresh)
    fresh_out[...] = fresh * UNIT


def attend_first_body(bias_ref, queries, cache, weight, out, chunk, stacked, arrived, *, first):
    run = lambda: attend_body(bias_ref, queries, cache, out, stacked, shift=0)
    beside(weight, chunk, arrived, first, run)


def attend_body(bias_ref, queries, cache, out, stacked, *, shift):
    kvb_count, seq_rep, own_width = queries.shape
    tp_count = lax.axis_size("tp")
    tokens = cache.shape[0] * BLK
    seq_total = kvb_count * seq_rep
    local_heads = own_width // HD
    group_size = QH // KVH
    kv_local = max(1, local_heads // group_size)
    per_kv = local_heads // kv_local
    bias = bias_ref[...]
    for r in range(kvb_count):
        stacked[r * seq_rep : (r + 1) * seq_rep, :] = queries[r].astype(jnp.float32)
    t = lax.axis_index("tp") + shift
    t = jnp.where(t < tp_count, t, t - tp_count)
    lane = lax.broadcasted_iota(jnp.int32, (seq_total, STATS), 1)
    stats = jnp.zeros((seq_total, STATS), jnp.float32)
    for v in range(kv_local):
        heads = range(v * per_kv, (v + 1) * per_kv)
        rows = jnp.concatenate(
            [stacked[:, h * HD : (h + 1) * HD] for h in heads], axis=0
        ).astype(jnp.bfloat16)
        g = t * local_heads // group_size + v
        at = pl.multiple_of(g * HD, HD)
        keys = cache[:, :, pl.ds(at, HD)].reshape(tokens, HD)
        at = pl.multiple_of((KVH + g) * HD, HD)
        values = cache[:, :, pl.ds(at, HD)].reshape(tokens, HD)
        scores = lax.dot_general(
            rows, keys, (((1,), (1,)), ((), ())), preferred_element_type=jnp.float32
        )
        scores = scores.reshape(per_kv, seq_total, tokens) * UNIT + bias[None]
        peaks = jnp.maximum(jnp.max(scores, axis=2, keepdims=True), FLOOR)
        peaks = peaks.astype(jnp.bfloat16).astype(jnp.float32)
        weights = jnp.exp2(scores - peaks)
        sums = jnp.sum(weights, axis=2, keepdims=True)
        partial = jnp.dot(
            weights.astype(jnp.bfloat16).reshape(per_kv * seq_total, tokens),
            values,
            preferred_element_type=jnp.float32,
        )
        high = sums.astype(jnp.bfloat16).astype(jnp.float32)
        low = sums - high
        for j, h in enumerate(heads):
            out[:, h * HD : (h + 1) * HD] = partial[j * seq_total : (j + 1) * seq_total].astype(
                jnp.bfloat16
            )
            for part, value in enumerate((peaks, high, low)):
                stats = jnp.where(lane == part * local_heads + h, value[j], stats)
    out[:, local_heads * HD :] = stats.astype(jnp.bfloat16)


def fetch_body(weight, *refs, first):
    chunk, arrived = refs[-2:]
    copy = pltpu.make_async_copy(weight.at[:, pl.ds(first, chunk.shape[1])], chunk, arrived)
    copy.start()
    copy.wait()


def unpack(ref, local_heads):
    stats = ref[:, local_heads * HD :].astype(jnp.float32)
    sums = stats[:, local_heads : 2 * local_heads] + stats[:, 2 * local_heads : 3 * local_heads]
    return stats[:, :local_heads], sums


def merge_body(*refs, sources):
    parts, outs = refs[:sources], refs[sources:]
    seq_total, width = parts[0].shape
    seq_rep = outs[0].shape[0]
    local_heads = (width - STATS) // HD
    pairs = [unpack(part, local_heads) for part in parts]
    peak = pairs[0][0]
    for other, _ in pairs[1:]:
        peak = jnp.maximum(peak, other)
    scaling = [jnp.exp2(p - peak) for p, _ in pairs]
    total = sum(s * c for s, (_, c) in zip(scaling, pairs))
    high = total.astype(jnp.bfloat16).astype(jnp.float32)
    pad = jnp.zeros((seq_total, STATS - 3 * local_heads), jnp.float32)
    stats = jnp.concatenate([peak, high, total - high, pad], axis=1)
    blocks = [
        sum(
            s[:, h : h + 1] * part[:, h * HD : (h + 1) * HD].astype(jnp.float32)
            for s, part in zip(scaling, parts)
        )
        for h in range(local_heads)
    ]
    for h, block in enumerate(blocks + [stats]):
        for r, out in enumerate(outs):
            out[:, h * HD : (h + 1) * HD] = block[r * seq_rep : (r + 1) * seq_rep].astype(
                jnp.bfloat16
            )


def project_body(*refs, sources):
    parts = refs[:sources]
    fresh_ref, value_ref, weight = refs[sources : sources + 3]
    pieces = len(LATE)
    chunks = list(refs[sources + 3 : -3 - pieces])
    out, *late = refs[-3 - pieces : -2]
    arrived, rows = refs[-2:]
    first = weight.shape[1] - sum(piece.shape[1] for piece in late)
    copies = []
    for n, piece in enumerate(late):
        columns = pl.ds(first, piece.shape[1])
        copies.append(pltpu.make_async_copy(weight.at[:, columns], piece, arrived.at[n]))
        copies[-1].start()
        first += piece.shape[1]
    def combine():
        local_heads = (parts[0].shape[1] - STATS) // HD
        kv_local = value_ref.shape[1] // HD
        pairs = [unpack(part, local_heads) for part in parts]
        fresh = fresh_ref[:, :local_heads]
        overall = fresh
        for peak, _ in pairs:
            overall = jnp.maximum(overall, peak)
        scaling = [jnp.exp2(peak - overall) for peak, _ in pairs]
        fresh_weight = jnp.exp2(fresh - overall)
        inverse = 1.0 / (fresh_weight + sum(s * c for s, (_, c) in zip(scaling, pairs)))
        scaling = [s * inverse for s in scaling]
        fresh_weight = fresh_weight * inverse
        attended = []
        for h in range(local_heads):
            v = h * kv_local // local_heads
            total = fresh_weight[:, h : h + 1] * value_ref[:, v * HD : (v + 1) * HD]
            for s, part in zip(scaling, parts):
                total = total + s[:, h : h + 1] * part[:, h * HD : (h + 1) * HD].astype(jnp.float32)
            attended.append(total.astype(jnp.bfloat16))
        rows[...] = jnp.concatenate(attended, axis=1)

    once(combine)
    attended = rows[...]
    first = 0
    for n, chunk in enumerate(chunks + late):
        if n >= len(chunks):
            copies[n - len(chunks)].wait()
        for at in range(0, chunk.shape[1], STEP):
            step = min(STEP, chunk.shape[1] - at)
            out[:, first + at : first + at + step] = jnp.dot(
                attended, chunk[:, at : at + step], preferred_element_type=jnp.float32
            ).astype(out.dtype)
        first += chunk.shape[1]


def finish_body(pieces, residual, gain, stream_out, normed_out):
    full = residual[...].astype(jnp.float32)
    width = full.shape[1]
    total = pieces[0].astype(jnp.float32)
    for t in range(1, pieces.shape[0]):
        total = total + pieces[t].astype(jnp.float32)
    full = (full + total).astype(jnp.bfloat16).astype(jnp.float32)
    mean_square = jnp.sum(full * full, axis=1, keepdims=True) / width
    inverse = lax.rsqrt(mean_square + EPSILON)
    own = stream_out.shape[1]
    at = pl.multiple_of(lax.axis_index("tp") * own, own)
    mine = residual[:, pl.ds(at, own)].astype(jnp.float32)
    total = pieces[0, :, pl.ds(at, own)].astype(jnp.float32)
    for t in range(1, pieces.shape[0]):
        total = total + pieces[t, :, pl.ds(at, own)].astype(jnp.float32)
    stream = (mine + total).astype(jnp.bfloat16)
    stream_out[...] = stream
    normed_out[...] = (stream.astype(jnp.float32) * inverse * gain[...].astype(jnp.float32)).astype(
        jnp.bfloat16
    )


def vmem():
    return pl.BlockSpec(memory_space=pltpu.VMEM)


def resident(array):
    return pltpu.with_memory_space_constraint(array, pltpu.VMEM)


def hbm():
    return pl.BlockSpec(memory_space=pltpu.HBM)


def on_device(
    residual,
    queries,
    new_kv,
    kv_cache,
    lengths,
    slot_seq,
    slot_block,
    block_counts,
    out_weight,
    norm_gain,
):
    tp_count = lax.axis_size("tp")
    kvb_count = lax.axis_size("kvb")
    seq_rep, own_width = queries.shape
    seq_total = kvb_count * seq_rep
    tokens = kv_cache.shape[0] * BLK
    kv_local = max(1, own_width // HD * KVH // QH)
    depth, columns = out_weight.shape
    out_weight = pltpu.with_memory_space_constraint(out_weight, pltpu.HBM)
    share = [columns * n // sum(SHARES) for n in SHARES]
    starts = [sum(share[:n]) for n in range(len(share))]
    arrived = [
        lax.ppermute(queries, "kvb", [(k, (k + r) % kvb_count) for k in range(kvb_count)])
        for r in range(1, kvb_count)
    ]
    bias, fresh, fresh_values, own_queries, under_prepare = pl.pallas_call(
        lambda *refs: prepare_body(*refs, first=starts[0]),
        out_shape=(
            jax.ShapeDtypeStruct((seq_total, tokens), jnp.float32),
            jax.ShapeDtypeStruct((seq_rep, STATS), jnp.float32),
            jax.ShapeDtypeStruct((seq_rep, kv_local * HD), jnp.float32),
            jax.ShapeDtypeStruct((seq_rep, own_width), jnp.bfloat16),
            pltpu.VMEM((depth, share[0]), out_weight.dtype),
        ),
        in_specs=[pl.BlockSpec(memory_space=pltpu.SMEM)] + [hbm()] * 6,
        out_specs=(vmem(),) * 5,
        scratch_shapes=[
            pltpu.SMEM(lengths.shape, jnp.int32),
            pltpu.VMEM((1,) + slot_seq.shape, jnp.int32),
            pltpu.VMEM((1,) + slot_block.shape, jnp.int32),
            pltpu.VMEM(queries.shape, queries.dtype),
            pltpu.VMEM(new_kv.shape, new_kv.dtype),
            pltpu.SemaphoreType.DMA((5,)),
            pltpu.SemaphoreType.DMA,
        ],
        compiler_params=pltpu.CompilerParams(vmem_limit_bytes=4 << 20),
        cost_estimate=pl.CostEstimate(flops=COVER, transcendentals=0, bytes_accessed=1 << 20),
        name="prepare",
    )(block_counts, *[
        pltpu.with_memory_space_constraint(array, pltpu.HBM)
        for array in (lengths, slot_seq[None], slot_block[None], queries, new_kv)
    ], out_weight)
    wide = jnp.stack([own_queries] + arrived)
    cache = resident(kv_cache)

    def fetch(first, size, *after):
        return pl.pallas_call(
            lambda *refs: fetch_body(*refs, first=first),
            out_shape=pltpu.VMEM((depth, size), out_weight.dtype),
            in_specs=[hbm()] + [pl.BlockSpec(memory_space=pl.ANY)] * len(after),
            out_specs=vmem(),
            scratch_shapes=[pltpu.SemaphoreType.DMA],
            compiler_params=pltpu.CompilerParams(vmem_limit_bytes=1 << 20),
            cost_estimate=pl.CostEstimate(flops=COVER, transcendentals=0, bytes_accessed=1 << 20),
            name="fetch",
        )(out_weight, *after)

    def attend(rows, shift):
        return pl.pallas_call(
            lambda *refs: attend_body(*refs, shift=shift),
            out_shape=jax.ShapeDtypeStruct((seq_total, own_width + STATS), jnp.bfloat16),
            in_specs=[vmem(), vmem(), vmem()],
            out_specs=vmem(),
            scratch_shapes=[pltpu.VMEM((seq_total, own_width), jnp.float32)],
            compiler_params=pltpu.CompilerParams(vmem_limit_bytes=6 << 20),
            cost_estimate=pl.CostEstimate(flops=COVER, transcendentals=0, bytes_accessed=1 << 20),
            name="attend",
        )(bias, rows, cache)

    def shifted(rows, shift):
        return lax.ppermute(rows, "tp", [(t, (t + shift) % tp_count) for t in range(tp_count)])

    first_part, under_attend = pl.pallas_call(
        lambda *refs: attend_first_body(*refs, first=starts[1]),
        out_shape=(
            jax.ShapeDtypeStruct((seq_total, own_width + STATS), jnp.bfloat16),
            pltpu.VMEM((depth, share[1]), out_weight.dtype),
        ),
        in_specs=[vmem(), vmem(), vmem(), hbm()],
        out_specs=(vmem(), vmem()),
        scratch_shapes=[
            pltpu.VMEM((seq_total, own_width), jnp.float32),
            pltpu.SemaphoreType.DMA,
        ],
        compiler_params=pltpu.CompilerParams(vmem_limit_bytes=6 << 20),
        cost_estimate=pl.CostEstimate(flops=COVER, transcendentals=0, bytes_accessed=1 << 20),
        name="attend_first",
    )(bias, wide, cache, out_weight)
    asked = [shifted(wide, -d) for d in range(1, tp_count)]
    parts = [first_part]
    chunks = [under_prepare, under_attend]
    for d in range(1, tp_count):
        parts.append(shifted(attend(asked[d - 1], d), d))
    chunks.append(fetch(starts[2], share[2], parts[0]))
    block = jax.ShapeDtypeStruct((seq_rep, own_width + STATS), jnp.bfloat16)
    dealt = pl.pallas_call(
        lambda *refs: merge_body(*refs, sources=tp_count),
        out_shape=(block,) * kvb_count,
        in_specs=[vmem()] * tp_count,
        out_specs=(vmem(),) * kvb_count,
        compiler_params=pltpu.CompilerParams(vmem_limit_bytes=4 << 20),
        name="merge",
    )(*parts)
    parts = [dealt[0]] + [
        lax.ppermute(dealt[r], "kvb", [(k, (k - r) % kvb_count) for k in range(kvb_count)])
        for r in range(1, kvb_count)
    ]
    chunks.append(fetch(starts[3], share[3], dealt[0]))
    projected = pl.pallas_call(
        lambda *refs: project_body(*refs, sources=kvb_count),
        out_shape=jax.ShapeDtypeStruct((seq_rep, out_weight.shape[1]), jnp.bfloat16),
        in_specs=[vmem()] * (kvb_count + 2) + [hbm()] + [vmem()] * len(chunks),
        out_specs=vmem(),
        scratch_shapes=[
            *[pltpu.VMEM((depth, share[4] * n // sum(LATE)), out_weight.dtype) for n in LATE],
            pltpu.SemaphoreType.DMA((len(LATE),)),
            pltpu.VMEM((seq_rep, own_width), jnp.bfloat16),
        ],
        compiler_params=pltpu.CompilerParams(vmem_limit_bytes=12 << 20),
        name="project",
    )(*parts, fresh, fresh_values, out_weight, *chunks)
    pieces = lax.all_gather(projected, "tp", axis=0, tiled=False)
    own = jax.ShapeDtypeStruct((seq_rep, norm_gain.shape[0]), jnp.bfloat16)
    return pl.pallas_call(
        finish_body,
        out_shape=(own, own),
        in_specs=[vmem(), vmem(), vmem()],
        out_specs=(vmem(), vmem()),
        compiler_params=pltpu.CompilerParams(vmem_limit_bytes=4 << 20),
        name="finish",
    )(pieces, residual, norm_gain[None])


def solution(mesh):
    placed = (
        P(("groups", "kvb"), None),
        P(("groups", "kvb"), "tp"),
        P(("groups", "kvb"), None),
        P(("groups", "kvb", "tp"), None, None),
        P("groups"),
        P(("groups", "kvb", "tp")),
        P(("groups", "kvb", "tp")),
        P(("groups", "kvb", "tp")),
        P("tp", None),
        P("tp"),
    )
    return jax.shard_map(
        on_device,
        mesh=mesh,
        in_specs=placed,
        out_specs=(P(("groups", "kvb"), "tp"), P(("groups", "kvb"), "tp")),
        check_vma=False,
    )
```

```python
import jax
import jax.numpy as jnp
from jax import lax
from jax.experimental import pallas as pl
from jax.experimental.pallas import tpu as pltpu
from jax.sharding import PartitionSpec as P

QH = 64
KVH = 8
HD = 128
BLK = 16

MASKED = -1e30
FLOOR = -1e20
EPSILON = 1e-06
UNIT = HD ** (-0.5) * 1.4426950408889634
STATS = 128
COVER = 20_000_000_000
SHARES = (4, 5, 10, 13)
LATE = (4, 4, 3, 2)
STEP = 512


def once(body):
    trips = jnp.where(lax.axis_index("tp") >= 0, 1, 0)

    def trip(_, carried):
        body()
        return carried

    lax.fori_loop(0, trips, trip, 0)


def beside(weight, chunk, arrived, first, body):
    copy = pltpu.make_async_copy(weight.at[:, pl.ds(first, chunk.shape[1])], chunk, arrived)
    copy.start()
    once(body)
    copy.wait()


def prepare_body(count, *refs, first):
    inputs, weight, outs, chunk = refs[:5], refs[5], refs[6:10], refs[10]
    held, arrived, landed = refs[11:16], refs[16], refs[17]
    copies = [
        pltpu.make_async_copy(source, target, arrived.at[n])
        for n, (source, target) in enumerate(zip(inputs, held))
    ]
    for copy in copies:
        copy.start()

    def run():
        for copy in copies:
            copy.wait()
        prepare(count, *held, *outs)

    beside(weight, chunk, landed, first, run)


def prepare(
    count, lengths, slot_seq, slot_block, queries, new_kv, bias, fresh_out, value_out, own_out
):
    seq_total, tokens = bias.shape
    slots = tokens // BLK
    seq_rep, own_width = queries.shape
    local_heads = own_width // HD
    group_size = QH // KVH
    kvb_count = seq_total // seq_rep
    seq = slot_seq[...]
    length_of = jnp.zeros_like(seq)
    for s in range(seq_total):
        length_of = jnp.where(seq == s, lengths[s], length_of)
    slot_ids = lax.broadcasted_iota(jnp.int32, seq.shape, 1)
    remaining = jnp.clip(length_of - slot_block[...] * BLK, 0, BLK)
    remaining = jnp.where(slot_ids < count[0], remaining, 0)
    row = lax.broadcasted_iota(jnp.int32, (8, slots), 0)
    codes = jnp.where(row == 0, seq, jnp.where(row == 1, remaining, 0))
    spread = (
        lax.broadcasted_iota(jnp.int32, (slots, tokens), 1) // BLK
        == lax.broadcasted_iota(jnp.int32, (slots, tokens), 0)
    )
    per_token = jnp.dot(
        codes.astype(jnp.float32).astype(jnp.bfloat16),
        jnp.where(spread, 1.0, 0.0).astype(jnp.bfloat16),
        preferred_element_type=jnp.float32,
    )
    row = lax.broadcasted_iota(jnp.int32, (seq_total, tokens), 0)
    replica = lax.axis_index("kvb") - row // seq_rep
    replica = jnp.where(replica < 0, replica + kvb_count, replica)
    seq_ids = (replica * seq_rep + row % seq_rep).astype(jnp.float32)
    offsets = (lax.broadcasted_iota(jnp.int32, (seq_total, tokens), 1) % BLK).astype(jnp.float32)
    live = (per_token[0:1] == seq_ids) & (offsets < per_token[1:2])
    bias[...] = jnp.where(live, 0.0, MASKED)

    own_out[...] = queries[...]
    kv_local = max(1, local_heads // group_size)
    kv_first = lax.axis_index("tp") * local_heads // group_size
    lane = lax.broadcasted_iota(jnp.int32, (seq_rep, STATS), 1)
    fresh = jnp.zeros((seq_rep, STATS), jnp.float32)
    for v in range(kv_local):
        at = pl.multiple_of((kv_first + v) * HD, HD)
        key = new_kv[:, pl.ds(at, HD)].astype(jnp.float32)
        at = pl.multiple_of((KVH + kv_first + v) * HD, HD)
        value_out[:, v * HD : (v + 1) * HD] = new_kv[:, pl.ds(at, HD)].astype(jnp.float32)
        for h in range(v * local_heads // kv_local, (v + 1) * local_heads // kv_local):
            query = queries[:, h * HD : (h + 1) * HD].astype(jnp.float32)
            score = jnp.sum(query * key, axis=1, keepdims=True)
            fresh = jnp.where(lane == h, score, fresh)
    fresh_out[...] = fresh * UNIT


def attend_body(bias_ref, queries, cache, out, stacked, *, shift):
    kvb_count, seq_rep, own_width = queries.shape
    tp_count = lax.axis_size("tp")
    tokens = cache.shape[0] * BLK
    seq_total = kvb_count * seq_rep
    local_heads = own_width // HD
    group_size = QH // KVH
    kv_local = max(1, local_heads // group_size)
    per_kv = local_heads // kv_local
    bias = bias_ref[...]
    for r in range(kvb_count):
        stacked[r * seq_rep : (r + 1) * seq_rep, :] = queries[r].astype(jnp.float32)
    t = lax.axis_index("tp") + shift
    t = jnp.where(t < tp_count, t, t - tp_count)
    lane = lax.broadcasted_iota(jnp.int32, (seq_total, STATS), 1)
    stats = jnp.zeros((seq_total, STATS), jnp.float32)
    for v in range(kv_local):
        heads = range(v * per_kv, (v + 1) * per_kv)
        rows = jnp.concatenate(
            [stacked[:, h * HD : (h + 1) * HD] for h in heads], axis=0
        ).astype(jnp.bfloat16)
        g = t * local_heads // group_size + v
        at = pl.multiple_of(g * HD, HD)
        keys = cache[:, :, pl.ds(at, HD)].reshape(tokens, HD)
        at = pl.multiple_of((KVH + g) * HD, HD)
        values = cache[:, :, pl.ds(at, HD)].reshape(tokens, HD)
        scores = lax.dot_general(
            rows, keys, (((1,), (1,)), ((), ())), preferred_element_type=jnp.float32
        )
        scores = scores.reshape(per_kv, seq_total, tokens) * UNIT + bias[None]
        peaks = jnp.maximum(jnp.max(scores, axis=2, keepdims=True), FLOOR)
        peaks = peaks.astype(jnp.bfloat16).astype(jnp.float32)
        weights = jnp.exp2(scores - peaks)
        sums = jnp.sum(weights, axis=2, keepdims=True)
        partial = jnp.dot(
            weights.astype(jnp.bfloat16).reshape(per_kv * seq_total, tokens),
            values,
            preferred_element_type=jnp.float32,
        )
        high = sums.astype(jnp.bfloat16).astype(jnp.float32)
        low = sums - high
        for j, h in enumerate(heads):
            out[:, h * HD : (h + 1) * HD] = partial[j * seq_total : (j + 1) * seq_total].astype(
                jnp.bfloat16
            )
            for part, value in enumerate((peaks, high, low)):
                stats = jnp.where(lane == part * local_heads + h, value[j], stats)
    out[:, local_heads * HD :] = stats.astype(jnp.bfloat16)


def fetch_body(weight, *refs, first):
    chunk, arrived = refs[-2:]
    copy = pltpu.make_async_copy(weight.at[:, pl.ds(first, chunk.shape[1])], chunk, arrived)
    copy.start()
    copy.wait()


def unpack(ref, local_heads):
    stats = ref[:, local_heads * HD :].astype(jnp.float32)
    sums = stats[:, local_heads : 2 * local_heads] + stats[:, 2 * local_heads : 3 * local_heads]
    return stats[:, :local_heads], sums


def merge_body(*refs, sources):
    parts, outs = refs[:sources], refs[sources:]
    seq_total, width = parts[0].shape
    seq_rep = outs[0].shape[0]
    local_heads = (width - STATS) // HD
    pairs = [unpack(part, local_heads) for part in parts]
    peak = pairs[0][0]
    for other, _ in pairs[1:]:
        peak = jnp.maximum(peak, other)
    scaling = [jnp.exp2(p - peak) for p, _ in pairs]
    total = sum(s * c for s, (_, c) in zip(scaling, pairs))
    high = total.astype(jnp.bfloat16).astype(jnp.float32)
    pad = jnp.zeros((seq_total, STATS - 3 * local_heads), jnp.float32)
    stats = jnp.concatenate([peak, high, total - high, pad], axis=1)
    blocks = [
        sum(
            s[:, h : h + 1] * part[:, h * HD : (h + 1) * HD].astype(jnp.float32)
            for s, part in zip(scaling, parts)
        )
        for h in range(local_heads)
    ]
    for h, block in enumerate(blocks + [stats]):
        for r, out in enumerate(outs):
            out[:, h * HD : (h + 1) * HD] = block[r * seq_rep : (r + 1) * seq_rep].astype(
                jnp.bfloat16
            )


def project_body(*refs, sources):
    parts = refs[:sources]
    fresh_ref, value_ref, weight = refs[sources : sources + 3]
    pieces = len(LATE)
    chunks = list(refs[sources + 3 : -3 - pieces])
    out, *late = refs[-3 - pieces : -2]
    arrived, rows = refs[-2:]
    first = weight.shape[1] - sum(piece.shape[1] for piece in late)
    copies = []
    for n, piece in enumerate(late):
        columns = pl.ds(first, piece.shape[1])
        copies.append(pltpu.make_async_copy(weight.at[:, columns], piece, arrived.at[n]))
        copies[-1].start()
        first += piece.shape[1]
    def combine():
        local_heads = (parts[0].shape[1] - STATS) // HD
        kv_local = value_ref.shape[1] // HD
        pairs = [unpack(part, local_heads) for part in parts]
        fresh = fresh_ref[:, :local_heads]
        overall = fresh
        for peak, _ in pairs:
            overall = jnp.maximum(overall, peak)
        scaling = [jnp.exp2(peak - overall) for peak, _ in pairs]
        fresh_weight = jnp.exp2(fresh - overall)
        inverse = 1.0 / (fresh_weight + sum(s * c for s, (_, c) in zip(scaling, pairs)))
        scaling = [s * inverse for s in scaling]
        fresh_weight = fresh_weight * inverse
        attended = []
        for h in range(local_heads):
            v = h * kv_local // local_heads
            total = fresh_weight[:, h : h + 1] * value_ref[:, v * HD : (v + 1) * HD]
            for s, part in zip(scaling, parts):
                total = total + s[:, h : h + 1] * part[:, h * HD : (h + 1) * HD].astype(jnp.float32)
            attended.append(total.astype(jnp.bfloat16))
        rows[...] = jnp.concatenate(attended, axis=1)

    once(combine)
    attended = rows[...]
    first = 0
    for n, chunk in enumerate(chunks + late):
        if n >= len(chunks):
            copies[n - len(chunks)].wait()
        for at in range(0, chunk.shape[1], STEP):
            step = min(STEP, chunk.shape[1] - at)
            out[:, first + at : first + at + step] = jnp.dot(
                attended, chunk[:, at : at + step], preferred_element_type=jnp.float32
            ).astype(out.dtype)
        first += chunk.shape[1]


def finish_body(pieces, residual, gain, stream_out, normed_out):
    full = residual[...].astype(jnp.float32)
    width = full.shape[1]
    total = pieces[0].astype(jnp.float32)
    for t in range(1, pieces.shape[0]):
        total = total + pieces[t].astype(jnp.float32)
    full = (full + total).astype(jnp.bfloat16).astype(jnp.float32)
    mean_square = jnp.sum(full * full, axis=1, keepdims=True) / width
    inverse = lax.rsqrt(mean_square + EPSILON)
    own = stream_out.shape[1]
    at = pl.multiple_of(lax.axis_index("tp") * own, own)
    mine = residual[:, pl.ds(at, own)].astype(jnp.float32)
    total = pieces[0, :, pl.ds(at, own)].astype(jnp.float32)
    for t in range(1, pieces.shape[0]):
        total = total + pieces[t, :, pl.ds(at, own)].astype(jnp.float32)
    stream = (mine + total).astype(jnp.bfloat16)
    stream_out[...] = stream
    normed_out[...] = (stream.astype(jnp.float32) * inverse * gain[...].astype(jnp.float32)).astype(
        jnp.bfloat16
    )


def vmem():
    return pl.BlockSpec(memory_space=pltpu.VMEM)


def resident(array):
    return pltpu.with_memory_space_constraint(array, pltpu.VMEM)


def hbm():
    return pl.BlockSpec(memory_space=pltpu.HBM)


def on_device(
    residual,
    queries,
    new_kv,
    kv_cache,
    lengths,
    slot_seq,
    slot_block,
    block_counts,
    out_weight,
    norm_gain,
):
    tp_count = lax.axis_size("tp")
    kvb_count = lax.axis_size("kvb")
    seq_rep, own_width = queries.shape
    seq_total = kvb_count * seq_rep
    tokens = kv_cache.shape[0] * BLK
    kv_local = max(1, own_width // HD * KVH // QH)
    depth, columns = out_weight.shape
    out_weight = pltpu.with_memory_space_constraint(out_weight, pltpu.HBM)
    share = [columns * n // sum(SHARES) for n in SHARES]
    starts = [sum(share[:n]) for n in range(len(share))]
    arrived = [
        lax.ppermute(queries, "kvb", [(k, (k + r) % kvb_count) for k in range(kvb_count)])
        for r in range(1, kvb_count)
    ]
    bias, fresh, fresh_values, own_queries, under_prepare = pl.pallas_call(
        lambda *refs: prepare_body(*refs, first=starts[0]),
        out_shape=(
            jax.ShapeDtypeStruct((seq_total, tokens), jnp.float32),
            jax.ShapeDtypeStruct((seq_rep, STATS), jnp.float32),
            jax.ShapeDtypeStruct((seq_rep, kv_local * HD), jnp.float32),
            jax.ShapeDtypeStruct((seq_rep, own_width), jnp.bfloat16),
            pltpu.VMEM((depth, share[0]), out_weight.dtype),
        ),
        in_specs=[pl.BlockSpec(memory_space=pltpu.SMEM)] + [hbm()] * 6,
        out_specs=(vmem(),) * 5,
        scratch_shapes=[
            pltpu.SMEM(lengths.shape, jnp.int32),
            pltpu.VMEM((1,) + slot_seq.shape, jnp.int32),
            pltpu.VMEM((1,) + slot_block.shape, jnp.int32),
            pltpu.VMEM(queries.shape, queries.dtype),
            pltpu.VMEM(new_kv.shape, new_kv.dtype),
            pltpu.SemaphoreType.DMA((5,)),
            pltpu.SemaphoreType.DMA,
        ],
        compiler_params=pltpu.CompilerParams(vmem_limit_bytes=4 << 20),
        cost_estimate=pl.CostEstimate(flops=COVER, transcendentals=0, bytes_accessed=1 << 20),
        name="prepare",
    )(block_counts, *[
        pltpu.with_memory_space_constraint(array, pltpu.HBM)
        for array in (lengths, slot_seq[None], slot_block[None], queries, new_kv)
    ], out_weight)
    wide = jnp.stack([own_queries] + arrived)
    cache = resident(kv_cache)

    def fetch(first, size, *after):
        return pl.pallas_call(
            lambda *refs: fetch_body(*refs, first=first),
            out_shape=pltpu.VMEM((depth, size), out_weight.dtype),
            in_specs=[hbm()] + [pl.BlockSpec(memory_space=pl.ANY)] * len(after),
            out_specs=vmem(),
            scratch_shapes=[pltpu.SemaphoreType.DMA],
            compiler_params=pltpu.CompilerParams(vmem_limit_bytes=1 << 20),
            cost_estimate=pl.CostEstimate(flops=COVER, transcendentals=0, bytes_accessed=1 << 20),
            name="fetch",
        )(out_weight, *after)

    def attend(rows, shift):
        return pl.pallas_call(
            lambda *refs: attend_body(*refs, shift=shift),
            out_shape=jax.ShapeDtypeStruct((seq_total, own_width + STATS), jnp.bfloat16),
            in_specs=[vmem(), vmem(), vmem()],
            out_specs=vmem(),
            scratch_shapes=[pltpu.VMEM((seq_total, own_width), jnp.float32)],
            compiler_params=pltpu.CompilerParams(vmem_limit_bytes=6 << 20),
            cost_estimate=pl.CostEstimate(flops=COVER, transcendentals=0, bytes_accessed=1 << 20),
            name="attend",
        )(bias, rows, cache)

    def shifted(rows, shift):
        return lax.ppermute(rows, "tp", [(t, (t + shift) % tp_count) for t in range(tp_count)])

    asked = [shifted(wide, -d) for d in range(1, tp_count)]
    parts = [attend(wide, 0)]
    chunks = [under_prepare]
    for d in range(1, tp_count):
        parts.append(shifted(attend(asked[d - 1], d), d))
    chunks.append(fetch(starts[1], share[1], parts[0]))
    block = jax.ShapeDtypeStruct((seq_rep, own_width + STATS), jnp.bfloat16)
    dealt = pl.pallas_call(
        lambda *refs: merge_body(*refs, sources=tp_count),
        out_shape=(block,) * kvb_count,
        in_specs=[vmem()] * tp_count,
        out_specs=(vmem(),) * kvb_count,
        compiler_params=pltpu.CompilerParams(vmem_limit_bytes=4 << 20),
        name="merge",
    )(*parts)
    parts = [dealt[0]] + [
        lax.ppermute(dealt[r], "kvb", [(k, (k - r) % kvb_count) for k in range(kvb_count)])
        for r in range(1, kvb_count)
    ]
    chunks.append(fetch(starts[2], share[2], dealt[0]))
    projected = pl.pallas_call(
        lambda *refs: project_body(*refs, sources=kvb_count),
        out_shape=jax.ShapeDtypeStruct((seq_rep, out_weight.shape[1]), jnp.bfloat16),
        in_specs=[vmem()] * (kvb_count + 2) + [hbm()] + [vmem()] * len(chunks),
        out_specs=vmem(),
        scratch_shapes=[
            *[pltpu.VMEM((depth, share[3] * n // sum(LATE)), out_weight.dtype) for n in LATE],
            pltpu.SemaphoreType.DMA((len(LATE),)),
            pltpu.VMEM((seq_rep, own_width), jnp.bfloat16),
        ],
        compiler_params=pltpu.CompilerParams(vmem_limit_bytes=18 << 20),
        name="project",
    )(*parts, fresh, fresh_values, out_weight, *chunks)
    pieces = lax.all_gather(projected, "tp", axis=0, tiled=False)
    own = jax.ShapeDtypeStruct((seq_rep, norm_gain.shape[0]), jnp.bfloat16)
    return pl.pallas_call(
        finish_body,
        out_shape=(own, own),
        in_specs=[vmem(), vmem(), vmem()],
        out_specs=(vmem(), vmem()),
        compiler_params=pltpu.CompilerParams(vmem_limit_bytes=4 << 20),
        name="finish",
    )(pieces, residual, norm_gain[None])


def solution(mesh):
    placed = (
        P(("groups", "kvb"), None),
        P(("groups", "kvb"), "tp"),
        P(("groups", "kvb"), None),
        P(("groups", "kvb", "tp"), None, None),
        P("groups"),
        P(("groups", "kvb", "tp")),
        P(("groups", "kvb", "tp")),
        P(("groups", "kvb", "tp")),
        P("tp", None),
        P("tp"),
    )
    return jax.shard_map(
        on_device,
        mesh=mesh,
        in_specs=placed,
        out_specs=(P(("groups", "kvb"), "tp"), P(("groups", "kvb"), "tp")),
        check_vma=False,
    )
```

```python
import jax
import jax.numpy as jnp
from jax import lax
from jax.experimental import pallas as pl
from jax.experimental.pallas import tpu as pltpu
from jax.sharding import PartitionSpec as P

QH = 64
KVH = 8
HD = 128
BLK = 16

MASKED = -1e30
FLOOR = -1e20
EPSILON = 1e-06
UNIT = HD ** (-0.5) * 1.4426950408889634
STATS = 128
COVER = 20_000_000_000
SHARES = (4, 5, 10, 13)
LATE = (4, 4, 3, 2)
STEP = 512


def ahead(index, step, count):
    if count & (count - 1) == 0:
        return index ^ step
    return (index + step) % count


def behind(index, step, count):
    if count & (count - 1) == 0:
        return index ^ step
    return (index - step + count) % count


def once(body):
    trips = jnp.where(lax.axis_index("tp") >= 0, 1, 0)

    def trip(_, carried):
        body()
        return carried

    lax.fori_loop(0, trips, trip, 0)


def beside(weight, chunk, arrived, first, body):
    copy = pltpu.make_async_copy(weight.at[:, pl.ds(first, chunk.shape[1])], chunk, arrived)
    copy.start()
    once(body)
    copy.wait()


def prepare_body(count, *refs, first):
    inputs, weight, outs, chunk = refs[:5], refs[5], refs[6:10], refs[10]
    held, arrived, landed = refs[11:16], refs[16], refs[17]
    copies = [
        pltpu.make_async_copy(source, target, arrived.at[n])
        for n, (source, target) in enumerate(zip(inputs, held))
    ]
    for copy in copies:
        copy.start()

    def run():
        for copy in copies:
            copy.wait()
        prepare(count, *held, *outs)

    beside(weight, chunk, landed, first, run)


def prepare(
    count, lengths, slot_seq, slot_block, queries, new_kv, bias, fresh_out, value_out, own_out
):
    seq_total, tokens = bias.shape
    slots = tokens // BLK
    seq_rep, own_width = queries.shape
    local_heads = own_width // HD
    group_size = QH // KVH
    kvb_count = seq_total // seq_rep
    seq = slot_seq[...]
    length_of = jnp.zeros_like(seq)
    for s in range(seq_total):
        length_of = jnp.where(seq == s, lengths[s], length_of)
    slot_ids = lax.broadcasted_iota(jnp.int32, seq.shape, 1)
    remaining = jnp.clip(length_of - slot_block[...] * BLK, 0, BLK)
    remaining = jnp.where(slot_ids < count[0], remaining, 0)
    row = lax.broadcasted_iota(jnp.int32, (8, slots), 0)
    codes = jnp.where(row == 0, seq, jnp.where(row == 1, remaining, 0))
    spread = (
        lax.broadcasted_iota(jnp.int32, (slots, tokens), 1) // BLK
        == lax.broadcasted_iota(jnp.int32, (slots, tokens), 0)
    )
    per_token = jnp.dot(
        codes.astype(jnp.float32).astype(jnp.bfloat16),
        jnp.where(spread, 1.0, 0.0).astype(jnp.bfloat16),
        preferred_element_type=jnp.float32,
    )
    row = lax.broadcasted_iota(jnp.int32, (seq_total, tokens), 0)
    replica = behind(lax.axis_index("kvb"), row // seq_rep, kvb_count)
    seq_ids = (replica * seq_rep + row % seq_rep).astype(jnp.float32)
    offsets = (lax.broadcasted_iota(jnp.int32, (seq_total, tokens), 1) % BLK).astype(jnp.float32)
    live = (per_token[0:1] == seq_ids) & (offsets < per_token[1:2])
    bias[...] = jnp.where(live, 0.0, MASKED)

    own_out[...] = queries[...]
    kv_local = max(1, local_heads // group_size)
    kv_first = lax.axis_index("tp") * local_heads // group_size
    lane = lax.broadcasted_iota(jnp.int32, (seq_rep, STATS), 1)
    fresh = jnp.zeros((seq_rep, STATS), jnp.float32)
    for v in range(kv_local):
        at = pl.multiple_of((kv_first + v) * HD, HD)
        key = new_kv[:, pl.ds(at, HD)].astype(jnp.float32)
        at = pl.multiple_of((KVH + kv_first + v) * HD, HD)
        value_out[:, v * HD : (v + 1) * HD] = new_kv[:, pl.ds(at, HD)].astype(jnp.float32)
        for h in range(v * local_heads // kv_local, (v + 1) * local_heads // kv_local):
            query = queries[:, h * HD : (h + 1) * HD].astype(jnp.float32)
            score = jnp.sum(query * key, axis=1, keepdims=True)
            fresh = jnp.where(lane == h, score, fresh)
    fresh_out[...] = fresh * UNIT


def attend_body(bias_ref, queries, cache, out, stacked, *, shift):
    kvb_count, seq_rep, own_width = queries.shape
    tp_count = lax.axis_size("tp")
    tokens = cache.shape[0] * BLK
    seq_total = kvb_count * seq_rep
    local_heads = own_width // HD
    group_size = QH // KVH
    kv_local = max(1, local_heads // group_size)
    per_kv = local_heads // kv_local
    bias = bias_ref[...]
    for r in range(kvb_count):
        stacked[r * seq_rep : (r + 1) * seq_rep, :] = queries[r].astype(jnp.float32)
    t = ahead(lax.axis_index("tp"), shift, tp_count)
    lane = lax.broadcasted_iota(jnp.int32, (seq_total, STATS), 1)
    stats = jnp.zeros((seq_total, STATS), jnp.float32)
    for v in range(kv_local):
        heads = range(v * per_kv, (v + 1) * per_kv)
        rows = jnp.concatenate(
            [stacked[:, h * HD : (h + 1) * HD] for h in heads], axis=0
        ).astype(jnp.bfloat16)
        g = t * local_heads // group_size + v
        at = pl.multiple_of(g * HD, HD)
        keys = cache[:, :, pl.ds(at, HD)].reshape(tokens, HD)
        at = pl.multiple_of((KVH + g) * HD, HD)
        values = cache[:, :, pl.ds(at, HD)].reshape(tokens, HD)
        scores = lax.dot_general(
            rows, keys, (((1,), (1,)), ((), ())), preferred_element_type=jnp.float32
        )
        scores = scores.reshape(per_kv, seq_total, tokens) * UNIT + bias[None]
        peaks = jnp.maximum(jnp.max(scores, axis=2, keepdims=True), FLOOR)
        peaks = peaks.astype(jnp.bfloat16).astype(jnp.float32)
        weights = jnp.exp2(scores - peaks)
        sums = jnp.sum(weights, axis=2, keepdims=True)
        partial = jnp.dot(
            weights.astype(jnp.bfloat16).reshape(per_kv * seq_total, tokens),
            values,
            preferred_element_type=jnp.float32,
        )
        high = sums.astype(jnp.bfloat16).astype(jnp.float32)
        low = sums - high
        for j, h in enumerate(heads):
            out[:, h * HD : (h + 1) * HD] = partial[j * seq_total : (j + 1) * seq_total].astype(
                jnp.bfloat16
            )
            for part, value in enumerate((peaks, high, low)):
                stats = jnp.where(lane == part * local_heads + h, value[j], stats)
    out[:, local_heads * HD :] = stats.astype(jnp.bfloat16)


def fetch_body(weight, *refs, first):
    chunk, arrived = refs[-2:]
    copy = pltpu.make_async_copy(weight.at[:, pl.ds(first, chunk.shape[1])], chunk, arrived)
    copy.start()
    copy.wait()


def unpack(ref, local_heads):
    stats = ref[:, local_heads * HD :].astype(jnp.float32)
    sums = stats[:, local_heads : 2 * local_heads] + stats[:, 2 * local_heads : 3 * local_heads]
    return stats[:, :local_heads], sums


def merge_body(*refs, sources):
    parts, outs = refs[:sources], refs[sources:]
    seq_total, width = parts[0].shape
    seq_rep = outs[0].shape[0]
    local_heads = (width - STATS) // HD
    pairs = [unpack(part, local_heads) for part in parts]
    peak = pairs[0][0]
    for other, _ in pairs[1:]:
        peak = jnp.maximum(peak, other)
    scaling = [jnp.exp2(p - peak) for p, _ in pairs]
    total = sum(s * c for s, (_, c) in zip(scaling, pairs))
    high = total.astype(jnp.bfloat16).astype(jnp.float32)
    pad = jnp.zeros((seq_total, STATS - 3 * local_heads), jnp.float32)
    stats = jnp.concatenate([peak, high, total - high, pad], axis=1)
    blocks = [
        sum(
            s[:, h : h + 1] * part[:, h * HD : (h + 1) * HD].astype(jnp.float32)
            for s, part in zip(scaling, parts)
        )
        for h in range(local_heads)
    ]
    for h, block in enumerate(blocks + [stats]):
        for r, out in enumerate(outs):
            out[:, h * HD : (h + 1) * HD] = block[r * seq_rep : (r + 1) * seq_rep].astype(
                jnp.bfloat16
            )


def project_body(*refs, sources):
    parts = refs[:sources]
    fresh_ref, value_ref, weight = refs[sources : sources + 3]
    pieces = len(LATE)
    chunks = list(refs[sources + 3 : -3 - pieces])
    out, *late = refs[-3 - pieces : -2]
    arrived, rows = refs[-2:]
    first = weight.shape[1] - sum(piece.shape[1] for piece in late)
    copies = []
    for n, piece in enumerate(late):
        columns = pl.ds(first, piece.shape[1])
        copies.append(pltpu.make_async_copy(weight.at[:, columns], piece, arrived.at[n]))
        copies[-1].start()
        first += piece.shape[1]
    def combine():
        local_heads = (parts[0].shape[1] - STATS) // HD
        kv_local = value_ref.shape[1] // HD
        pairs = [unpack(part, local_heads) for part in parts]
        fresh = fresh_ref[:, :local_heads]
        overall = fresh
        for peak, _ in pairs:
            overall = jnp.maximum(overall, peak)
        scaling = [jnp.exp2(peak - overall) for peak, _ in pairs]
        fresh_weight = jnp.exp2(fresh - overall)
        inverse = 1.0 / (fresh_weight + sum(s * c for s, (_, c) in zip(scaling, pairs)))
        scaling = [s * inverse for s in scaling]
        fresh_weight = fresh_weight * inverse
        attended = []
        for h in range(local_heads):
            v = h * kv_local // local_heads
            total = fresh_weight[:, h : h + 1] * value_ref[:, v * HD : (v + 1) * HD]
            for s, part in zip(scaling, parts):
                total = total + s[:, h : h + 1] * part[:, h * HD : (h + 1) * HD].astype(jnp.float32)
            attended.append(total.astype(jnp.bfloat16))
        rows[...] = jnp.concatenate(attended, axis=1)

    once(combine)
    attended = rows[...]
    first = 0
    for n, chunk in enumerate(chunks + late):
        if n >= len(chunks):
            copies[n - len(chunks)].wait()
        for at in range(0, chunk.shape[1], STEP):
            step = min(STEP, chunk.shape[1] - at)
            out[:, first + at : first + at + step] = jnp.dot(
                attended, chunk[:, at : at + step], preferred_element_type=jnp.float32
            ).astype(out.dtype)
        first += chunk.shape[1]


def finish_body(pieces, residual, gain, stream_out, normed_out):
    full = residual[...].astype(jnp.float32)
    width = full.shape[1]
    total = pieces[0].astype(jnp.float32)
    for t in range(1, pieces.shape[0]):
        total = total + pieces[t].astype(jnp.float32)
    full = (full + total).astype(jnp.bfloat16).astype(jnp.float32)
    mean_square = jnp.sum(full * full, axis=1, keepdims=True) / width
    inverse = lax.rsqrt(mean_square + EPSILON)
    own = stream_out.shape[1]
    at = pl.multiple_of(lax.axis_index("tp") * own, own)
    mine = residual[:, pl.ds(at, own)].astype(jnp.float32)
    total = pieces[0, :, pl.ds(at, own)].astype(jnp.float32)
    for t in range(1, pieces.shape[0]):
        total = total + pieces[t, :, pl.ds(at, own)].astype(jnp.float32)
    stream = (mine + total).astype(jnp.bfloat16)
    stream_out[...] = stream
    normed_out[...] = (stream.astype(jnp.float32) * inverse * gain[...].astype(jnp.float32)).astype(
        jnp.bfloat16
    )


def vmem():
    return pl.BlockSpec(memory_space=pltpu.VMEM)


def resident(array):
    return pltpu.with_memory_space_constraint(array, pltpu.VMEM)


def hbm():
    return pl.BlockSpec(memory_space=pltpu.HBM)


def on_device(
    residual,
    queries,
    new_kv,
    kv_cache,
    lengths,
    slot_seq,
    slot_block,
    block_counts,
    out_weight,
    norm_gain,
):
    tp_count = lax.axis_size("tp")
    kvb_count = lax.axis_size("kvb")
    seq_rep, own_width = queries.shape
    seq_total = kvb_count * seq_rep
    tokens = kv_cache.shape[0] * BLK
    kv_local = max(1, own_width // HD * KVH // QH)
    depth, columns = out_weight.shape
    out_weight = pltpu.with_memory_space_constraint(out_weight, pltpu.HBM)
    share = [columns * n // sum(SHARES) for n in SHARES]
    starts = [sum(share[:n]) for n in range(len(share))]
    arrived = [
        lax.ppermute(queries, "kvb", [(k, ahead(k, r, kvb_count)) for k in range(kvb_count)])
        for r in range(1, kvb_count)
    ]
    bias, fresh, fresh_values, own_queries, under_prepare = pl.pallas_call(
        lambda *refs: prepare_body(*refs, first=starts[0]),
        out_shape=(
            jax.ShapeDtypeStruct((seq_total, tokens), jnp.float32),
            jax.ShapeDtypeStruct((seq_rep, STATS), jnp.float32),
            jax.ShapeDtypeStruct((seq_rep, kv_local * HD), jnp.float32),
            jax.ShapeDtypeStruct((seq_rep, own_width), jnp.bfloat16),
            pltpu.VMEM((depth, share[0]), out_weight.dtype),
        ),
        in_specs=[pl.BlockSpec(memory_space=pltpu.SMEM)] + [hbm()] * 6,
        out_specs=(vmem(),) * 5,
        scratch_shapes=[
            pltpu.SMEM(lengths.shape, jnp.int32),
            pltpu.VMEM((1,) + slot_seq.shape, jnp.int32),
            pltpu.VMEM((1,) + slot_block.shape, jnp.int32),
            pltpu.VMEM(queries.shape, queries.dtype),
            pltpu.VMEM(new_kv.shape, new_kv.dtype),
            pltpu.SemaphoreType.DMA((5,)),
            pltpu.SemaphoreType.DMA,
        ],
        compiler_params=pltpu.CompilerParams(vmem_limit_bytes=4 << 20),
        cost_estimate=pl.CostEstimate(flops=COVER, transcendentals=0, bytes_accessed=1 << 20),
        name="prepare",
    )(block_counts, *[
        pltpu.with_memory_space_constraint(array, pltpu.HBM)
        for array in (lengths, slot_seq[None], slot_block[None], queries, new_kv)
    ], out_weight)
    wide = jnp.stack([own_queries] + arrived)
    cache = resident(kv_cache)

    def fetch(first, size, *after):
        return pl.pallas_call(
            lambda *refs: fetch_body(*refs, first=first),
            out_shape=pltpu.VMEM((depth, size), out_weight.dtype),
            in_specs=[hbm()] + [pl.BlockSpec(memory_space=pl.ANY)] * len(after),
            out_specs=vmem(),
            scratch_shapes=[pltpu.SemaphoreType.DMA],
            compiler_params=pltpu.CompilerParams(vmem_limit_bytes=1 << 20),
            cost_estimate=pl.CostEstimate(flops=COVER, transcendentals=0, bytes_accessed=1 << 20),
            name="fetch",
        )(out_weight, *after)

    def attend(rows, shift):
        return pl.pallas_call(
            lambda *refs: attend_body(*refs, shift=shift),
            out_shape=jax.ShapeDtypeStruct((seq_total, own_width + STATS), jnp.bfloat16),
            in_specs=[vmem(), vmem(), vmem()],
            out_specs=vmem(),
            scratch_shapes=[pltpu.VMEM((seq_total, own_width), jnp.float32)],
            compiler_params=pltpu.CompilerParams(vmem_limit_bytes=6 << 20),
            cost_estimate=pl.CostEstimate(flops=COVER, transcendentals=0, bytes_accessed=1 << 20),
            name="attend",
        )(bias, rows, cache)

    def swapped(rows, partner, d):
        return lax.ppermute(rows, "tp", [(t, partner(t, d, tp_count)) for t in range(tp_count)])

    asked = [swapped(wide, behind, d) for d in range(1, tp_count)]
    parts = [attend(wide, 0)]
    chunks = [under_prepare]
    for d in range(1, tp_count):
        parts.append(swapped(attend(asked[d - 1], d), ahead, d))
    chunks.append(fetch(starts[1], share[1], parts[0]))
    block = jax.ShapeDtypeStruct((seq_rep, own_width + STATS), jnp.bfloat16)
    dealt = pl.pallas_call(
        lambda *refs: merge_body(*refs, sources=tp_count),
        out_shape=(block,) * kvb_count,
        in_specs=[vmem()] * tp_count,
        out_specs=(vmem(),) * kvb_count,
        compiler_params=pltpu.CompilerParams(vmem_limit_bytes=4 << 20),
        name="merge",
    )(*parts)
    parts = [dealt[0]] + [
        lax.ppermute(dealt[r], "kvb", [(k, behind(k, r, kvb_count)) for k in range(kvb_count)])
        for r in range(1, kvb_count)
    ]
    chunks.append(fetch(starts[2], share[2], dealt[0]))
    projected = pl.pallas_call(
        lambda *refs: project_body(*refs, sources=kvb_count),
        out_shape=jax.ShapeDtypeStruct((seq_rep, out_weight.shape[1]), jnp.bfloat16),
        in_specs=[vmem()] * (kvb_count + 2) + [hbm()] + [vmem()] * len(chunks),
        out_specs=vmem(),
        scratch_shapes=[
            *[pltpu.VMEM((depth, share[3] * n // sum(LATE)), out_weight.dtype) for n in LATE],
            pltpu.SemaphoreType.DMA((len(LATE),)),
            pltpu.VMEM((seq_rep, own_width), jnp.bfloat16),
        ],
        compiler_params=pltpu.CompilerParams(vmem_limit_bytes=18 << 20),
        name="project",
    )(*parts, fresh, fresh_values, out_weight, *chunks)
    pieces = lax.all_gather(projected, "tp", axis=0, tiled=False)
    own = jax.ShapeDtypeStruct((seq_rep, norm_gain.shape[0]), jnp.bfloat16)
    return pl.pallas_call(
        finish_body,
        out_shape=(own, own),
        in_specs=[vmem(), vmem(), vmem()],
        out_specs=(vmem(), vmem()),
        compiler_params=pltpu.CompilerParams(vmem_limit_bytes=4 << 20),
        name="finish",
    )(pieces, residual, norm_gain[None])


def solution(mesh):
    placed = (
        P(("groups", "kvb"), None),
        P(("groups", "kvb"), "tp"),
        P(("groups", "kvb"), None),
        P(("groups", "kvb", "tp"), None, None),
        P("groups"),
        P(("groups", "kvb", "tp")),
        P(("groups", "kvb", "tp")),
        P(("groups", "kvb", "tp")),
        P("tp", None),
        P("tp"),
    )
    return jax.shard_map(
        on_device,
        mesh=mesh,
        in_specs=placed,
        out_specs=(P(("groups", "kvb"), "tp"), P(("groups", "kvb"), "tp")),
        check_vma=False,
    )
```

```python
import jax
import jax.numpy as jnp
from jax import lax
from jax.experimental import pallas as pl
from jax.experimental.pallas import tpu as pltpu
from jax.sharding import PartitionSpec as P

QH = 64
KVH = 8
HD = 128
BLK = 16

MASKED = -1e30
FLOOR = -1e20
EPSILON = 1e-06
UNIT = HD ** (-0.5) * 1.4426950408889634
STATS = 128
COVER = 20_000_000_000
SHARES = (4, 5, 10, 13)
LATE = (4, 4, 3, 2)
STEP = 512


def ahead(index, step, count):
    if count & (count - 1) == 0:
        return index ^ step
    return (index + step) % count


def behind(index, step, count):
    if count & (count - 1) == 0:
        return index ^ step
    return (index - step + count) % count


def once(body):
    trips = jnp.where(lax.axis_index("tp") >= 0, 1, 0)

    def trip(_, carried):
        body()
        return carried

    lax.fori_loop(0, trips, trip, 0)


def beside(weight, chunk, arrived, first, body):
    copy = pltpu.make_async_copy(weight.at[:, pl.ds(first, chunk.shape[1])], chunk, arrived)
    copy.start()
    once(body)
    copy.wait()


def prepare_body(count, *refs, first):
    inputs, weight, outs, chunk = refs[:5], refs[5], refs[6:10], refs[10]
    held, arrived, landed = refs[11:16], refs[16], refs[17]
    copies = [
        pltpu.make_async_copy(source, target, arrived.at[n])
        for n, (source, target) in enumerate(zip(inputs, held))
    ]
    for copy in copies:
        copy.start()

    def run():
        for copy in copies:
            copy.wait()
        prepare(count, *held, *outs)

    beside(weight, chunk, landed, first, run)


def prepare(
    count, lengths, slot_seq, slot_block, queries, new_kv, bias, fresh_out, value_out, own_out
):
    seq_total, tokens = bias.shape
    slots = tokens // BLK
    seq_rep, own_width = queries.shape
    local_heads = own_width // HD
    group_size = QH // KVH
    kvb_count = seq_total // seq_rep
    seq = slot_seq[...]
    length_of = jnp.zeros_like(seq)
    for s in range(seq_total):
        length_of = jnp.where(seq == s, lengths[s], length_of)
    slot_ids = lax.broadcasted_iota(jnp.int32, seq.shape, 1)
    remaining = jnp.clip(length_of - slot_block[...] * BLK, 0, BLK)
    remaining = jnp.where(slot_ids < count[0], remaining, 0)
    row = lax.broadcasted_iota(jnp.int32, (8, slots), 0)
    codes = jnp.where(row == 0, seq, jnp.where(row == 1, remaining, 0))
    spread = (
        lax.broadcasted_iota(jnp.int32, (slots, tokens), 1) // BLK
        == lax.broadcasted_iota(jnp.int32, (slots, tokens), 0)
    )
    per_token = jnp.dot(
        codes.astype(jnp.float32).astype(jnp.bfloat16),
        jnp.where(spread, 1.0, 0.0).astype(jnp.bfloat16),
        preferred_element_type=jnp.float32,
    )
    row = lax.broadcasted_iota(jnp.int32, (seq_total, tokens), 0)
    replica = behind(lax.axis_index("kvb"), row // seq_rep, kvb_count)
    seq_ids = (replica * seq_rep + row % seq_rep).astype(jnp.float32)
    offsets = (lax.broadcasted_iota(jnp.int32, (seq_total, tokens), 1) % BLK).astype(jnp.float32)
    live = (per_token[0:1] == seq_ids) & (offsets < per_token[1:2])
    bias[...] = jnp.where(live, 0.0, MASKED)

    own_out[...] = queries[...]
    kv_local = max(1, local_heads // group_size)
    kv_first = lax.axis_index("tp") * local_heads // group_size
    lane = lax.broadcasted_iota(jnp.int32, (seq_rep, STATS), 1)
    fresh = jnp.zeros((seq_rep, STATS), jnp.float32)
    for v in range(kv_local):
        at = pl.multiple_of((kv_first + v) * HD, HD)
        key = new_kv[:, pl.ds(at, HD)].astype(jnp.float32)
        at = pl.multiple_of((KVH + kv_first + v) * HD, HD)
        value_out[:, v * HD : (v + 1) * HD] = new_kv[:, pl.ds(at, HD)].astype(jnp.float32)
        for h in range(v * local_heads // kv_local, (v + 1) * local_heads // kv_local):
            query = queries[:, h * HD : (h + 1) * HD].astype(jnp.float32)
            score = jnp.sum(query * key, axis=1, keepdims=True)
            fresh = jnp.where(lane == h, score, fresh)
    fresh_out[...] = fresh * UNIT


def attend_body(bias_ref, queries, cache, out, stacked, *, shift):
    kvb_count, seq_rep, own_width = queries.shape
    tp_count = lax.axis_size("tp")
    tokens = cache.shape[0] * BLK
    seq_total = kvb_count * seq_rep
    local_heads = own_width // HD
    group_size = QH // KVH
    kv_local = max(1, local_heads // group_size)
    per_kv = local_heads // kv_local
    bias = bias_ref[...]
    for r in range(kvb_count):
        stacked[r * seq_rep : (r + 1) * seq_rep, :] = queries[r].astype(jnp.float32)
    t = lax.axis_index("tp") + shift
    t = jnp.where(t < tp_count, t, t - tp_count)
    lane = lax.broadcasted_iota(jnp.int32, (seq_total, STATS), 1)
    stats = jnp.zeros((seq_total, STATS), jnp.float32)
    for v in range(kv_local):
        heads = range(v * per_kv, (v + 1) * per_kv)
        rows = jnp.concatenate(
            [stacked[:, h * HD : (h + 1) * HD] for h in heads], axis=0
        ).astype(jnp.bfloat16)
        g = t * local_heads // group_size + v
        at = pl.multiple_of(g * HD, HD)
        keys = cache[:, :, pl.ds(at, HD)].reshape(tokens, HD)
        at = pl.multiple_of((KVH + g) * HD, HD)
        values = cache[:, :, pl.ds(at, HD)].reshape(tokens, HD)
        scores = lax.dot_general(
            rows, keys, (((1,), (1,)), ((), ())), preferred_element_type=jnp.float32
        )
        scores = scores.reshape(per_kv, seq_total, tokens) * UNIT + bias[None]
        peaks = jnp.maximum(jnp.max(scores, axis=2, keepdims=True), FLOOR)
        peaks = peaks.astype(jnp.bfloat16).astype(jnp.float32)
        weights = jnp.exp2(scores - peaks)
        sums = jnp.sum(weights, axis=2, keepdims=True)
        partial = jnp.dot(
            weights.astype(jnp.bfloat16).reshape(per_kv * seq_total, tokens),
            values,
            preferred_element_type=jnp.float32,
        )
        high = sums.astype(jnp.bfloat16).astype(jnp.float32)
        low = sums - high
        for j, h in enumerate(heads):
            out[:, h * HD : (h + 1) * HD] = partial[j * seq_total : (j + 1) * seq_total].astype(
                jnp.bfloat16
            )
            for part, value in enumerate((peaks, high, low)):
                stats = jnp.where(lane == part * local_heads + h, value[j], stats)
    out[:, local_heads * HD :] = stats.astype(jnp.bfloat16)


def fetch_body(weight, *refs, first):
    chunk, arrived = refs[-2:]
    copy = pltpu.make_async_copy(weight.at[:, pl.ds(first, chunk.shape[1])], chunk, arrived)
    copy.start()
    copy.wait()


def unpack(ref, local_heads):
    stats = ref[:, local_heads * HD :].astype(jnp.float32)
    sums = stats[:, local_heads : 2 * local_heads] + stats[:, 2 * local_heads : 3 * local_heads]
    return stats[:, :local_heads], sums


def merge_body(*refs, sources):
    parts, outs = refs[:sources], refs[sources:]
    seq_total, width = parts[0].shape
    seq_rep = outs[0].shape[0]
    local_heads = (width - STATS) // HD
    pairs = [unpack(part, local_heads) for part in parts]
    peak = pairs[0][0]
    for other, _ in pairs[1:]:
        peak = jnp.maximum(peak, other)
    scaling = [jnp.exp2(p - peak) for p, _ in pairs]
    total = sum(s * c for s, (_, c) in zip(scaling, pairs))
    high = total.astype(jnp.bfloat16).astype(jnp.float32)
    pad = jnp.zeros((seq_total, STATS - 3 * local_heads), jnp.float32)
    stats = jnp.concatenate([peak, high, total - high, pad], axis=1)
    blocks = [
        sum(
            s[:, h : h + 1] * part[:, h * HD : (h + 1) * HD].astype(jnp.float32)
            for s, part in zip(scaling, parts)
        )
        for h in range(local_heads)
    ]
    for h, block in enumerate(blocks + [stats]):
        for r, out in enumerate(outs):
            out[:, h * HD : (h + 1) * HD] = block[r * seq_rep : (r + 1) * seq_rep].astype(
                jnp.bfloat16
            )


def project_body(*refs, sources):
    parts = refs[:sources]
    fresh_ref, value_ref, weight = refs[sources : sources + 3]
    pieces = len(LATE)
    chunks = list(refs[sources + 3 : -3 - pieces])
    out, *late = refs[-3 - pieces : -2]
    arrived, rows = refs[-2:]
    first = weight.shape[1] - sum(piece.shape[1] for piece in late)
    copies = []
    for n, piece in enumerate(late):
        columns = pl.ds(first, piece.shape[1])
        copies.append(pltpu.make_async_copy(weight.at[:, columns], piece, arrived.at[n]))
        copies[-1].start()
        first += piece.shape[1]
    def combine():
        local_heads = (parts[0].shape[1] - STATS) // HD
        kv_local = value_ref.shape[1] // HD
        pairs = [unpack(part, local_heads) for part in parts]
        fresh = fresh_ref[:, :local_heads]
        overall = fresh
        for peak, _ in pairs:
            overall = jnp.maximum(overall, peak)
        scaling = [jnp.exp2(peak - overall) for peak, _ in pairs]
        fresh_weight = jnp.exp2(fresh - overall)
        inverse = 1.0 / (fresh_weight + sum(s * c for s, (_, c) in zip(scaling, pairs)))
        scaling = [s * inverse for s in scaling]
        fresh_weight = fresh_weight * inverse
        attended = []
        for h in range(local_heads):
            v = h * kv_local // local_heads
            total = fresh_weight[:, h : h + 1] * value_ref[:, v * HD : (v + 1) * HD]
            for s, part in zip(scaling, parts):
                total = total + s[:, h : h + 1] * part[:, h * HD : (h + 1) * HD].astype(jnp.float32)
            attended.append(total.astype(jnp.bfloat16))
        rows[...] = jnp.concatenate(attended, axis=1)

    once(combine)
    attended = rows[...]
    first = 0
    for n, chunk in enumerate(chunks + late):
        if n >= len(chunks):
            copies[n - len(chunks)].wait()
        for at in range(0, chunk.shape[1], STEP):
            step = min(STEP, chunk.shape[1] - at)
            out[:, first + at : first + at + step] = jnp.dot(
                attended, chunk[:, at : at + step], preferred_element_type=jnp.float32
            ).astype(out.dtype)
        first += chunk.shape[1]


def finish_body(pieces, residual, gain, stream_out, normed_out):
    full = residual[...].astype(jnp.float32)
    width = full.shape[1]
    total = pieces[0].astype(jnp.float32)
    for t in range(1, pieces.shape[0]):
        total = total + pieces[t].astype(jnp.float32)
    full = (full + total).astype(jnp.bfloat16).astype(jnp.float32)
    mean_square = jnp.sum(full * full, axis=1, keepdims=True) / width
    inverse = lax.rsqrt(mean_square + EPSILON)
    own = stream_out.shape[1]
    at = pl.multiple_of(lax.axis_index("tp") * own, own)
    mine = residual[:, pl.ds(at, own)].astype(jnp.float32)
    total = pieces[0, :, pl.ds(at, own)].astype(jnp.float32)
    for t in range(1, pieces.shape[0]):
        total = total + pieces[t, :, pl.ds(at, own)].astype(jnp.float32)
    stream = (mine + total).astype(jnp.bfloat16)
    stream_out[...] = stream
    normed_out[...] = (stream.astype(jnp.float32) * inverse * gain[...].astype(jnp.float32)).astype(
        jnp.bfloat16
    )


def vmem():
    return pl.BlockSpec(memory_space=pltpu.VMEM)


def resident(array):
    return pltpu.with_memory_space_constraint(array, pltpu.VMEM)


def hbm():
    return pl.BlockSpec(memory_space=pltpu.HBM)


def on_device(
    residual,
    queries,
    new_kv,
    kv_cache,
    lengths,
    slot_seq,
    slot_block,
    block_counts,
    out_weight,
    norm_gain,
):
    tp_count = lax.axis_size("tp")
    kvb_count = lax.axis_size("kvb")
    seq_rep, own_width = queries.shape
    seq_total = kvb_count * seq_rep
    tokens = kv_cache.shape[0] * BLK
    kv_local = max(1, own_width // HD * KVH // QH)
    depth, columns = out_weight.shape
    out_weight = pltpu.with_memory_space_constraint(out_weight, pltpu.HBM)
    share = [columns * n // sum(SHARES) for n in SHARES]
    starts = [sum(share[:n]) for n in range(len(share))]
    arrived = [
        lax.ppermute(queries, "kvb", [(k, ahead(k, r, kvb_count)) for k in range(kvb_count)])
        for r in range(1, kvb_count)
    ]
    bias, fresh, fresh_values, own_queries, under_prepare = pl.pallas_call(
        lambda *refs: prepare_body(*refs, first=starts[0]),
        out_shape=(
            jax.ShapeDtypeStruct((seq_total, tokens), jnp.float32),
            jax.ShapeDtypeStruct((seq_rep, STATS), jnp.float32),
            jax.ShapeDtypeStruct((seq_rep, kv_local * HD), jnp.float32),
            jax.ShapeDtypeStruct((seq_rep, own_width), jnp.bfloat16),
            pltpu.VMEM((depth, share[0]), out_weight.dtype),
        ),
        in_specs=[pl.BlockSpec(memory_space=pltpu.SMEM)] + [hbm()] * 6,
        out_specs=(vmem(),) * 5,
        scratch_shapes=[
            pltpu.SMEM(lengths.shape, jnp.int32),
            pltpu.VMEM((1,) + slot_seq.shape, jnp.int32),
            pltpu.VMEM((1,) + slot_block.shape, jnp.int32),
            pltpu.VMEM(queries.shape, queries.dtype),
            pltpu.VMEM(new_kv.shape, new_kv.dtype),
            pltpu.SemaphoreType.DMA((5,)),
            pltpu.SemaphoreType.DMA,
        ],
        compiler_params=pltpu.CompilerParams(vmem_limit_bytes=4 << 20),
        cost_estimate=pl.CostEstimate(flops=COVER, transcendentals=0, bytes_accessed=1 << 20),
        name="prepare",
    )(block_counts, *[
        pltpu.with_memory_space_constraint(array, pltpu.HBM)
        for array in (lengths, slot_seq[None], slot_block[None], queries, new_kv)
    ], out_weight)
    wide = jnp.stack([own_queries] + arrived)
    cache = resident(kv_cache)

    def fetch(first, size, *after):
        return pl.pallas_call(
            lambda *refs: fetch_body(*refs, first=first),
            out_shape=pltpu.VMEM((depth, size), out_weight.dtype),
            in_specs=[hbm()] + [pl.BlockSpec(memory_space=pl.ANY)] * len(after),
            out_specs=vmem(),
            scratch_shapes=[pltpu.SemaphoreType.DMA],
            compiler_params=pltpu.CompilerParams(vmem_limit_bytes=1 << 20),
            cost_estimate=pl.CostEstimate(flops=COVER, transcendentals=0, bytes_accessed=1 << 20),
            name="fetch",
        )(out_weight, *after)

    def attend(rows, shift):
        return pl.pallas_call(
            lambda *refs: attend_body(*refs, shift=shift),
            out_shape=jax.ShapeDtypeStruct((seq_total, own_width + STATS), jnp.bfloat16),
            in_specs=[vmem(), vmem(), vmem()],
            out_specs=vmem(),
            scratch_shapes=[pltpu.VMEM((seq_total, own_width), jnp.float32)],
            compiler_params=pltpu.CompilerParams(vmem_limit_bytes=6 << 20),
            cost_estimate=pl.CostEstimate(flops=COVER, transcendentals=0, bytes_accessed=1 << 20),
            name="attend",
        )(bias, rows, cache)

    def shifted(rows, shift):
        return lax.ppermute(rows, "tp", [(t, (t + shift) % tp_count) for t in range(tp_count)])

    asked = [shifted(wide, -d) for d in range(1, tp_count)]
    parts = [attend(wide, 0)]
    chunks = [under_prepare]
    for d in range(1, tp_count):
        parts.append(shifted(attend(asked[d - 1], d), d))
    chunks.append(fetch(starts[1], share[1], parts[0]))
    block = jax.ShapeDtypeStruct((seq_rep, own_width + STATS), jnp.bfloat16)
    dealt = pl.pallas_call(
        lambda *refs: merge_body(*refs, sources=tp_count),
        out_shape=(block,) * kvb_count,
        in_specs=[vmem()] * tp_count,
        out_specs=(vmem(),) * kvb_count,
        compiler_params=pltpu.CompilerParams(vmem_limit_bytes=4 << 20),
        name="merge",
    )(*parts)
    parts = [dealt[0]] + [
        lax.ppermute(dealt[r], "kvb", [(k, behind(k, r, kvb_count)) for k in range(kvb_count)])
        for r in range(1, kvb_count)
    ]
    chunks.append(fetch(starts[2], share[2], dealt[0]))
    projected = pl.pallas_call(
        lambda *refs: project_body(*refs, sources=kvb_count),
        out_shape=jax.ShapeDtypeStruct((seq_rep, out_weight.shape[1]), jnp.bfloat16),
        in_specs=[vmem()] * (kvb_count + 2) + [hbm()] + [vmem()] * len(chunks),
        out_specs=vmem(),
        scratch_shapes=[
            *[pltpu.VMEM((depth, share[3] * n // sum(LATE)), out_weight.dtype) for n in LATE],
            pltpu.SemaphoreType.DMA((len(LATE),)),
            pltpu.VMEM((seq_rep, own_width), jnp.bfloat16),
        ],
        compiler_params=pltpu.CompilerParams(vmem_limit_bytes=18 << 20),
        name="project",
    )(*parts, fresh, fresh_values, out_weight, *chunks)
    pieces = lax.all_gather(projected, "tp", axis=0, tiled=False)
    own = jax.ShapeDtypeStruct((seq_rep, norm_gain.shape[0]), jnp.bfloat16)
    return pl.pallas_call(
        finish_body,
        out_shape=(own, own),
        in_specs=[vmem(), vmem(), vmem()],
        out_specs=(vmem(), vmem()),
        compiler_params=pltpu.CompilerParams(vmem_limit_bytes=4 << 20),
        name="finish",
    )(pieces, residual, norm_gain[None])


def solution(mesh):
    placed = (
        P(("groups", "kvb"), None),
        P(("groups", "kvb"), "tp"),
        P(("groups", "kvb"), None),
        P(("groups", "kvb", "tp"), None, None),
        P("groups"),
        P(("groups", "kvb", "tp")),
        P(("groups", "kvb", "tp")),
        P(("groups", "kvb", "tp")),
        P("tp", None),
        P("tp"),
    )
    return jax.shard_map(
        on_device,
        mesh=mesh,
        in_specs=placed,
        out_specs=(P(("groups", "kvb"), "tp"), P(("groups", "kvb"), "tp")),
        check_vma=False,
    )
```

```python
import jax
import jax.numpy as jnp
from jax import lax
from jax.experimental import pallas as pl
from jax.experimental.pallas import tpu as pltpu
from jax.sharding import PartitionSpec as P

QH = 64
KVH = 8
HD = 128
BLK = 16

MASKED = -1e30
FLOOR = -1e20
EPSILON = 1e-06
UNIT = HD ** (-0.5) * 1.4426950408889634
STATS = 128
COVER = 20_000_000_000
SHARES = (4, 5, 10, 13)
LATE = (4, 4, 3, 2)
STEP = 512


def ahead(index, step, count):
    if count & (count - 1) == 0:
        return index ^ step
    return (index + step) % count


def behind(index, step, count):
    if count & (count - 1) == 0:
        return index ^ step
    return (index - step + count) % count


def once(body):
    trips = jnp.where(lax.axis_index("tp") >= 0, 1, 0)

    def trip(_, carried):
        body()
        return carried

    lax.fori_loop(0, trips, trip, 0)


def beside(weight, chunk, arrived, first, body):
    copy = pltpu.make_async_copy(weight.at[:, pl.ds(first, chunk.shape[1])], chunk, arrived)
    copy.start()
    once(body)
    copy.wait()


def prepare_body(count, *refs, first):
    inputs, weight, outs, chunk = refs[:5], refs[5], refs[6:10], refs[10]
    held, arrived, landed = refs[11:16], refs[16], refs[17]
    copies = [
        pltpu.make_async_copy(source, target, arrived.at[n])
        for n, (source, target) in enumerate(zip(inputs, held))
    ]
    for copy in copies:
        copy.start()

    def run():
        for copy in copies:
            copy.wait()
        prepare(count, *held, *outs)

    beside(weight, chunk, landed, first, run)


def prepare(
    count, lengths, slot_seq, slot_block, queries, new_kv, bias, fresh_out, value_out, own_out
):
    seq_total, tokens = bias.shape
    slots = tokens // BLK
    seq_rep, own_width = queries.shape
    local_heads = own_width // HD
    group_size = QH // KVH
    kvb_count = seq_total // seq_rep
    seq = slot_seq[...]
    length_of = jnp.zeros_like(seq)
    for s in range(seq_total):
        length_of = jnp.where(seq == s, lengths[s], length_of)
    slot_ids = lax.broadcasted_iota(jnp.int32, seq.shape, 1)
    remaining = jnp.clip(length_of - slot_block[...] * BLK, 0, BLK)
    remaining = jnp.where(slot_ids < count[0], remaining, 0)
    row = lax.broadcasted_iota(jnp.int32, (8, slots), 0)
    codes = jnp.where(row == 0, seq, jnp.where(row == 1, remaining, 0))
    spread = (
        lax.broadcasted_iota(jnp.int32, (slots, tokens), 1) // BLK
        == lax.broadcasted_iota(jnp.int32, (slots, tokens), 0)
    )
    per_token = jnp.dot(
        codes.astype(jnp.float32).astype(jnp.bfloat16),
        jnp.where(spread, 1.0, 0.0).astype(jnp.bfloat16),
        preferred_element_type=jnp.float32,
    )
    row = lax.broadcasted_iota(jnp.int32, (seq_total, tokens), 0)
    replica = behind(lax.axis_index("kvb"), row // seq_rep, kvb_count)
    seq_ids = (replica * seq_rep + row % seq_rep).astype(jnp.float32)
    offsets = (lax.broadcasted_iota(jnp.int32, (seq_total, tokens), 1) % BLK).astype(jnp.float32)
    live = (per_token[0:1] == seq_ids) & (offsets < per_token[1:2])
    bias[...] = jnp.where(live, 0.0, MASKED)

    own_out[...] = queries[...]
    kv_local = max(1, local_heads // group_size)
    kv_first = lax.axis_index("tp") * local_heads // group_size
    lane = lax.broadcasted_iota(jnp.int32, (seq_rep, STATS), 1)
    fresh = jnp.zeros((seq_rep, STATS), jnp.float32)
    for v in range(kv_local):
        at = pl.multiple_of((kv_first + v) * HD, HD)
        key = new_kv[:, pl.ds(at, HD)].astype(jnp.float32)
        at = pl.multiple_of((KVH + kv_first + v) * HD, HD)
        value_out[:, v * HD : (v + 1) * HD] = new_kv[:, pl.ds(at, HD)].astype(jnp.float32)
        for h in range(v * local_heads // kv_local, (v + 1) * local_heads // kv_local):
            query = queries[:, h * HD : (h + 1) * HD].astype(jnp.float32)
            score = jnp.sum(query * key, axis=1, keepdims=True)
            fresh = jnp.where(lane == h, score, fresh)
    fresh_out[...] = fresh * UNIT


def attend_body(bias_ref, queries, cache, out, stacked, *, shift):
    kvb_count, seq_rep, own_width = queries.shape
    tp_count = lax.axis_size("tp")
    tokens = cache.shape[0] * BLK
    seq_total = kvb_count * seq_rep
    local_heads = own_width // HD
    group_size = QH // KVH
    kv_local = max(1, local_heads // group_size)
    per_kv = local_heads // kv_local
    bias = bias_ref[...]
    for r in range(kvb_count):
        stacked[r * seq_rep : (r + 1) * seq_rep, :] = queries[r].astype(jnp.float32)
    t = lax.axis_index("tp") + shift
    t = jnp.where(t < tp_count, t, t - tp_count)
    lane = lax.broadcasted_iota(jnp.int32, (seq_total, STATS), 1)
    stats = jnp.zeros((seq_total, STATS), jnp.float32)
    for v in range(kv_local):
        heads = range(v * per_kv, (v + 1) * per_kv)
        rows = jnp.concatenate(
            [stacked[:, h * HD : (h + 1) * HD] for h in heads], axis=0
        ).astype(jnp.bfloat16)
        g = t * local_heads // group_size + v
        at = pl.multiple_of(g * HD, HD)
        keys = cache[:, :, pl.ds(at, HD)].reshape(tokens, HD)
        at = pl.multiple_of((KVH + g) * HD, HD)
        values = cache[:, :, pl.ds(at, HD)].reshape(tokens, HD)
        scores = lax.dot_general(
            rows, keys, (((1,), (1,)), ((), ())), preferred_element_type=jnp.float32
        )
        scores = scores.reshape(per_kv, seq_total, tokens) * UNIT + bias[None]
        peaks = jnp.maximum(jnp.max(scores, axis=2, keepdims=True), FLOOR)
        peaks = peaks.astype(jnp.bfloat16).astype(jnp.float32)
        weights = jnp.exp2(scores - peaks)
        sums = jnp.sum(weights, axis=2, keepdims=True)
        partial = jnp.dot(
            weights.astype(jnp.bfloat16).reshape(per_kv * seq_total, tokens),
            values,
            preferred_element_type=jnp.float32,
        )
        high = sums.astype(jnp.bfloat16).astype(jnp.float32)
        low = sums - high
        for j, h in enumerate(heads):
            out[:, h * HD : (h + 1) * HD] = partial[j * seq_total : (j + 1) * seq_total].astype(
                jnp.bfloat16
            )
            for part, value in enumerate((peaks, high, low)):
                stats = jnp.where(lane == part * local_heads + h, value[j], stats)
    out[:, local_heads * HD :] = stats.astype(jnp.bfloat16)


def fetch_body(weight, *refs, first):
    chunk, arrived = refs[-2:]
    copy = pltpu.make_async_copy(weight.at[:, pl.ds(first, chunk.shape[1])], chunk, arrived)
    copy.start()
    copy.wait()


def unpack(ref, local_heads):
    stats = ref[:, local_heads * HD :].astype(jnp.float32)
    sums = stats[:, local_heads : 2 * local_heads] + stats[:, 2 * local_heads : 3 * local_heads]
    return stats[:, :local_heads], sums


def merge_body(*refs, sources):
    parts, outs = refs[:sources], refs[sources:]
    seq_total, width = parts[0].shape
    seq_rep = outs[0].shape[0]
    local_heads = (width - STATS) // HD
    pairs = [unpack(part, local_heads) for part in parts]
    peak = pairs[0][0]
    for other, _ in pairs[1:]:
        peak = jnp.maximum(peak, other)
    scaling = [jnp.exp2(p - peak) for p, _ in pairs]
    total = sum(s * c for s, (_, c) in zip(scaling, pairs))
    high = total.astype(jnp.bfloat16).astype(jnp.float32)
    pad = jnp.zeros((seq_total, STATS - 3 * local_heads), jnp.float32)
    stats = jnp.concatenate([peak, high, total - high, pad], axis=1)
    blocks = [
        sum(
            s[:, h : h + 1] * part[:, h * HD : (h + 1) * HD].astype(jnp.float32)
            for s, part in zip(scaling, parts)
        )
        for h in range(local_heads)
    ]
    for h, block in enumerate(blocks + [stats]):
        for r, out in enumerate(outs):
            out[:, h * HD : (h + 1) * HD] = block[r * seq_rep : (r + 1) * seq_rep].astype(
                jnp.bfloat16
            )


def project_body(*refs, sources):
    parts = refs[:sources]
    fresh_ref, value_ref, weight = refs[sources : sources + 3]
    pieces = len(LATE)
    chunks = list(refs[sources + 3 : -3 - pieces])
    out, *late = refs[-3 - pieces : -2]
    arrived, rows = refs[-2:]
    first = weight.shape[1] - sum(piece.shape[1] for piece in late)
    copies = []
    for n, piece in enumerate(late):
        columns = pl.ds(first, piece.shape[1])
        copies.append(pltpu.make_async_copy(weight.at[:, columns], piece, arrived.at[n]))
        copies[-1].start()
        first += piece.shape[1]
    def combine():
        local_heads = (parts[0].shape[1] - STATS) // HD
        kv_local = value_ref.shape[1] // HD
        pairs = [unpack(part, local_heads) for part in parts]
        fresh = fresh_ref[:, :local_heads]
        overall = fresh
        for peak, _ in pairs:
            overall = jnp.maximum(overall, peak)
        scaling = [jnp.exp2(peak - overall) for peak, _ in pairs]
        fresh_weight = jnp.exp2(fresh - overall)
        inverse = 1.0 / (fresh_weight + sum(s * c for s, (_, c) in zip(scaling, pairs)))
        scaling = [s * inverse for s in scaling]
        fresh_weight = fresh_weight * inverse
        attended = []
        for h in range(local_heads):
            v = h * kv_local // local_heads
            total = fresh_weight[:, h : h + 1] * value_ref[:, v * HD : (v + 1) * HD]
            for s, part in zip(scaling, parts):
                total = total + s[:, h : h + 1] * part[:, h * HD : (h + 1) * HD].astype(jnp.float32)
            attended.append(total.astype(jnp.bfloat16))
        rows[...] = jnp.concatenate(attended, axis=1)

    once(combine)
    attended = rows[...]
    first = 0
    for n, chunk in enumerate(chunks + late):
        if n >= len(chunks):
            copies[n - len(chunks)].wait()
        for at in range(0, chunk.shape[1], STEP):
            step = min(STEP, chunk.shape[1] - at)
            out[:, first + at : first + at + step] = jnp.dot(
                attended, chunk[:, at : at + step], preferred_element_type=jnp.float32
            ).astype(out.dtype)
        first += chunk.shape[1]


def finish_body(pieces, residual, gain, stream_out, normed_out):
    full = residual[...].astype(jnp.float32)
    width = full.shape[1]
    total = pieces[0].astype(jnp.float32)
    for t in range(1, pieces.shape[0]):
        total = total + pieces[t].astype(jnp.float32)
    full = (full + total).astype(jnp.bfloat16).astype(jnp.float32)
    mean_square = jnp.sum(full * full, axis=1, keepdims=True) / width
    inverse = lax.rsqrt(mean_square + EPSILON)
    own = stream_out.shape[1]
    at = pl.multiple_of(lax.axis_index("tp") * own, own)
    mine = residual[:, pl.ds(at, own)].astype(jnp.float32)
    total = pieces[0, :, pl.ds(at, own)].astype(jnp.float32)
    for t in range(1, pieces.shape[0]):
        total = total + pieces[t, :, pl.ds(at, own)].astype(jnp.float32)
    stream = (mine + total).astype(jnp.bfloat16)
    stream_out[...] = stream
    normed_out[...] = (stream.astype(jnp.float32) * inverse * gain[...].astype(jnp.float32)).astype(
        jnp.bfloat16
    )


def vmem():
    return pl.BlockSpec(memory_space=pltpu.VMEM)


def resident(array):
    return pltpu.with_memory_space_constraint(array, pltpu.VMEM)


def hbm():
    return pl.BlockSpec(memory_space=pltpu.HBM)


def on_device(
    residual,
    queries,
    new_kv,
    kv_cache,
    lengths,
    slot_seq,
    slot_block,
    block_counts,
    out_weight,
    norm_gain,
):
    tp_count = lax.axis_size("tp")
    kvb_count = lax.axis_size("kvb")
    seq_rep, own_width = queries.shape
    seq_total = kvb_count * seq_rep
    tokens = kv_cache.shape[0] * BLK
    kv_local = max(1, own_width // HD * KVH // QH)
    depth, columns = out_weight.shape
    out_weight = pltpu.with_memory_space_constraint(out_weight, pltpu.HBM)
    share = [columns * n // sum(SHARES) for n in SHARES]
    starts = [sum(share[:n]) for n in range(len(share))]
    arrived = [
        lax.ppermute(queries, "kvb", [(k, ahead(k, r, kvb_count)) for k in range(kvb_count)])
        for r in range(1, kvb_count)
    ]
    bias, fresh, fresh_values, own_queries, under_prepare = pl.pallas_call(
        lambda *refs: prepare_body(*refs, first=starts[0]),
        out_shape=(
            jax.ShapeDtypeStruct((seq_total, tokens), jnp.float32),
            jax.ShapeDtypeStruct((seq_rep, STATS), jnp.float32),
            jax.ShapeDtypeStruct((seq_rep, kv_local * HD), jnp.float32),
            jax.ShapeDtypeStruct((seq_rep, own_width), jnp.bfloat16),
            pltpu.VMEM((depth, share[0]), out_weight.dtype),
        ),
        in_specs=[pl.BlockSpec(memory_space=pltpu.SMEM)] + [hbm()] * 6,
        out_specs=(vmem(),) * 5,
        scratch_shapes=[
            pltpu.SMEM(lengths.shape, jnp.int32),
            pltpu.VMEM((1,) + slot_seq.shape, jnp.int32),
            pltpu.VMEM((1,) + slot_block.shape, jnp.int32),
            pltpu.VMEM(queries.shape, queries.dtype),
            pltpu.VMEM(new_kv.shape, new_kv.dtype),
            pltpu.SemaphoreType.DMA((5,)),
            pltpu.SemaphoreType.DMA,
        ],
        compiler_params=pltpu.CompilerParams(vmem_limit_bytes=4 << 20),
        cost_estimate=pl.CostEstimate(flops=COVER, transcendentals=0, bytes_accessed=1 << 20),
        name="prepare",
    )(block_counts, *[
        pltpu.with_memory_space_constraint(array, pltpu.HBM)
        for array in (lengths, slot_seq[None], slot_block[None], queries, new_kv)
    ], out_weight)
    wide = jnp.stack([own_queries] + arrived)
    cache = resident(kv_cache)

    def fetch(first, size, *after):
        return pl.pallas_call(
            lambda *refs: fetch_body(*refs, first=first),
            out_shape=pltpu.VMEM((depth, size), out_weight.dtype),
            in_specs=[hbm()] + [pl.BlockSpec(memory_space=pl.ANY)] * len(after),
            out_specs=vmem(),
            scratch_shapes=[pltpu.SemaphoreType.DMA],
            compiler_params=pltpu.CompilerParams(vmem_limit_bytes=1 << 20),
            cost_estimate=pl.CostEstimate(flops=COVER, transcendentals=0, bytes_accessed=1 << 20),
            name="fetch",
        )(out_weight, *after)

    def attend(rows, shift):
        return pl.pallas_call(
            lambda *refs: attend_body(*refs, shift=shift),
            out_shape=jax.ShapeDtypeStruct((seq_total, own_width + STATS), jnp.bfloat16),
            in_specs=[vmem(), vmem(), vmem()],
            out_specs=vmem(),
            scratch_shapes=[pltpu.VMEM((seq_total, own_width), jnp.float32)],
            compiler_params=pltpu.CompilerParams(vmem_limit_bytes=6 << 20),
            cost_estimate=pl.CostEstimate(flops=COVER, transcendentals=0, bytes_accessed=1 << 20),
            name="attend",
        )(bias, rows, cache)

    def shifted(rows, shift):
        return lax.ppermute(rows, "tp", [(t, (t + shift) % tp_count) for t in range(tp_count)])

    asked = [shifted(wide, -d) for d in range(1, tp_count)]
    parts = [attend(wide, 0)]
    chunks = [under_prepare]
    for d in range(1, tp_count):
        parts.append(shifted(attend(asked[d - 1], d), d))
    chunks.append(fetch(starts[1], share[1], parts[0]))
    block = jax.ShapeDtypeStruct((seq_rep, own_width + STATS), jnp.bfloat16)
    dealt = pl.pallas_call(
        lambda *refs: merge_body(*refs, sources=tp_count),
        out_shape=(block,) * kvb_count,
        in_specs=[vmem()] * tp_count,
        out_specs=(vmem(),) * kvb_count,
        compiler_params=pltpu.CompilerParams(vmem_limit_bytes=4 << 20),
        name="merge",
    )(*parts)
    parts = [
        lax.ppermute(dealt[r], "kvb", [(k, behind(k, r, kvb_count)) for k in range(kvb_count)])
        for r in reversed(range(1, kvb_count))
    ]
    parts.append(dealt[0])
    chunks.append(fetch(starts[2], share[2], dealt[0]))
    projected = pl.pallas_call(
        lambda *refs: project_body(*refs, sources=kvb_count),
        out_shape=jax.ShapeDtypeStruct((seq_rep, out_weight.shape[1]), jnp.bfloat16),
        in_specs=[vmem()] * (kvb_count + 2) + [hbm()] + [vmem()] * len(chunks),
        out_specs=vmem(),
        scratch_shapes=[
            *[pltpu.VMEM((depth, share[3] * n // sum(LATE)), out_weight.dtype) for n in LATE],
            pltpu.SemaphoreType.DMA((len(LATE),)),
            pltpu.VMEM((seq_rep, own_width), jnp.bfloat16),
        ],
        compiler_params=pltpu.CompilerParams(vmem_limit_bytes=18 << 20),
        name="project",
    )(*parts, fresh, fresh_values, out_weight, *chunks)
    pieces = lax.all_gather(projected, "tp", axis=0, tiled=False)
    own = jax.ShapeDtypeStruct((seq_rep, norm_gain.shape[0]), jnp.bfloat16)
    return pl.pallas_call(
        finish_body,
        out_shape=(own, own),
        in_specs=[vmem(), vmem(), vmem()],
        out_specs=(vmem(), vmem()),
        compiler_params=pltpu.CompilerParams(vmem_limit_bytes=4 << 20),
        name="finish",
    )(pieces, residual, norm_gain[None])


def solution(mesh):
    placed = (
        P(("groups", "kvb"), None),
        P(("groups", "kvb"), "tp"),
        P(("groups", "kvb"), None),
        P(("groups", "kvb", "tp"), None, None),
        P("groups"),
        P(("groups", "kvb", "tp")),
        P(("groups", "kvb", "tp")),
        P(("groups", "kvb", "tp")),
        P("tp", None),
        P("tp"),
    )
    return jax.shard_map(
        on_device,
        mesh=mesh,
        in_specs=placed,
        out_specs=(P(("groups", "kvb"), "tp"), P(("groups", "kvb"), "tp")),
        check_vma=False,
    )
```

```python
import jax
import jax.numpy as jnp
from jax import lax
from jax.experimental import pallas as pl
from jax.experimental.pallas import tpu as pltpu
from jax.sharding import PartitionSpec as P

QH = 64
KVH = 8
HD = 128
BLK = 16

MASKED = -1e30
FLOOR = -1e20
EPSILON = 1e-06
UNIT = HD ** (-0.5) * 1.4426950408889634
STATS = 128
COVER = 20_000_000_000
SHARES = (4, 4, 5, 7, 12)
LATE = (4, 4, 4)
STEP = 512


def ahead(index, step, count):
    if count & (count - 1) == 0:
        return index ^ step
    return (index + step) % count


def behind(index, step, count):
    if count & (count - 1) == 0:
        return index ^ step
    return (index - step + count) % count


def once(body):
    trips = jnp.where(lax.axis_index("tp") >= 0, 1, 0)

    def trip(_, carried):
        body()
        return carried

    lax.fori_loop(0, trips, trip, 0)


def beside(weight, chunk, arrived, first, body):
    copy = pltpu.make_async_copy(weight.at[:, pl.ds(first, chunk.shape[1])], chunk, arrived)
    copy.start()
    once(body)
    copy.wait()


def prepare_body(count, *refs, first):
    inputs, weight, outs, chunk = refs[:5], refs[5], refs[6:10], refs[10]
    held, arrived, landed = refs[11:16], refs[16], refs[17]
    copies = [
        pltpu.make_async_copy(source, target, arrived.at[n])
        for n, (source, target) in enumerate(zip(inputs, held))
    ]
    for copy in copies:
        copy.start()

    def run():
        for copy in copies:
            copy.wait()
        prepare(count, *held, *outs)

    beside(weight, chunk, landed, first, run)


def prepare(
    count, lengths, slot_seq, slot_block, queries, new_kv, bias, fresh_out, value_out, own_out
):
    seq_total, tokens = bias.shape
    slots = tokens // BLK
    seq_rep, own_width = queries.shape
    local_heads = own_width // HD
    group_size = QH // KVH
    kvb_count = seq_total // seq_rep
    seq = slot_seq[...]
    length_of = jnp.zeros_like(seq)
    for s in range(seq_total):
        length_of = jnp.where(seq == s, lengths[s], length_of)
    slot_ids = lax.broadcasted_iota(jnp.int32, seq.shape, 1)
    remaining = jnp.clip(length_of - slot_block[...] * BLK, 0, BLK)
    remaining = jnp.where(slot_ids < count[0], remaining, 0)
    row = lax.broadcasted_iota(jnp.int32, (8, slots), 0)
    codes = jnp.where(row == 0, seq, jnp.where(row == 1, remaining, 0))
    spread = (
        lax.broadcasted_iota(jnp.int32, (slots, tokens), 1) // BLK
        == lax.broadcasted_iota(jnp.int32, (slots, tokens), 0)
    )
    per_token = jnp.dot(
        codes.astype(jnp.float32).astype(jnp.bfloat16),
        jnp.where(spread, 1.0, 0.0).astype(jnp.bfloat16),
        preferred_element_type=jnp.float32,
    )
    row = lax.broadcasted_iota(jnp.int32, (seq_total, tokens), 0)
    replica = behind(lax.axis_index("kvb"), row // seq_rep, kvb_count)
    seq_ids = (replica * seq_rep + row % seq_rep).astype(jnp.float32)
    offsets = (lax.broadcasted_iota(jnp.int32, (seq_total, tokens), 1) % BLK).astype(jnp.float32)
    live = (per_token[0:1] == seq_ids) & (offsets < per_token[1:2])
    bias[...] = jnp.where(live, 0.0, MASKED)

    own_out[...] = queries[...]
    kv_local = max(1, local_heads // group_size)
    kv_first = lax.axis_index("tp") * local_heads // group_size
    lane = lax.broadcasted_iota(jnp.int32, (seq_rep, STATS), 1)
    fresh = jnp.zeros((seq_rep, STATS), jnp.float32)
    for v in range(kv_local):
        at = pl.multiple_of((kv_first + v) * HD, HD)
        key = new_kv[:, pl.ds(at, HD)].astype(jnp.float32)
        at = pl.multiple_of((KVH + kv_first + v) * HD, HD)
        value_out[:, v * HD : (v + 1) * HD] = new_kv[:, pl.ds(at, HD)].astype(jnp.float32)
        for h in range(v * local_heads // kv_local, (v + 1) * local_heads // kv_local):
            query = queries[:, h * HD : (h + 1) * HD].astype(jnp.float32)
            score = jnp.sum(query * key, axis=1, keepdims=True)
            fresh = jnp.where(lane == h, score, fresh)
    fresh_out[...] = fresh * UNIT


def attend_first_body(bias_ref, queries, cache, weight, out, chunk, stacked, arrived, *, first):
    run = lambda: attend_body(bias_ref, queries, cache, out, stacked, shift=0)
    beside(weight, chunk, arrived, first, run)


def attend_body(bias_ref, queries, cache, out, stacked, *, shift):
    kvb_count, seq_rep, own_width = queries.shape
    tp_count = lax.axis_size("tp")
    tokens = cache.shape[0] * BLK
    seq_total = kvb_count * seq_rep
    local_heads = own_width // HD
    group_size = QH // KVH
    kv_local = max(1, local_heads // group_size)
    per_kv = local_heads // kv_local
    bias = bias_ref[...]
    for r in range(kvb_count):
        stacked[r * seq_rep : (r + 1) * seq_rep, :] = queries[r].astype(jnp.float32)
    t = lax.axis_index("tp") + shift
    t = jnp.where(t < tp_count, t, t - tp_count)
    lane = lax.broadcasted_iota(jnp.int32, (seq_total, STATS), 1)
    stats = jnp.zeros((seq_total, STATS), jnp.float32)
    for v in range(kv_local):
        heads = range(v * per_kv, (v + 1) * per_kv)
        rows = jnp.concatenate(
            [stacked[:, h * HD : (h + 1) * HD] for h in heads], axis=0
        ).astype(jnp.bfloat16)
        g = t * local_heads // group_size + v
        at = pl.multiple_of(g * HD, HD)
        keys = cache[:, :, pl.ds(at, HD)].reshape(tokens, HD)
        at = pl.multiple_of((KVH + g) * HD, HD)
        values = cache[:, :, pl.ds(at, HD)].reshape(tokens, HD)
        scores = lax.dot_general(
            rows, keys, (((1,), (1,)), ((), ())), preferred_element_type=jnp.float32
        )
        scores = scores.reshape(per_kv, seq_total, tokens) * UNIT + bias[None]
        peaks = jnp.maximum(jnp.max(scores, axis=2, keepdims=True), FLOOR)
        peaks = peaks.astype(jnp.bfloat16).astype(jnp.float32)
        weights = jnp.exp2(scores - peaks)
        sums = jnp.sum(weights, axis=2, keepdims=True)
        partial = jnp.dot(
            weights.astype(jnp.bfloat16).reshape(per_kv * seq_total, tokens),
            values,
            preferred_element_type=jnp.float32,
        )
        high = sums.astype(jnp.bfloat16).astype(jnp.float32)
        low = sums - high
        for j, h in enumerate(heads):
            out[:, h * HD : (h + 1) * HD] = partial[j * seq_total : (j + 1) * seq_total].astype(
                jnp.bfloat16
            )
            for part, value in enumerate((peaks, high, low)):
                stats = jnp.where(lane == part * local_heads + h, value[j], stats)
    out[:, local_heads * HD :] = stats.astype(jnp.bfloat16)


def fetch_body(weight, *refs, first):
    chunk, arrived = refs[-2:]
    copy = pltpu.make_async_copy(weight.at[:, pl.ds(first, chunk.shape[1])], chunk, arrived)
    copy.start()
    copy.wait()


def unpack(ref, local_heads):
    stats = ref[:, local_heads * HD :].astype(jnp.float32)
    sums = stats[:, local_heads : 2 * local_heads] + stats[:, 2 * local_heads : 3 * local_heads]
    return stats[:, :local_heads], sums


def merge_body(*refs, sources):
    parts, outs = refs[:sources], refs[sources:]
    seq_total, width = parts[0].shape
    seq_rep = outs[0].shape[0]
    local_heads = (width - STATS) // HD
    pairs = [unpack(part, local_heads) for part in parts]
    peak = pairs[0][0]
    for other, _ in pairs[1:]:
        peak = jnp.maximum(peak, other)
    scaling = [jnp.exp2(p - peak) for p, _ in pairs]
    total = sum(s * c for s, (_, c) in zip(scaling, pairs))
    high = total.astype(jnp.bfloat16).astype(jnp.float32)
    pad = jnp.zeros((seq_total, STATS - 3 * local_heads), jnp.float32)
    stats = jnp.concatenate([peak, high, total - high, pad], axis=1)
    blocks = [
        sum(
            s[:, h : h + 1] * part[:, h * HD : (h + 1) * HD].astype(jnp.float32)
            for s, part in zip(scaling, parts)
        )
        for h in range(local_heads)
    ]
    for h, block in enumerate(blocks + [stats]):
        for r, out in enumerate(outs):
            out[:, h * HD : (h + 1) * HD] = block[r * seq_rep : (r + 1) * seq_rep].astype(
                jnp.bfloat16
            )


def project_body(*refs, sources):
    parts = refs[:sources]
    fresh_ref, value_ref, weight = refs[sources : sources + 3]
    pieces = len(LATE)
    chunks = list(refs[sources + 3 : -3 - pieces])
    out, *late = refs[-3 - pieces : -2]
    arrived, rows = refs[-2:]
    first = weight.shape[1] - sum(piece.shape[1] for piece in late)
    copies = []
    for n, piece in enumerate(late):
        columns = pl.ds(first, piece.shape[1])
        copies.append(pltpu.make_async_copy(weight.at[:, columns], piece, arrived.at[n]))
        copies[-1].start()
        first += piece.shape[1]
    def combine():
        local_heads = (parts[0].shape[1] - STATS) // HD
        kv_local = value_ref.shape[1] // HD
        pairs = [unpack(part, local_heads) for part in parts]
        fresh = fresh_ref[:, :local_heads]
        overall = fresh
        for peak, _ in pairs:
            overall = jnp.maximum(overall, peak)
        scaling = [jnp.exp2(peak - overall) for peak, _ in pairs]
        fresh_weight = jnp.exp2(fresh - overall)
        inverse = 1.0 / (fresh_weight + sum(s * c for s, (_, c) in zip(scaling, pairs)))
        scaling = [s * inverse for s in scaling]
        fresh_weight = fresh_weight * inverse
        attended = []
        for h in range(local_heads):
            v = h * kv_local // local_heads
            total = fresh_weight[:, h : h + 1] * value_ref[:, v * HD : (v + 1) * HD]
            for s, part in zip(scaling, parts):
                total = total + s[:, h : h + 1] * part[:, h * HD : (h + 1) * HD].astype(jnp.float32)
            attended.append(total.astype(jnp.bfloat16))
        rows[...] = jnp.concatenate(attended, axis=1)

    once(combine)
    attended = rows[...]
    first = 0
    for n, chunk in enumerate(chunks + late):
        if n >= len(chunks):
            copies[n - len(chunks)].wait()
        for at in range(0, chunk.shape[1], STEP):
            step = min(STEP, chunk.shape[1] - at)
            out[:, first + at : first + at + step] = jnp.dot(
                attended, chunk[:, at : at + step], preferred_element_type=jnp.float32
            ).astype(out.dtype)
        first += chunk.shape[1]


def finish_body(pieces, residual, gain, stream_out, normed_out):
    full = residual[...].astype(jnp.float32)
    width = full.shape[1]
    total = pieces[0].astype(jnp.float32)
    for t in range(1, pieces.shape[0]):
        total = total + pieces[t].astype(jnp.float32)
    full = (full + total).astype(jnp.bfloat16).astype(jnp.float32)
    mean_square = jnp.sum(full * full, axis=1, keepdims=True) / width
    inverse = lax.rsqrt(mean_square + EPSILON)
    own = stream_out.shape[1]
    at = pl.multiple_of(lax.axis_index("tp") * own, own)
    mine = residual[:, pl.ds(at, own)].astype(jnp.float32)
    total = pieces[0, :, pl.ds(at, own)].astype(jnp.float32)
    for t in range(1, pieces.shape[0]):
        total = total + pieces[t, :, pl.ds(at, own)].astype(jnp.float32)
    stream = (mine + total).astype(jnp.bfloat16)
    stream_out[...] = stream
    normed_out[...] = (stream.astype(jnp.float32) * inverse * gain[...].astype(jnp.float32)).astype(
        jnp.bfloat16
    )


def vmem():
    return pl.BlockSpec(memory_space=pltpu.VMEM)


def resident(array):
    return pltpu.with_memory_space_constraint(array, pltpu.VMEM)


def hbm():
    return pl.BlockSpec(memory_space=pltpu.HBM)


def on_device(
    residual,
    queries,
    new_kv,
    kv_cache,
    lengths,
    slot_seq,
    slot_block,
    block_counts,
    out_weight,
    norm_gain,
):
    tp_count = lax.axis_size("tp")
    kvb_count = lax.axis_size("kvb")
    seq_rep, own_width = queries.shape
    seq_total = kvb_count * seq_rep
    tokens = kv_cache.shape[0] * BLK
    kv_local = max(1, own_width // HD * KVH // QH)
    depth, columns = out_weight.shape
    out_weight = pltpu.with_memory_space_constraint(out_weight, pltpu.HBM)
    share = [columns * n // sum(SHARES) for n in SHARES]
    starts = [sum(share[:n]) for n in range(len(share))]
    arrived = [
        lax.ppermute(queries, "kvb", [(k, ahead(k, r, kvb_count)) for k in range(kvb_count)])
        for r in range(1, kvb_count)
    ]
    bias, fresh, fresh_values, own_queries, under_prepare = pl.pallas_call(
        lambda *refs: prepare_body(*refs, first=starts[0]),
        out_shape=(
            jax.ShapeDtypeStruct((seq_total, tokens), jnp.float32),
            jax.ShapeDtypeStruct((seq_rep, STATS), jnp.float32),
            jax.ShapeDtypeStruct((seq_rep, kv_local * HD), jnp.float32),
            jax.ShapeDtypeStruct((seq_rep, own_width), jnp.bfloat16),
            pltpu.VMEM((depth, share[0]), out_weight.dtype),
        ),
        in_specs=[pl.BlockSpec(memory_space=pltpu.SMEM)] + [hbm()] * 6,
        out_specs=(vmem(),) * 5,
        scratch_shapes=[
            pltpu.SMEM(lengths.shape, jnp.int32),
            pltpu.VMEM((1,) + slot_seq.shape, jnp.int32),
            pltpu.VMEM((1,) + slot_block.shape, jnp.int32),
            pltpu.VMEM(queries.shape, queries.dtype),
            pltpu.VMEM(new_kv.shape, new_kv.dtype),
            pltpu.SemaphoreType.DMA((5,)),
            pltpu.SemaphoreType.DMA,
        ],
        compiler_params=pltpu.CompilerParams(vmem_limit_bytes=4 << 20),
        cost_estimate=pl.CostEstimate(flops=COVER, transcendentals=0, bytes_accessed=1 << 20),
        name="prepare",
    )(block_counts, *[
        pltpu.with_memory_space_constraint(array, pltpu.HBM)
        for array in (lengths, slot_seq[None], slot_block[None], queries, new_kv)
    ], out_weight)
    wide = jnp.stack([own_queries] + arrived)
    cache = resident(kv_cache)

    def fetch(first, size, *after):
        return pl.pallas_call(
            lambda *refs: fetch_body(*refs, first=first),
            out_shape=pltpu.VMEM((depth, size), out_weight.dtype),
            in_specs=[hbm()] + [pl.BlockSpec(memory_space=pl.ANY)] * len(after),
            out_specs=vmem(),
            scratch_shapes=[pltpu.SemaphoreType.DMA],
            compiler_params=pltpu.CompilerParams(vmem_limit_bytes=1 << 20),
            cost_estimate=pl.CostEstimate(flops=COVER, transcendentals=0, bytes_accessed=1 << 20),
            name="fetch",
        )(out_weight, *after)

    def attend(rows, shift):
        return pl.pallas_call(
            lambda *refs: attend_body(*refs, shift=shift),
            out_shape=jax.ShapeDtypeStruct((seq_total, own_width + STATS), jnp.bfloat16),
            in_specs=[vmem(), vmem(), vmem()],
            out_specs=vmem(),
            scratch_shapes=[pltpu.VMEM((seq_total, own_width), jnp.float32)],
            compiler_params=pltpu.CompilerParams(vmem_limit_bytes=6 << 20),
            cost_estimate=pl.CostEstimate(flops=COVER, transcendentals=0, bytes_accessed=1 << 20),
            name="attend",
        )(bias, rows, cache)

    def shifted(rows, shift):
        return lax.ppermute(rows, "tp", [(t, (t + shift) % tp_count) for t in range(tp_count)])

    first_part, under_attend = pl.pallas_call(
        lambda *refs: attend_first_body(*refs, first=starts[1]),
        out_shape=(
            jax.ShapeDtypeStruct((seq_total, own_width + STATS), jnp.bfloat16),
            pltpu.VMEM((depth, share[1]), out_weight.dtype),
        ),
        in_specs=[vmem(), vmem(), vmem(), hbm()],
        out_specs=(vmem(), vmem()),
        scratch_shapes=[
            pltpu.VMEM((seq_total, own_width), jnp.float32),
            pltpu.SemaphoreType.DMA,
        ],
        compiler_params=pltpu.CompilerParams(vmem_limit_bytes=6 << 20),
        cost_estimate=pl.CostEstimate(flops=COVER, transcendentals=0, bytes_accessed=1 << 20),
        name="attend_first",
    )(bias, wide, cache, out_weight)
    asked = [shifted(wide, -d) for d in range(1, tp_count)]
    parts = [first_part]
    chunks = [under_prepare, under_attend]
    for d in range(1, tp_count):
        parts.append(shifted(attend(asked[d - 1], d), d))
    chunks.append(fetch(starts[2], share[2], parts[0]))
    block = jax.ShapeDtypeStruct((seq_rep, own_width + STATS), jnp.bfloat16)
    dealt = pl.pallas_call(
        lambda *refs: merge_body(*refs, sources=tp_count),
        out_shape=(block,) * kvb_count,
        in_specs=[vmem()] * tp_count,
        out_specs=(vmem(),) * kvb_count,
        compiler_params=pltpu.CompilerParams(vmem_limit_bytes=4 << 20),
        name="merge",
    )(*parts)
    parts = [
        lax.ppermute(dealt[r], "kvb", [(k, behind(k, r, kvb_count)) for k in range(kvb_count)])
        for r in reversed(range(1, kvb_count))
    ]
    parts.append(dealt[0])
    chunks.append(fetch(starts[3], share[3], dealt[0]))
    projected = pl.pallas_call(
        lambda *refs: project_body(*refs, sources=kvb_count),
        out_shape=jax.ShapeDtypeStruct((seq_rep, out_weight.shape[1]), jnp.bfloat16),
        in_specs=[vmem()] * (kvb_count + 2) + [hbm()] + [vmem()] * len(chunks),
        out_specs=vmem(),
        scratch_shapes=[
            *[pltpu.VMEM((depth, share[4] * n // sum(LATE)), out_weight.dtype) for n in LATE],
            pltpu.SemaphoreType.DMA((len(LATE),)),
            pltpu.VMEM((seq_rep, own_width), jnp.bfloat16),
        ],
        compiler_params=pltpu.CompilerParams(vmem_limit_bytes=18 << 20),
        name="project",
    )(*parts, fresh, fresh_values, out_weight, *chunks)
    pieces = lax.all_gather(projected, "tp", axis=0, tiled=False)
    own = jax.ShapeDtypeStruct((seq_rep, norm_gain.shape[0]), jnp.bfloat16)
    return pl.pallas_call(
        finish_body,
        out_shape=(own, own),
        in_specs=[vmem(), vmem(), vmem()],
        out_specs=(vmem(), vmem()),
        compiler_params=pltpu.CompilerParams(vmem_limit_bytes=4 << 20),
        name="finish",
    )(pieces, residual, norm_gain[None])


def solution(mesh):
    placed = (
        P(("groups", "kvb"), None),
        P(("groups", "kvb"), "tp"),
        P(("groups", "kvb"), None),
        P(("groups", "kvb", "tp"), None, None),
        P("groups"),
        P(("groups", "kvb", "tp")),
        P(("groups", "kvb", "tp")),
        P(("groups", "kvb", "tp")),
        P("tp", None),
        P("tp"),
    )
    return jax.shard_map(
        on_device,
        mesh=mesh,
        in_specs=placed,
        out_specs=(P(("groups", "kvb"), "tp"), P(("groups", "kvb"), "tp")),
        check_vma=False,
    )
```

```python
import jax
import jax.numpy as jnp
from jax import lax
from jax.experimental import pallas as pl
from jax.experimental.pallas import tpu as pltpu
from jax.sharding import PartitionSpec as P

QH = 64
KVH = 8
HD = 128
BLK = 16

MASKED = -1e30
FLOOR = -1e20
EPSILON = 1e-06
UNIT = HD ** (-0.5) * 1.4426950408889634
STATS = 128
COVER = 20_000_000_000
SHARES = (4, 4, 5, 7, 12)
LATE = (5, 3, 2, 2)
STEP = 512


def ahead(index, step, count):
    if count & (count - 1) == 0:
        return index ^ step
    return (index + step) % count


def behind(index, step, count):
    if count & (count - 1) == 0:
        return index ^ step
    return (index - step + count) % count


def once(body):
    trips = jnp.where(lax.axis_index("tp") >= 0, 1, 0)

    def trip(_, carried):
        body()
        return carried

    lax.fori_loop(0, trips, trip, 0)


def beside(weight, chunk, arrived, first, body):
    copy = pltpu.make_async_copy(weight.at[:, pl.ds(first, chunk.shape[1])], chunk, arrived)
    copy.start()
    once(body)
    copy.wait()


def prepare_body(count, *refs, first):
    inputs, weight, outs, chunk = refs[:5], refs[5], refs[6:10], refs[10]
    held, arrived, landed = refs[11:16], refs[16], refs[17]
    copies = [
        pltpu.make_async_copy(source, target, arrived.at[n])
        for n, (source, target) in enumerate(zip(inputs, held))
    ]
    for copy in copies:
        copy.start()

    def run():
        for copy in copies:
            copy.wait()
        prepare(count, *held, *outs)

    beside(weight, chunk, landed, first, run)


def prepare(
    count, lengths, slot_seq, slot_block, queries, new_kv, bias, fresh_out, value_out, own_out
):
    seq_total, tokens = bias.shape
    slots = tokens // BLK
    seq_rep, own_width = queries.shape
    local_heads = own_width // HD
    group_size = QH // KVH
    kvb_count = seq_total // seq_rep
    seq = slot_seq[...]
    length_of = jnp.zeros_like(seq)
    for s in range(seq_total):
        length_of = jnp.where(seq == s, lengths[s], length_of)
    slot_ids = lax.broadcasted_iota(jnp.int32, seq.shape, 1)
    remaining = jnp.clip(length_of - slot_block[...] * BLK, 0, BLK)
    remaining = jnp.where(slot_ids < count[0], remaining, 0)
    row = lax.broadcasted_iota(jnp.int32, (8, slots), 0)
    codes = jnp.where(row == 0, seq, jnp.where(row == 1, remaining, 0))
    spread = (
        lax.broadcasted_iota(jnp.int32, (slots, tokens), 1) // BLK
        == lax.broadcasted_iota(jnp.int32, (slots, tokens), 0)
    )
    per_token = jnp.dot(
        codes.astype(jnp.float32).astype(jnp.bfloat16),
        jnp.where(spread, 1.0, 0.0).astype(jnp.bfloat16),
        preferred_element_type=jnp.float32,
    )
    row = lax.broadcasted_iota(jnp.int32, (seq_total, tokens), 0)
    replica = behind(lax.axis_index("kvb"), row // seq_rep, kvb_count)
    seq_ids = (replica * seq_rep + row % seq_rep).astype(jnp.float32)
    offsets = (lax.broadcasted_iota(jnp.int32, (seq_total, tokens), 1) % BLK).astype(jnp.float32)
    live = (per_token[0:1] == seq_ids) & (offsets < per_token[1:2])
    bias[...] = jnp.where(live, 0.0, MASKED)

    own_out[...] = queries[...]
    kv_local = max(1, local_heads // group_size)
    kv_first = lax.axis_index("tp") * local_heads // group_size
    lane = lax.broadcasted_iota(jnp.int32, (seq_rep, STATS), 1)
    fresh = jnp.zeros((seq_rep, STATS), jnp.float32)
    for v in range(kv_local):
        at = pl.multiple_of((kv_first + v) * HD, HD)
        key = new_kv[:, pl.ds(at, HD)].astype(jnp.float32)
        at = pl.multiple_of((KVH + kv_first + v) * HD, HD)
        value_out[:, v * HD : (v + 1) * HD] = new_kv[:, pl.ds(at, HD)].astype(jnp.float32)
        for h in range(v * local_heads // kv_local, (v + 1) * local_heads // kv_local):
            query = queries[:, h * HD : (h + 1) * HD].astype(jnp.float32)
            score = jnp.sum(query * key, axis=1, keepdims=True)
            fresh = jnp.where(lane == h, score, fresh)
    fresh_out[...] = fresh * UNIT


def attend_first_body(bias_ref, queries, cache, weight, out, chunk, stacked, arrived, *, first):
    run = lambda: attend_body(bias_ref, queries, cache, out, stacked, shift=0)
    beside(weight, chunk, arrived, first, run)


def attend_body(bias_ref, queries, cache, out, stacked, *, shift):
    kvb_count, seq_rep, own_width = queries.shape
    tp_count = lax.axis_size("tp")
    tokens = cache.shape[0] * BLK
    seq_total = kvb_count * seq_rep
    local_heads = own_width // HD
    group_size = QH // KVH
    kv_local = max(1, local_heads // group_size)
    per_kv = local_heads // kv_local
    bias = bias_ref[...]
    for r in range(kvb_count):
        stacked[r * seq_rep : (r + 1) * seq_rep, :] = queries[r].astype(jnp.float32)
    t = lax.axis_index("tp") + shift
    t = jnp.where(t < tp_count, t, t - tp_count)
    lane = lax.broadcasted_iota(jnp.int32, (seq_total, STATS), 1)
    stats = jnp.zeros((seq_total, STATS), jnp.float32)
    for v in range(kv_local):
        heads = range(v * per_kv, (v + 1) * per_kv)
        rows = jnp.concatenate(
            [stacked[:, h * HD : (h + 1) * HD] for h in heads], axis=0
        ).astype(jnp.bfloat16)
        g = t * local_heads // group_size + v
        at = pl.multiple_of(g * HD, HD)
        keys = cache[:, :, pl.ds(at, HD)].reshape(tokens, HD)
        at = pl.multiple_of((KVH + g) * HD, HD)
        values = cache[:, :, pl.ds(at, HD)].reshape(tokens, HD)
        scores = lax.dot_general(
            rows, keys, (((1,), (1,)), ((), ())), preferred_element_type=jnp.float32
        )
        scores = scores.reshape(per_kv, seq_total, tokens) * UNIT + bias[None]
        peaks = jnp.maximum(jnp.max(scores, axis=2, keepdims=True), FLOOR)
        peaks = peaks.astype(jnp.bfloat16).astype(jnp.float32)
        weights = jnp.exp2(scores - peaks)
        sums = jnp.sum(weights, axis=2, keepdims=True)
        partial = jnp.dot(
            weights.astype(jnp.bfloat16).reshape(per_kv * seq_total, tokens),
            values,
            preferred_element_type=jnp.float32,
        )
        high = sums.astype(jnp.bfloat16).astype(jnp.float32)
        low = sums - high
        for j, h in enumerate(heads):
            out[:, h * HD : (h + 1) * HD] = partial[j * seq_total : (j + 1) * seq_total].astype(
                jnp.bfloat16
            )
            for part, value in enumerate((peaks, high, low)):
                stats = jnp.where(lane == part * local_heads + h, value[j], stats)
    out[:, local_heads * HD :] = stats.astype(jnp.bfloat16)


def fetch_body(weight, *refs, first):
    chunk, arrived = refs[-2:]
    copy = pltpu.make_async_copy(weight.at[:, pl.ds(first, chunk.shape[1])], chunk, arrived)
    copy.start()
    copy.wait()


def unpack(ref, local_heads):
    stats = ref[:, local_heads * HD :].astype(jnp.float32)
    sums = stats[:, local_heads : 2 * local_heads] + stats[:, 2 * local_heads : 3 * local_heads]
    return stats[:, :local_heads], sums


def merge_body(*refs, sources):
    parts, outs = refs[:sources], refs[sources:]
    seq_total, width = parts[0].shape
    seq_rep = outs[0].shape[0]
    local_heads = (width - STATS) // HD
    pairs = [unpack(part, local_heads) for part in parts]
    peak = pairs[0][0]
    for other, _ in pairs[1:]:
        peak = jnp.maximum(peak, other)
    scaling = [jnp.exp2(p - peak) for p, _ in pairs]
    total = sum(s * c for s, (_, c) in zip(scaling, pairs))
    high = total.astype(jnp.bfloat16).astype(jnp.float32)
    pad = jnp.zeros((seq_total, STATS - 3 * local_heads), jnp.float32)
    stats = jnp.concatenate([peak, high, total - high, pad], axis=1)
    blocks = [
        sum(
            s[:, h : h + 1] * part[:, h * HD : (h + 1) * HD].astype(jnp.float32)
            for s, part in zip(scaling, parts)
        )
        for h in range(local_heads)
    ]
    for h, block in enumerate(blocks + [stats]):
        for r, out in enumerate(outs):
            out[:, h * HD : (h + 1) * HD] = block[r * seq_rep : (r + 1) * seq_rep].astype(
                jnp.bfloat16
            )


def project_body(*refs, sources):
    parts = refs[:sources]
    fresh_ref, value_ref, weight = refs[sources : sources + 3]
    pieces = len(LATE)
    chunks = list(refs[sources + 3 : -3 - pieces])
    out, *late = refs[-3 - pieces : -2]
    arrived, rows = refs[-2:]
    first = weight.shape[1] - sum(piece.shape[1] for piece in late)
    copies = []
    for n, piece in enumerate(late):
        columns = pl.ds(first, piece.shape[1])
        copies.append(pltpu.make_async_copy(weight.at[:, columns], piece, arrived.at[n]))
        copies[-1].start()
        first += piece.shape[1]
    def combine():
        local_heads = (parts[0].shape[1] - STATS) // HD
        kv_local = value_ref.shape[1] // HD
        pairs = [unpack(part, local_heads) for part in parts]
        fresh = fresh_ref[:, :local_heads]
        overall = fresh
        for peak, _ in pairs:
            overall = jnp.maximum(overall, peak)
        scaling = [jnp.exp2(peak - overall) for peak, _ in pairs]
        fresh_weight = jnp.exp2(fresh - overall)
        inverse = 1.0 / (fresh_weight + sum(s * c for s, (_, c) in zip(scaling, pairs)))
        scaling = [s * inverse for s in scaling]
        fresh_weight = fresh_weight * inverse
        attended = []
        for h in range(local_heads):
            v = h * kv_local // local_heads
            total = fresh_weight[:, h : h + 1] * value_ref[:, v * HD : (v + 1) * HD]
            for s, part in zip(scaling, parts):
                total = total + s[:, h : h + 1] * part[:, h * HD : (h + 1) * HD].astype(jnp.float32)
            attended.append(total.astype(jnp.bfloat16))
        rows[...] = jnp.concatenate(attended, axis=1)

    once(combine)
    attended = rows[...]
    first = 0
    for n, chunk in enumerate(chunks + late):
        if n >= len(chunks):
            copies[n - len(chunks)].wait()
        for at in range(0, chunk.shape[1], STEP):
            step = min(STEP, chunk.shape[1] - at)
            out[:, first + at : first + at + step] = jnp.dot(
                attended, chunk[:, at : at + step], preferred_element_type=jnp.float32
            ).astype(out.dtype)
        first += chunk.shape[1]


def finish_body(pieces, residual, gain, stream_out, normed_out):
    full = residual[...].astype(jnp.float32)
    width = full.shape[1]
    total = pieces[0].astype(jnp.float32)
    for t in range(1, pieces.shape[0]):
        total = total + pieces[t].astype(jnp.float32)
    full = (full + total).astype(jnp.bfloat16).astype(jnp.float32)
    mean_square = jnp.sum(full * full, axis=1, keepdims=True) / width
    inverse = lax.rsqrt(mean_square + EPSILON)
    own = stream_out.shape[1]
    at = pl.multiple_of(lax.axis_index("tp") * own, own)
    mine = residual[:, pl.ds(at, own)].astype(jnp.float32)
    total = pieces[0, :, pl.ds(at, own)].astype(jnp.float32)
    for t in range(1, pieces.shape[0]):
        total = total + pieces[t, :, pl.ds(at, own)].astype(jnp.float32)
    stream = (mine + total).astype(jnp.bfloat16)
    stream_out[...] = stream
    normed_out[...] = (stream.astype(jnp.float32) * inverse * gain[...].astype(jnp.float32)).astype(
        jnp.bfloat16
    )


def vmem():
    return pl.BlockSpec(memory_space=pltpu.VMEM)


def resident(array):
    return pltpu.with_memory_space_constraint(array, pltpu.VMEM)


def hbm():
    return pl.BlockSpec(memory_space=pltpu.HBM)


def on_device(
    residual,
    queries,
    new_kv,
    kv_cache,
    lengths,
    slot_seq,
    slot_block,
    block_counts,
    out_weight,
    norm_gain,
):
    tp_count = lax.axis_size("tp")
    kvb_count = lax.axis_size("kvb")
    seq_rep, own_width = queries.shape
    seq_total = kvb_count * seq_rep
    tokens = kv_cache.shape[0] * BLK
    kv_local = max(1, own_width // HD * KVH // QH)
    depth, columns = out_weight.shape
    out_weight = pltpu.with_memory_space_constraint(out_weight, pltpu.HBM)
    share = [columns * n // sum(SHARES) for n in SHARES]
    starts = [sum(share[:n]) for n in range(len(share))]
    arrived = [
        lax.ppermute(queries, "kvb", [(k, ahead(k, r, kvb_count)) for k in range(kvb_count)])
        for r in range(1, kvb_count)
    ]
    bias, fresh, fresh_values, own_queries, under_prepare = pl.pallas_call(
        lambda *refs: prepare_body(*refs, first=starts[0]),
        out_shape=(
            jax.ShapeDtypeStruct((seq_total, tokens), jnp.float32),
            jax.ShapeDtypeStruct((seq_rep, STATS), jnp.float32),
            jax.ShapeDtypeStruct((seq_rep, kv_local * HD), jnp.float32),
            jax.ShapeDtypeStruct((seq_rep, own_width), jnp.bfloat16),
            pltpu.VMEM((depth, share[0]), out_weight.dtype),
        ),
        in_specs=[pl.BlockSpec(memory_space=pltpu.SMEM)] + [hbm()] * 6,
        out_specs=(vmem(),) * 5,
        scratch_shapes=[
            pltpu.SMEM(lengths.shape, jnp.int32),
            pltpu.VMEM((1,) + slot_seq.shape, jnp.int32),
            pltpu.VMEM((1,) + slot_block.shape, jnp.int32),
            pltpu.VMEM(queries.shape, queries.dtype),
            pltpu.VMEM(new_kv.shape, new_kv.dtype),
            pltpu.SemaphoreType.DMA((5,)),
            pltpu.SemaphoreType.DMA,
        ],
        compiler_params=pltpu.CompilerParams(vmem_limit_bytes=4 << 20),
        cost_estimate=pl.CostEstimate(flops=COVER, transcendentals=0, bytes_accessed=1 << 20),
        name="prepare",
    )(block_counts, *[
        pltpu.with_memory_space_constraint(array, pltpu.HBM)
        for array in (lengths, slot_seq[None], slot_block[None], queries, new_kv)
    ], out_weight)
    wide = jnp.stack([own_queries] + arrived)
    cache = resident(kv_cache)

    def fetch(first, size, *after):
        return pl.pallas_call(
            lambda *refs: fetch_body(*refs, first=first),
            out_shape=pltpu.VMEM((depth, size), out_weight.dtype),
            in_specs=[hbm()] + [pl.BlockSpec(memory_space=pl.ANY)] * len(after),
            out_specs=vmem(),
            scratch_shapes=[pltpu.SemaphoreType.DMA],
            compiler_params=pltpu.CompilerParams(vmem_limit_bytes=1 << 20),
            cost_estimate=pl.CostEstimate(flops=COVER, transcendentals=0, bytes_accessed=1 << 20),
            name="fetch",
        )(out_weight, *after)

    def attend(rows, shift):
        return pl.pallas_call(
            lambda *refs: attend_body(*refs, shift=shift),
            out_shape=jax.ShapeDtypeStruct((seq_total, own_width + STATS), jnp.bfloat16),
            in_specs=[vmem(), vmem(), vmem()],
            out_specs=vmem(),
            scratch_shapes=[pltpu.VMEM((seq_total, own_width), jnp.float32)],
            compiler_params=pltpu.CompilerParams(vmem_limit_bytes=6 << 20),
            cost_estimate=pl.CostEstimate(flops=COVER, transcendentals=0, bytes_accessed=1 << 20),
            name="attend",
        )(bias, rows, cache)

    def shifted(rows, shift):
        return lax.ppermute(rows, "tp", [(t, (t + shift) % tp_count) for t in range(tp_count)])

    first_part, under_attend = pl.pallas_call(
        lambda *refs: attend_first_body(*refs, first=starts[1]),
        out_shape=(
            jax.ShapeDtypeStruct((seq_total, own_width + STATS), jnp.bfloat16),
            pltpu.VMEM((depth, share[1]), out_weight.dtype),
        ),
        in_specs=[vmem(), vmem(), vmem(), hbm()],
        out_specs=(vmem(), vmem()),
        scratch_shapes=[
            pltpu.VMEM((seq_total, own_width), jnp.float32),
            pltpu.SemaphoreType.DMA,
        ],
        compiler_params=pltpu.CompilerParams(vmem_limit_bytes=6 << 20),
        cost_estimate=pl.CostEstimate(flops=COVER, transcendentals=0, bytes_accessed=1 << 20),
        name="attend_first",
    )(bias, wide, cache, out_weight)
    asked = [shifted(wide, -d) for d in range(1, tp_count)]
    parts = [first_part]
    chunks = [under_prepare, under_attend]
    for d in range(1, tp_count):
        parts.append(shifted(attend(asked[d - 1], d), d))
    chunks.append(fetch(starts[2], share[2], parts[0]))
    block = jax.ShapeDtypeStruct((seq_rep, own_width + STATS), jnp.bfloat16)
    dealt = pl.pallas_call(
        lambda *refs: merge_body(*refs, sources=tp_count),
        out_shape=(block,) * kvb_count,
        in_specs=[vmem()] * tp_count,
        out_specs=(vmem(),) * kvb_count,
        compiler_params=pltpu.CompilerParams(vmem_limit_bytes=4 << 20),
        name="merge",
    )(*parts)
    parts = [
        lax.ppermute(dealt[r], "kvb", [(k, behind(k, r, kvb_count)) for k in range(kvb_count)])
        for r in reversed(range(1, kvb_count))
    ]
    parts.append(dealt[0])
    chunks.append(fetch(starts[3], share[3], dealt[0]))
    projected = pl.pallas_call(
        lambda *refs: project_body(*refs, sources=kvb_count),
        out_shape=jax.ShapeDtypeStruct((seq_rep, out_weight.shape[1]), jnp.bfloat16),
        in_specs=[vmem()] * (kvb_count + 2) + [hbm()] + [vmem()] * len(chunks),
        out_specs=vmem(),
        scratch_shapes=[
            *[pltpu.VMEM((depth, share[4] * n // sum(LATE)), out_weight.dtype) for n in LATE],
            pltpu.SemaphoreType.DMA((len(LATE),)),
            pltpu.VMEM((seq_rep, own_width), jnp.bfloat16),
        ],
        compiler_params=pltpu.CompilerParams(vmem_limit_bytes=18 << 20),
        name="project",
    )(*parts, fresh, fresh_values, out_weight, *chunks)
    pieces = lax.all_gather(projected, "tp", axis=0, tiled=False)
    own = jax.ShapeDtypeStruct((seq_rep, norm_gain.shape[0]), jnp.bfloat16)
    return pl.pallas_call(
        finish_body,
        out_shape=(own, own),
        in_specs=[vmem(), vmem(), vmem()],
        out_specs=(vmem(), vmem()),
        compiler_params=pltpu.CompilerParams(vmem_limit_bytes=4 << 20),
        name="finish",
    )(pieces, residual, norm_gain[None])


def solution(mesh):
    placed = (
        P(("groups", "kvb"), None),
        P(("groups", "kvb"), "tp"),
        P(("groups", "kvb"), None),
        P(("groups", "kvb", "tp"), None, None),
        P("groups"),
        P(("groups", "kvb", "tp")),
        P(("groups", "kvb", "tp")),
        P(("groups", "kvb", "tp")),
        P("tp", None),
        P("tp"),
    )
    return jax.shard_map(
        on_device,
        mesh=mesh,
        in_specs=placed,
        out_specs=(P(("groups", "kvb"), "tp"), P(("groups", "kvb"), "tp")),
        check_vma=False,
    )
```

```python
import jax
import jax.numpy as jnp
from jax import lax
from jax.experimental import pallas as pl
from jax.experimental.pallas import tpu as pltpu
from jax.sharding import PartitionSpec as P

QH = 64
KVH = 8
HD = 128
BLK = 16

MASKED = -1e30
FLOOR = -1e20
EPSILON = 1e-06
UNIT = HD ** (-0.5) * 1.4426950408889634
STATS = 128
COVER = 20_000_000_000
SHARES = (4, 4, 4, 8, 12)
LATE = (4, 4, 4)
STEP = 512


def ahead(index, step, count):
    if count & (count - 1) == 0:
        return index ^ step
    return (index + step) % count


def behind(index, step, count):
    if count & (count - 1) == 0:
        return index ^ step
    return (index - step + count) % count


def once(body):
    trips = jnp.where(lax.axis_index("tp") >= 0, 1, 0)

    def trip(_, carried):
        body()
        return carried

    lax.fori_loop(0, trips, trip, 0)


def beside(weight, chunk, arrived, first, body):
    copy = pltpu.make_async_copy(weight.at[:, pl.ds(first, chunk.shape[1])], chunk, arrived)
    copy.start()
    once(body)
    copy.wait()


def prepare_body(count, *refs, first):
    inputs, weight, outs, chunk = refs[:5], refs[5], refs[6:10], refs[10]
    held, arrived, landed = refs[11:16], refs[16], refs[17]
    copies = [
        pltpu.make_async_copy(source, target, arrived.at[n])
        for n, (source, target) in enumerate(zip(inputs, held))
    ]
    for copy in copies:
        copy.start()

    def run():
        for copy in copies:
            copy.wait()
        prepare(count, *held, *outs)

    beside(weight, chunk, landed, first, run)


def prepare(
    count, lengths, slot_seq, slot_block, queries, new_kv, bias, fresh_out, value_out, own_out
):
    seq_total, tokens = bias.shape
    slots = tokens // BLK
    seq_rep, own_width = queries.shape
    local_heads = own_width // HD
    group_size = QH // KVH
    kvb_count = seq_total // seq_rep
    seq = slot_seq[...]
    length_of = jnp.zeros_like(seq)
    for s in range(seq_total):
        length_of = jnp.where(seq == s, lengths[s], length_of)
    slot_ids = lax.broadcasted_iota(jnp.int32, seq.shape, 1)
    remaining = jnp.clip(length_of - slot_block[...] * BLK, 0, BLK)
    remaining = jnp.where(slot_ids < count[0], remaining, 0)
    row = lax.broadcasted_iota(jnp.int32, (8, slots), 0)
    codes = jnp.where(row == 0, seq, jnp.where(row == 1, remaining, 0))
    spread = (
        lax.broadcasted_iota(jnp.int32, (slots, tokens), 1) // BLK
        == lax.broadcasted_iota(jnp.int32, (slots, tokens), 0)
    )
    per_token = jnp.dot(
        codes.astype(jnp.float32).astype(jnp.bfloat16),
        jnp.where(spread, 1.0, 0.0).astype(jnp.bfloat16),
        preferred_element_type=jnp.float32,
    )
    row = lax.broadcasted_iota(jnp.int32, (seq_total, tokens), 0)
    replica = behind(lax.axis_index("kvb"), row // seq_rep, kvb_count)
    seq_ids = (replica * seq_rep + row % seq_rep).astype(jnp.float32)
    offsets = (lax.broadcasted_iota(jnp.int32, (seq_total, tokens), 1) % BLK).astype(jnp.float32)
    live = (per_token[0:1] == seq_ids) & (offsets < per_token[1:2])
    bias[...] = jnp.where(live, 0.0, MASKED)

    own_out[...] = queries[...]
    kv_local = max(1, local_heads // group_size)
    kv_first = lax.axis_index("tp") * local_heads // group_size
    lane = lax.broadcasted_iota(jnp.int32, (seq_rep, STATS), 1)
    fresh = jnp.zeros((seq_rep, STATS), jnp.float32)
    for v in range(kv_local):
        at = pl.multiple_of((kv_first + v) * HD, HD)
        key = new_kv[:, pl.ds(at, HD)].astype(jnp.float32)
        at = pl.multiple_of((KVH + kv_first + v) * HD, HD)
        value_out[:, v * HD : (v + 1) * HD] = new_kv[:, pl.ds(at, HD)].astype(jnp.float32)
        for h in range(v * local_heads // kv_local, (v + 1) * local_heads // kv_local):
            query = queries[:, h * HD : (h + 1) * HD].astype(jnp.float32)
            score = jnp.sum(query * key, axis=1, keepdims=True)
            fresh = jnp.where(lane == h, score, fresh)
    fresh_out[...] = fresh * UNIT


def attend_first_body(bias_ref, queries, cache, weight, out, chunk, stacked, arrived, *, first):
    run = lambda: attend_body(bias_ref, queries, cache, out, stacked, shift=0)
    beside(weight, chunk, arrived, first, run)


def attend_body(bias_ref, queries, cache, out, stacked, *, shift):
    kvb_count, seq_rep, own_width = queries.shape
    tp_count = lax.axis_size("tp")
    tokens = cache.shape[0] * BLK
    seq_total = kvb_count * seq_rep
    local_heads = own_width // HD
    group_size = QH // KVH
    kv_local = max(1, local_heads // group_size)
    per_kv = local_heads // kv_local
    bias = bias_ref[...]
    for r in range(kvb_count):
        stacked[r * seq_rep : (r + 1) * seq_rep, :] = queries[r].astype(jnp.float32)
    t = lax.axis_index("tp") + shift
    t = jnp.where(t < tp_count, t, t - tp_count)
    lane = lax.broadcasted_iota(jnp.int32, (seq_total, STATS), 1)
    stats = jnp.zeros((seq_total, STATS), jnp.float32)
    for v in range(kv_local):
        heads = range(v * per_kv, (v + 1) * per_kv)
        rows = jnp.concatenate(
            [stacked[:, h * HD : (h + 1) * HD] for h in heads], axis=0
        ).astype(jnp.bfloat16)
        g = t * local_heads // group_size + v
        at = pl.multiple_of(g * HD, HD)
        keys = cache[:, :, pl.ds(at, HD)].reshape(tokens, HD)
        at = pl.multiple_of((KVH + g) * HD, HD)
        values = cache[:, :, pl.ds(at, HD)].reshape(tokens, HD)
        scores = lax.dot_general(
            rows, keys, (((1,), (1,)), ((), ())), preferred_element_type=jnp.float32
        )
        scores = scores.reshape(per_kv, seq_total, tokens) * UNIT + bias[None]
        peaks = jnp.maximum(jnp.max(scores, axis=2, keepdims=True), FLOOR)
        peaks = peaks.astype(jnp.bfloat16).astype(jnp.float32)
        weights = jnp.exp2(scores - peaks)
        sums = jnp.sum(weights, axis=2, keepdims=True)
        partial = jnp.dot(
            weights.astype(jnp.bfloat16).reshape(per_kv * seq_total, tokens),
            values,
            preferred_element_type=jnp.float32,
        )
        high = sums.astype(jnp.bfloat16).astype(jnp.float32)
        low = sums - high
        for j, h in enumerate(heads):
            out[:, h * HD : (h + 1) * HD] = partial[j * seq_total : (j + 1) * seq_total].astype(
                jnp.bfloat16
            )
            for part, value in enumerate((peaks, high, low)):
                stats = jnp.where(lane == part * local_heads + h, value[j], stats)
    out[:, local_heads * HD :] = stats.astype(jnp.bfloat16)


def fetch_body(weight, *refs, first):
    chunk, arrived = refs[-2:]
    copy = pltpu.make_async_copy(weight.at[:, pl.ds(first, chunk.shape[1])], chunk, arrived)
    copy.start()
    copy.wait()


def unpack(ref, local_heads):
    stats = ref[:, local_heads * HD :].astype(jnp.float32)
    sums = stats[:, local_heads : 2 * local_heads] + stats[:, 2 * local_heads : 3 * local_heads]
    return stats[:, :local_heads], sums


def merge_body(*refs, sources):
    parts, outs = refs[:sources], refs[sources:]
    seq_total, width = parts[0].shape
    seq_rep = outs[0].shape[0]
    local_heads = (width - STATS) // HD
    pairs = [unpack(part, local_heads) for part in parts]
    peak = pairs[0][0]
    for other, _ in pairs[1:]:
        peak = jnp.maximum(peak, other)
    scaling = [jnp.exp2(p - peak) for p, _ in pairs]
    total = sum(s * c for s, (_, c) in zip(scaling, pairs))
    high = total.astype(jnp.bfloat16).astype(jnp.float32)
    pad = jnp.zeros((seq_total, STATS - 3 * local_heads), jnp.float32)
    stats = jnp.concatenate([peak, high, total - high, pad], axis=1)
    blocks = [
        sum(
            s[:, h : h + 1] * part[:, h * HD : (h + 1) * HD].astype(jnp.float32)
            for s, part in zip(scaling, parts)
        )
        for h in range(local_heads)
    ]
    for h, block in enumerate(blocks + [stats]):
        for r, out in enumerate(outs):
            out[:, h * HD : (h + 1) * HD] = block[r * seq_rep : (r + 1) * seq_rep].astype(
                jnp.bfloat16
            )


def project_body(*refs, sources):
    parts = refs[:sources]
    fresh_ref, value_ref, weight = refs[sources : sources + 3]
    pieces = len(LATE)
    chunks = list(refs[sources + 3 : -3 - pieces])
    out, *late = refs[-3 - pieces : -2]
    arrived, rows = refs[-2:]
    first = weight.shape[1] - sum(piece.shape[1] for piece in late)
    copies = []
    for n, piece in enumerate(late):
        columns = pl.ds(first, piece.shape[1])
        copies.append(pltpu.make_async_copy(weight.at[:, columns], piece, arrived.at[n]))
        copies[-1].start()
        first += piece.shape[1]
    def combine():
        local_heads = (parts[0].shape[1] - STATS) // HD
        kv_local = value_ref.shape[1] // HD
        pairs = [unpack(part, local_heads) for part in parts]
        fresh = fresh_ref[:, :local_heads]
        overall = fresh
        for peak, _ in pairs:
            overall = jnp.maximum(overall, peak)
        scaling = [jnp.exp2(peak - overall) for peak, _ in pairs]
        fresh_weight = jnp.exp2(fresh - overall)
        inverse = 1.0 / (fresh_weight + sum(s * c for s, (_, c) in zip(scaling, pairs)))
        scaling = [s * inverse for s in scaling]
        fresh_weight = fresh_weight * inverse
        attended = []
        for h in range(local_heads):
            v = h * kv_local // local_heads
            total = fresh_weight[:, h : h + 1] * value_ref[:, v * HD : (v + 1) * HD]
            for s, part in zip(scaling, parts):
                total = total + s[:, h : h + 1] * part[:, h * HD : (h + 1) * HD].astype(jnp.float32)
            attended.append(total.astype(jnp.bfloat16))
        rows[...] = jnp.concatenate(attended, axis=1)

    once(combine)
    attended = rows[...]
    first = 0
    for n, chunk in enumerate(chunks + late):
        if n >= len(chunks):
            copies[n - len(chunks)].wait()
        for at in range(0, chunk.shape[1], STEP):
            step = min(STEP, chunk.shape[1] - at)
            out[:, first + at : first + at + step] = jnp.dot(
                attended, chunk[:, at : at + step], preferred_element_type=jnp.float32
            ).astype(out.dtype)
        first += chunk.shape[1]


def finish_body(pieces, residual, gain, stream_out, normed_out):
    full = residual[...].astype(jnp.float32)
    width = full.shape[1]
    total = pieces[0].astype(jnp.float32)
    for t in range(1, pieces.shape[0]):
        total = total + pieces[t].astype(jnp.float32)
    full = (full + total).astype(jnp.bfloat16).astype(jnp.float32)
    mean_square = jnp.sum(full * full, axis=1, keepdims=True) / width
    inverse = lax.rsqrt(mean_square + EPSILON)
    own = stream_out.shape[1]
    at = pl.multiple_of(lax.axis_index("tp") * own, own)
    mine = residual[:, pl.ds(at, own)].astype(jnp.float32)
    total = pieces[0, :, pl.ds(at, own)].astype(jnp.float32)
    for t in range(1, pieces.shape[0]):
        total = total + pieces[t, :, pl.ds(at, own)].astype(jnp.float32)
    stream = (mine + total).astype(jnp.bfloat16)
    stream_out[...] = stream
    normed_out[...] = (stream.astype(jnp.float32) * inverse * gain[...].astype(jnp.float32)).astype(
        jnp.bfloat16
    )


def vmem():
    return pl.BlockSpec(memory_space=pltpu.VMEM)


def resident(array):
    return pltpu.with_memory_space_constraint(array, pltpu.VMEM)


def hbm():
    return pl.BlockSpec(memory_space=pltpu.HBM)


def on_device(
    residual,
    queries,
    new_kv,
    kv_cache,
    lengths,
    slot_seq,
    slot_block,
    block_counts,
    out_weight,
    norm_gain,
):
    tp_count = lax.axis_size("tp")
    kvb_count = lax.axis_size("kvb")
    seq_rep, own_width = queries.shape
    seq_total = kvb_count * seq_rep
    tokens = kv_cache.shape[0] * BLK
    kv_local = max(1, own_width // HD * KVH // QH)
    depth, columns = out_weight.shape
    out_weight = pltpu.with_memory_space_constraint(out_weight, pltpu.HBM)
    share = [columns * n // sum(SHARES) for n in SHARES]
    starts = [sum(share[:n]) for n in range(len(share))]
    arrived = [
        lax.ppermute(queries, "kvb", [(k, ahead(k, r, kvb_count)) for k in range(kvb_count)])
        for r in range(1, kvb_count)
    ]
    bias, fresh, fresh_values, own_queries, under_prepare = pl.pallas_call(
        lambda *refs: prepare_body(*refs, first=starts[0]),
        out_shape=(
            jax.ShapeDtypeStruct((seq_total, tokens), jnp.float32),
            jax.ShapeDtypeStruct((seq_rep, STATS), jnp.float32),
            jax.ShapeDtypeStruct((seq_rep, kv_local * HD), jnp.float32),
            jax.ShapeDtypeStruct((seq_rep, own_width), jnp.bfloat16),
            pltpu.VMEM((depth, share[0]), out_weight.dtype),
        ),
        in_specs=[pl.BlockSpec(memory_space=pltpu.SMEM)] + [hbm()] * 6,
        out_specs=(vmem(),) * 5,
        scratch_shapes=[
            pltpu.SMEM(lengths.shape, jnp.int32),
            pltpu.VMEM((1,) + slot_seq.shape, jnp.int32),
            pltpu.VMEM((1,) + slot_block.shape, jnp.int32),
            pltpu.VMEM(queries.shape, queries.dtype),
            pltpu.VMEM(new_kv.shape, new_kv.dtype),
            pltpu.SemaphoreType.DMA((5,)),
            pltpu.SemaphoreType.DMA,
        ],
        compiler_params=pltpu.CompilerParams(vmem_limit_bytes=4 << 20),
        cost_estimate=pl.CostEstimate(flops=COVER, transcendentals=0, bytes_accessed=1 << 20),
        name="prepare",
    )(block_counts, *[
        pltpu.with_memory_space_constraint(array, pltpu.HBM)
        for array in (lengths, slot_seq[None], slot_block[None], queries, new_kv)
    ], out_weight)
    wide = jnp.stack([own_queries] + arrived)
    cache = resident(kv_cache)

    def fetch(first, size, *after):
        return pl.pallas_call(
            lambda *refs: fetch_body(*refs, first=first),
            out_shape=pltpu.VMEM((depth, size), out_weight.dtype),
            in_specs=[hbm()] + [pl.BlockSpec(memory_space=pl.ANY)] * len(after),
            out_specs=vmem(),
            scratch_shapes=[pltpu.SemaphoreType.DMA],
            compiler_params=pltpu.CompilerParams(vmem_limit_bytes=1 << 20),
            cost_estimate=pl.CostEstimate(flops=COVER, transcendentals=0, bytes_accessed=1 << 20),
            name="fetch",
        )(out_weight, *after)

    def attend(rows, shift):
        return pl.pallas_call(
            lambda *refs: attend_body(*refs, shift=shift),
            out_shape=jax.ShapeDtypeStruct((seq_total, own_width + STATS), jnp.bfloat16),
            in_specs=[vmem(), vmem(), vmem()],
            out_specs=vmem(),
            scratch_shapes=[pltpu.VMEM((seq_total, own_width), jnp.float32)],
            compiler_params=pltpu.CompilerParams(vmem_limit_bytes=6 << 20),
            cost_estimate=pl.CostEstimate(flops=COVER, transcendentals=0, bytes_accessed=1 << 20),
            name="attend",
        )(bias, rows, cache)

    def shifted(rows, shift):
        return lax.ppermute(rows, "tp", [(t, (t + shift) % tp_count) for t in range(tp_count)])

    first_part, under_attend = pl.pallas_call(
        lambda *refs: attend_first_body(*refs, first=starts[1]),
        out_shape=(
            jax.ShapeDtypeStruct((seq_total, own_width + STATS), jnp.bfloat16),
            pltpu.VMEM((depth, share[1]), out_weight.dtype),
        ),
        in_specs=[vmem(), vmem(), vmem(), hbm()],
        out_specs=(vmem(), vmem()),
        scratch_shapes=[
            pltpu.VMEM((seq_total, own_width), jnp.float32),
            pltpu.SemaphoreType.DMA,
        ],
        compiler_params=pltpu.CompilerParams(vmem_limit_bytes=6 << 20),
        cost_estimate=pl.CostEstimate(flops=COVER, transcendentals=0, bytes_accessed=1 << 20),
        name="attend_first",
    )(bias, wide, cache, out_weight)
    asked = [shifted(wide, -d) for d in range(1, tp_count)]
    parts = [first_part]
    chunks = [under_prepare, under_attend]
    for d in range(1, tp_count):
        parts.append(shifted(attend(asked[d - 1], d), d))
    chunks.append(fetch(starts[2], share[2], parts[0]))
    block = jax.ShapeDtypeStruct((seq_rep, own_width + STATS), jnp.bfloat16)
    dealt = pl.pallas_call(
        lambda *refs: merge_body(*refs, sources=tp_count),
        out_shape=(block,) * kvb_count,
        in_specs=[vmem()] * tp_count,
        out_specs=(vmem(),) * kvb_count,
        compiler_params=pltpu.CompilerParams(vmem_limit_bytes=4 << 20),
        name="merge",
    )(*parts)
    parts = [
        lax.ppermute(dealt[r], "kvb", [(k, behind(k, r, kvb_count)) for k in range(kvb_count)])
        for r in reversed(range(1, kvb_count))
    ]
    parts.append(dealt[0])
    chunks.append(fetch(starts[3], share[3], dealt[0]))
    projected = pl.pallas_call(
        lambda *refs: project_body(*refs, sources=kvb_count),
        out_shape=jax.ShapeDtypeStruct((seq_rep, out_weight.shape[1]), jnp.bfloat16),
        in_specs=[vmem()] * (kvb_count + 2) + [hbm()] + [vmem()] * len(chunks),
        out_specs=vmem(),
        scratch_shapes=[
            *[pltpu.VMEM((depth, share[4] * n // sum(LATE)), out_weight.dtype) for n in LATE],
            pltpu.SemaphoreType.DMA((len(LATE),)),
            pltpu.VMEM((seq_rep, own_width), jnp.bfloat16),
        ],
        compiler_params=pltpu.CompilerParams(vmem_limit_bytes=18 << 20),
        name="project",
    )(*parts, fresh, fresh_values, out_weight, *chunks)
    pieces = lax.all_gather(projected, "tp", axis=0, tiled=False)
    own = jax.ShapeDtypeStruct((seq_rep, norm_gain.shape[0]), jnp.bfloat16)
    return pl.pallas_call(
        finish_body,
        out_shape=(own, own),
        in_specs=[vmem(), vmem(), vmem()],
        out_specs=(vmem(), vmem()),
        compiler_params=pltpu.CompilerParams(vmem_limit_bytes=4 << 20),
        name="finish",
    )(pieces, residual, norm_gain[None])


def solution(mesh):
    placed = (
        P(("groups", "kvb"), None),
        P(("groups", "kvb"), "tp"),
        P(("groups", "kvb"), None),
        P(("groups", "kvb", "tp"), None, None),
        P("groups"),
        P(("groups", "kvb", "tp")),
        P(("groups", "kvb", "tp")),
        P(("groups", "kvb", "tp")),
        P("tp", None),
        P("tp"),
    )
    return jax.shard_map(
        on_device,
        mesh=mesh,
        in_specs=placed,
        out_specs=(P(("groups", "kvb"), "tp"), P(("groups", "kvb"), "tp")),
        check_vma=False,
    )
```
